256 devices in a mesh: ens: 2 (over z), gy: 128 (over x, y, core).
Axes of the slice: x: 8, y: 8, z: 2, core: 2. Of those that a mesh axis runs over, the one named last changes fastest.
The devices are a block of a 8x8x16 slice.
Arguments:
- forcing: float32 [4096, 16384], P(('ens', 'gy')), parts along dimension 0, may hold values from -6 to 6
- east: float32 [2048, 16384], P('gy'), may hold values from 0.5 to 2
- north: float32 [2048, 16384], P('gy'), may hold values from 0.5 to 2
- storage: float32 [2048, 16384], P('gy'), may hold values from 0.05 to 0.5
- coarse_inverse: float32 [64, 16, 16], replicated, as said below
- membership: int32 [32, 256], replicated, may hold values from 0 to 63, as said below
- land: int32 [32, 256], replicated, may hold values 0 or 1
Outputs:
- solution: float32 [4096, 16384], P(('ens', 'gy')), parts along dimension 0
- residual: float32 [4096, 16384], P(('ens', 'gy')), parts along dimension 0
The draws below stay inside these ranges and needn't reach their ends.
There are 2 independent parts, one for each index of `ens`. The reference program is written for one: setup_inputs(seed, part) draws one part's arguments, and reference() takes and returns one part's arrays. A program takes and returns all parts, laid end to end along the dimension named above; an argument that names none is the same for every part. Nothing has to cross between parts.
Inputs may be any that keep to these rules, and one draw needn't show every extreme that they name: `coarse_inverse`: each inverse is symmetric positive definite. `membership`: every basin holds one tile or more.
All inputs are finite; a program needn't handle non-finite values.
Results may differ from the reference program's by a relative error of at most 0.0003.
Values sent between devices are 32-bit elements; how exact they have to be, the bound alone decides.
No kernel may reach another device: no remote copies, remote signals or barrier semaphores. Data moves between devices by JAX's collectives and lax.ppermute only.
A program may use at most 64 MiB of HBM per device.

```python
import math
import jax
import jax.numpy as jnp
from jax import lax

TILES_X = 256
TILE = 64
BASINS = 64
ORDER = 4
ITERS = 2
COARSE = 16
NX = 16384
NY = 2048
TILE_ROWS = 32


def draw_forcing(key, part):
    return jnp.clip(jax.random.normal(key, (NY, NX), jnp.float32), -6.0, 6.0)


def draw_coarse_inverse(key, part):
    first = jax.random.fold_in(key, 11)
    second = jax.random.fold_in(key, 12)
    offdiag = jax.random.uniform(first, (BASINS, COARSE, COARSE), jnp.float32, -0.1, 0.1)
    offdiag = offdiag + jnp.swapaxes(offdiag, 1, 2)
    identity = jnp.eye(COARSE, dtype=jnp.float32)
    leading = jnp.exp(jax.random.uniform(second, (BASINS, COARSE), jnp.float32, math.log(3.5), math.log(6.0)))
    matrix = offdiag * (1.0 - identity)[None, :, :] + identity[None, :, :] * leading[:, :, None]
    cells = float(TILE_ROWS * TILES_X * TILE * TILE) / BASINS
    factor = 0.07 / math.sqrt(cells)
    return matrix * factor


def draw_membership(key, part):
    total = TILE_ROWS * TILES_X
    chosen = jax.random.permutation(jax.random.fold_in(key, 21), total)[:BASINS].astype(jnp.int32)
    seed_row = chosen // TILES_X
    seed_col = chosen % TILES_X
    rows = jnp.arange(TILE_ROWS, dtype=jnp.int32)[:, None, None]
    cols = jnp.arange(TILES_X, dtype=jnp.int32)[None, :, None]
    across = jnp.abs(cols - seed_col[None, None, :])
    across = jnp.minimum(across, TILES_X - across)
    distance = (rows - seed_row[None, None, :]) ** 2 + across ** 2
    score = distance * BASINS + jnp.arange(BASINS, dtype=jnp.int32)[None, None, :]
    return jnp.argmin(score, axis=-1).astype(jnp.int32)


def touch_ends(result, stream_key, smallest, top_value):
    index_at = [jax.random.randint(jax.random.fold_in(stream_key, axis), (), 0, length) for axis, length in enumerate(result.shape)]
    main_axis = result.shape.index(max(result.shape))
    next_to = index_at[:main_axis] + [(index_at[main_axis] + 1) % result.shape[main_axis]] + index_at[main_axis + 1:]
    return result.at[tuple(index_at)].set(smallest).at[tuple(next_to)].set(top_value)


def steps_of(stream_key, shape, shards, low, top_value):
    gain, own = 1.0, jax.random.fold_in(stream_key, 6)
    for position, shards_of in shards:
        steps = jnp.exp(jax.random.uniform(jax.random.fold_in(own, position), (shards_of,), jnp.float32, low / len(shards), top_value / len(shards)))
        gain = gain * jnp.repeat(steps, shape[position] // shards_of).reshape([-1 if axis == position else 1 for axis in range(len(shape))])
    return gain


def setup_inputs(seed: int = 0, part: int = 0) -> dict:
    keys = jax.random.split(jax.random.key(seed), 8)
    part_splits = jax.random.split(jax.random.fold_in(keys[7], part), 8)
    forcing = draw_forcing(jax.random.fold_in(jax.random.fold_in(keys[7], part), 71), part)
    east = jnp.clip(jnp.exp(math.log(2.0) - 1.3862944 * jax.random.uniform(keys[1], (NY, NX), jnp.float32) ** steps_of(keys[1], (NY, NX), ((0, 128),), -0.2, 0.2)), 0.5, 2.0)
    north = jnp.clip(jnp.exp(math.log(2.0) - 1.3862944 * jax.random.uniform(keys[2], (NY, NX), jnp.float32) ** steps_of(keys[2], (NY, NX), ((0, 128),), -0.2, 0.2)), 0.5, 2.0)
    storage = jnp.clip(jnp.exp(math.log(0.5) - 2.3025851 * jax.random.uniform(keys[3], (NY, NX), jnp.float32) ** steps_of(keys[3], (NY, NX), ((0, 128),), -0.2, 0.2)), 0.05, 0.5)
    coarse_inverse = draw_coarse_inverse(jax.random.fold_in(keys[7], 71), part)
    membership = draw_membership(jax.random.fold_in(keys[7], 71), part)
    land = touch_ends((jax.random.randint(keys[6], (TILE_ROWS, TILES_X), 0, 4) < 1).astype(jnp.int32), jax.random.fold_in(keys[6], 1), 0, 1)
    return dict(forcing=forcing, east=east, north=north, storage=storage, coarse_inverse=coarse_inverse, membership=membership, land=land)


HIGHEST = lax.Precision.HIGHEST


def mode_table():
    degree = jnp.arange(ORDER).astype(jnp.float32)
    local = jnp.arange(TILE).astype(jnp.float32)
    return jnp.cos(jnp.pi * degree[:, None] * (local[None, :] + 0.5) / TILE)


def reference(forcing, east, north, storage, coarse_inverse, membership, land):
    tile_rows, tiles_x = membership.shape
    modes = mode_table()
    wet = jnp.repeat(jnp.repeat(1.0 - land.astype(jnp.float32), TILE, axis=0), TILE, axis=1)
    above = jnp.concatenate([wet[1:], jnp.zeros_like(wet[:1])], axis=0)
    east_face = east * wet * jnp.roll(wet, -1, axis=1)
    north_face = north * wet * above
    south_face = jnp.concatenate([jnp.zeros_like(north_face[:1]), north_face[:-1]], axis=0)
    west_face = jnp.roll(east_face, 1, axis=1)
    center = (1.0 - wet) + wet * storage + east_face + west_face + north_face + south_face
    jacobi = 1.0 / center
    owned = (membership[:, :, None] == jnp.arange(BASINS)[None, None, :]).astype(jnp.float32)

    def operate(field):
        north_v = jnp.concatenate([field[1:], jnp.zeros_like(field[:1])], axis=0)
        south_v = jnp.concatenate([jnp.zeros_like(field[:1]), field[:-1]], axis=0)
        return (center * field - east_face * jnp.roll(field, -1, axis=1) - west_face * jnp.roll(field, 1, axis=1)
                - north_face * north_v - south_face * south_v)

    def precondition(field):
        blocks = (wet * field).reshape(tile_rows, TILE, tiles_x, TILE)
        lifted = jnp.einsum("aibk,pi->apbk", blocks, modes, precision=HIGHEST)
        per_tile = jnp.einsum("apbk,qk->abpq", lifted, modes, precision=HIGHEST).reshape(tile_rows, tiles_x, COARSE)
        sums = jnp.einsum("abn,abc->nc", owned, per_tile, precision=HIGHEST)
        coef = jnp.einsum("nij,nj->ni", coarse_inverse, sums, precision=HIGHEST)
        tile_coef = jnp.einsum("abn,nc->abc", owned, coef, precision=HIGHEST).reshape(tile_rows, tiles_x, ORDER, ORDER)
        spread = jnp.einsum("abpq,qk->apbk", tile_coef, modes, precision=HIGHEST)
        back = jnp.einsum("apbk,pi->aibk", spread, modes, precision=HIGHEST).reshape(field.shape)
        return jacobi * field + wet * back

    solution = jnp.zeros_like(forcing)
    residual = forcing
    smoothed = precondition(residual)
    direction = smoothed
    energy = jnp.sum(residual * smoothed)
    for step in range(ITERS):
        image = operate(direction)
        alpha = energy / jnp.sum(direction * image)
        solution = solution + alpha * direction
        residual = residual - alpha * image
        smoothed = precondition(residual)
        energy_next = jnp.sum(residual * smoothed)
        direction = smoothed + (energy_next / energy) * direction
        energy = energy_next
    return solution, residual
```

```python
import jax
import jax.numpy as jnp
import numpy as np
from jax import lax
from jax.experimental import pallas as pl
from jax.experimental.pallas import tpu as pltpu
from jax.sharding import Mesh
from jax.sharding import PartitionSpec as P

TILE = 64
ORDER = 4
GY = ("gy_0", "gy_1", "gy_2")
ENS_GY = ("ens", "gy_0", "gy_1", "gy_2")
F32, BF16, I32 = jnp.float32, jnp.bfloat16, jnp.int32
STEP = 16
PIECE = 8
BLOCK = 32


def tables():
    degree = np.arange(ORDER)[:, None]
    mode = np.cos(np.pi * degree * (np.arange(TILE)[None, :] + 0.5) / TILE)
    p_of = np.tile(np.repeat(np.arange(ORDER), ORDER), 2)
    q_of = np.tile(np.arange(ORDER), 2 * ORDER)
    half = np.repeat(np.arange(2), ORDER * ORDER)
    lane = np.arange(128)
    cols = (mode[q_of][:, lane % TILE] * (half[:, None] == lane[None, :] // TILE)).astype(np.float32)
    high = cols.astype(BF16)
    low = (cols - high.astype(np.float32)).astype(BF16)
    gather = np.concatenate([high, low], axis=0)
    scatter = np.concatenate([high, high, low, np.zeros_like(low)], axis=0)
    rows = mode[p_of].reshape(32, 8, 8).transpose(1, 0, 2).astype(np.float32)
    row_lanes = np.tile(rows, (1, 1, 16))
    row_subs = np.tile(rows.transpose(0, 2, 1), (1, 1, 4))
    ends = np.zeros((TILE // 16, 8, 128), np.float32)
    for k in range(TILE // 16):
        ends[k] = row_subs[(2 * k - 1) % 8, 7]
        ends[k, 0] = row_subs[(2 * k + 2) % 8, 0]
    return gather, scatter, row_lanes, row_subs, ends


def iotas(n):
    return lax.broadcasted_iota(I32, (n, 8, 128), 1), lax.broadcasted_iota(I32, (n, 8, 128), 2)


def onehot(left, right):
    lane = lax.broadcasted_iota(I32, (8, 128), 1)
    return jnp.where(jnp.where(lane < TILE, left, right) == lane % TILE, 1.0, 0.0)


def dot_nt(a, b):
    return lax.dot_general(a, b, (((1,), (1,)), ((), ())), preferred_element_type=F32)


def dot_nn(a, b):
    return lax.dot_general(a, b, (((1,), (0,)), ((), ())), preferred_element_type=F32)


def split(x):
    high = x.astype(BF16)
    return high, (x - high.astype(F32)).astype(BF16)


def moments(field, own, gather, row_lanes, block):
    lanes = [jnp.concatenate([row_lanes[block + r]] * (BLOCK * 8 // 128), axis=1) for r in range(2)]

    def step(k, total):
        first = pl.multiple_of(k * BLOCK, BLOCK)
        lifted = jnp.zeros((32, BLOCK * 8), F32)
        for r in range(2):
            high, low = split(field[r, pl.ds(first, BLOCK)].reshape(BLOCK * 8, 128))
            both = dot_nt(gather[...], high)
            lifted = lifted + lanes[r] * (both[:32] + both[32:] + dot_nt(gather[0:32], low))
        parts = dot_nn(jnp.concatenate(split(lifted), axis=0), own[pl.ds(first * 8, BLOCK * 8)])
        return total + parts[:32] + parts[32:]

    total = lax.fori_loop(0, field.shape[1] // BLOCK, step, jnp.zeros((32, 128), F32))
    sums = total[:16] + pltpu.roll(total[16:], TILE, 1)
    lane = lax.broadcasted_iota(I32, (8, 128), 1)
    return jnp.where(lane < TILE, sums[:8], pltpu.roll(sums[8:], TILE, 1))


def unpack(tile):
    return jnp.concatenate([tile, pltpu.roll(tile, TILE, 1)], axis=0)[:, :TILE]


def coarse_solve(inverse, sums):
    coef = jnp.zeros_like(sums)
    for j in range(sums.shape[0]):
        coef = coef + inverse[j] * sums[j : j + 1]
    return coef


def total_of(x):
    return jnp.sum(jnp.sum(x, axis=1, keepdims=True), axis=0, keepdims=True)


def spreader(coef, scatter, row_subs, ends, block):
    zero = jnp.zeros_like(coef)
    rows = [jnp.concatenate([coef, zero], axis=1), jnp.concatenate([zero, coef], axis=1)]
    high, low = split(jnp.concatenate(rows * 4, axis=0))
    patterns = [row_subs[block], row_subs[block + 1], ends[block // 2]]
    lane = lax.broadcasted_iota(I32, (1, 8, 128), 2)
    middle = (lane >= 32) & (lane < 64)

    def spread(own, ids):
        per_tile = (dot_nt(own, high) + dot_nt(own, low)).reshape(-1, 8, 128)
        result = []
        for r in ids:
            scaled = per_tile * patterns[r][None]
            rounded = scaled.astype(BF16).astype(F32)
            pieces = jnp.where(middle, scaled - rounded, rounded).astype(BF16)
            result.append(dot_nn(pieces.reshape(-1, 128), scatter[...]).reshape(-1, 8, 128))
        return result

    return spread


def first_kernel(codes, info, forcing, east, north, storage, gather, row_lanes,
                 east_o, north_o, center_o, own_o, own_end_o, sums_o, down_o, up_o):
    chunks = forcing.shape[1]
    basins = TILE
    lane = lax.broadcasted_iota(I32, (8, 128), 1)
    sub = lax.broadcasted_iota(I32, (8, 128), 0)

    def wet_of(code):
        return jnp.where(code < basins, 1.0, 0.0)

    def east_of(c):
        left, right = codes[0, 2 * c], codes[0, 2 * c + 1]
        after = codes[0, lax.rem(2 * c + 2, 2 * chunks)]
        wet = wet_of(jnp.where(lane < TILE, left, right))
        other = wet_of(jnp.where(lane < TILE - 1, left, jnp.where(lane < 127, right, after)))
        mask = wet * other
        return wet, [east[r, c] * mask for r in range(2)]

    def rolled(pair):
        return [pltpu.roll(x, 1, 1) for x in pair]

    last = east_of(chunks - 1)[1]
    for r in range(2):
        east_o[r, 0] = last[r]

    def pair_step(k, carry):
        owns, owns_end = [], []
        for j in range(2):
            c = 2 * k + j
            wet, face = east_of(c)
            up = wet_of(jnp.where(lane < TILE, codes[1, 2 * c], codes[1, 2 * c + 1]))
            turned = rolled(face)
            west = [jnp.where(lane == 0, carry[r], turned[r]) for r in range(2)]
            norths = [north[0, c] * wet, north[1, c] * jnp.where(sub < 7, wet, wet * up)]
            shifted = [pltpu.roll(x, 1, 0) for x in norths]
            south = [jnp.where(sub == 0, 0.0, shifted[0]), jnp.where(sub == 0, shifted[0], shifted[1])]
            for r in range(2):
                center = (1.0 - wet) + wet * storage[r, c] + face[r] + west[r] + norths[r] + south[r]
                east_o[r, c + 1] = face[r]
                north_o[r, c] = norths[r]
                center_o[r, c] = center
                if r == 0:
                    down_o[0, c] = forcing[0, c, 0:1]
                    down_o[1, c] = center[0:1]
                else:
                    up_o[0, c] = forcing[1, c, 7:8]
                    up_o[1, c] = center[7:8]
                    up_o[2, c] = norths[1][7:8]
            owns.append(onehot(codes[0, 2 * c], codes[0, 2 * c + 1]))
            owns_end.append(onehot(*[jnp.where(sub == 0, codes[1, 2 * c + i], codes[2, 2 * c + i]) for i in range(2)]))
            carry = turned
        own_o[pl.ds(pl.multiple_of(k * 16, 16), 16)] = jnp.concatenate(owns, axis=0).astype(BF16)
        own_end_o[pl.ds(pl.multiple_of(k * 16, 16), 16)] = jnp.concatenate(owns_end, axis=0).astype(BF16)
        return carry

    lax.fori_loop(0, chunks // 2, pair_step, rolled(last), unroll=2)
    tile = moments(forcing, own_o, gather, row_lanes, info[0])
    sums_o[...] = jnp.broadcast_to(tile[None], sums_o.shape)


def ends_of(from_up, from_down):
    sub = iotas(from_up.shape[0])[0]
    return jnp.where(sub == 0, from_up, from_down)


def apply_operator(z_pad, east, north, center, from_down, out, down_o, up_o):
    chunks = north.shape[1]
    z_pad[:, 0] = z_pad[:, chunks]
    z_pad[:, chunks + 1] = z_pad[:, 1]
    n = PIECE
    sub, lane = iotas(n)

    def step(k, total):
        c = pl.multiple_of(k * n, n)
        near = z_pad[2, pl.ds(c + 1, n)]
        own = [z_pad[r, pl.ds(c + 1, n)] for r in range(2)]
        faces = [north[r, pl.ds(c, n)] for r in range(2)]
        south_face = from_down[2, pl.ds(c, n)]
        below = [pltpu.roll(x, 1, 1) for x in (near * south_face, faces[0] * own[0], faces[1] * own[1])]
        above = [pltpu.roll(x, 7, 1) for x in (own[0], own[1], near)]
        for r in range(2):
            middle = center[r, pl.ds(c, n)]
            if r == 0:
                middle = middle + jnp.where(sub == 0, south_face, 0.0)
            ahead = pltpu.roll(z_pad[r, pl.ds(c + 1, n + 1)], 127, 2)
            ahead = jnp.where(lane == 127, ahead[1:], ahead[:-1])
            behind = pltpu.roll(east[r, pl.ds(c, n + 1)] * z_pad[r, pl.ds(c, n + 1)], 1, 2)
            behind = jnp.where(lane == 0, behind[:-1], behind[1:])
            image = (middle * own[r] - east[r, pl.ds(c + 1, n)] * ahead - behind
                     - faces[r] * jnp.where(sub == 7, above[r + 1], above[r])
                     - jnp.where(sub == 0, below[r], below[r + 1]))
            out[r, pl.ds(c, n)] = image
            if r == 0 and down_o is not None:
                down_o[pl.ds(c, n)] = image[:, 0:1]
            if r == 1 and up_o is not None:
                up_o[pl.ds(c, n)] = image[:, 7:8]
            total = total + jnp.sum(own[r] * image, axis=0)
        return total

    return lax.fori_loop(0, chunks // n, step, jnp.zeros((8, 128), F32))


def scalar_rows(values):
    sub = lax.broadcasted_iota(I32, (8, 128), 0)
    tile = jnp.zeros((8, 128), F32)
    for k, value in enumerate(values):
        tile = jnp.where(sub == k, value, tile)
    return tile


def second_kernel(info, parts, inverse, forcing, east, north, center, own, own_end, from_up, from_down,
                  gather, scatter, row_lanes, row_subs, ends,
                  z_o, image_o, jacobi_o, sums_o, kept_o, down_o, up_o, z_pad):
    chunks = forcing.shape[1]
    tile = jnp.sum(parts[...], axis=0)
    sums = unpack(tile)
    coef = coarse_solve(inverse, sums)
    kept_o[0:8] = tile
    kept_o[8:16] = jnp.broadcast_to(total_of(sums * coef), (8, 128))
    spread = spreader(coef, scatter, row_subs, ends, info[0])
    sub = iotas(STEP)[0]

    def step(k, total):
        c = pl.multiple_of(k * STEP, STEP)
        rows = pl.multiple_of(k * STEP * 8, STEP * 8)
        added = spread(own[pl.ds(rows, STEP * 8)], (0, 1)) + spread(own_end[pl.ds(rows, STEP * 8)], (2,))
        part = pl.ds(c, STEP)
        above = from_up[1, part] + pltpu.roll(north[1, part], 1, 1)
        below = jnp.broadcast_to(from_down[1, part], (STEP, 8, 128))
        near = jnp.where(sub == 0, above, below)
        centers = [center[0, part] + jnp.where(sub == 0, from_down[2, part], 0.0), center[1, part],
                   jnp.where(near == 0.0, 1.0, near)]
        fields = [forcing[0, part], forcing[1, part], ends_of(from_up[0, part], from_down[0, part])]
        for r in range(3):
            jacobi = 1.0 / centers[r]
            smooth = jacobi * fields[r]
            jacobi_o[r, part] = jacobi
            z = smooth + added[r]
            z_pad[r, pl.ds(c + 1, STEP)] = z
            if r < 2:
                z_o[r, part] = z
                total = total + jnp.sum(fields[r] * smooth, axis=0)
        return total

    smooth_total = lax.fori_loop(0, chunks // STEP, step, jnp.zeros((8, 128), F32))
    image_total = apply_operator(z_pad, east, north, center, from_down, image_o, down_o, up_o)
    tile = moments(image_o, own, gather, row_lanes, info[0])
    scalars = scalar_rows([jnp.sum(smooth_total, axis=0, keepdims=True), jnp.sum(image_total, axis=0, keepdims=True)])
    sums_o[...] = jnp.broadcast_to(jnp.concatenate([tile, scalars], axis=0)[None], sums_o.shape)


def third_kernel(info, parts, kept, inverse, forcing, image, jacobi, east, north, center, own, own_end,
                 from_up, from_down, image_up, image_down, scatter, row_subs, ends,
                 z_o, image_o, sums_o, scalars_o, z_pad):
    chunks = forcing.shape[1]
    tile = jnp.sum(parts[...], axis=0)
    energy = jnp.sum(tile[8:9], axis=1, keepdims=True) + kept[8:9, 0:1]
    alpha = energy / jnp.sum(tile[9:10], axis=1, keepdims=True)
    sums = unpack(kept[0:8] - alpha * tile[0:8])
    coef = coarse_solve(inverse, sums)
    scalars_o[...] = scalar_rows([alpha, energy, total_of(sums * coef)])
    spread = spreader(coef, scatter, row_subs, ends, info[0])
    factor = alpha.reshape(1, 1, 1)

    def step(k, total):
        c = pl.multiple_of(k * STEP, STEP)
        rows = pl.multiple_of(k * STEP * 8, STEP * 8)
        added = spread(own[pl.ds(rows, STEP * 8)], (0, 1)) + spread(own_end[pl.ds(rows, STEP * 8)], (2,))
        part = pl.ds(c, STEP)
        fields = [forcing[0, part], forcing[1, part], ends_of(from_up[0, part], from_down[0, part])]
        images = [image[0, part], image[1, part], ends_of(image_up[part], image_down[part])]
        for r in range(3):
            residual = fields[r] - factor * images[r]
            smooth = jacobi[r, part] * residual
            z = smooth + added[r]
            z_pad[r, pl.ds(c + 1, STEP)] = z
            if r < 2:
                z_o[r, part] = z
                total = total + jnp.sum(residual * smooth, axis=0)
        return total

    smooth_total = lax.fori_loop(0, chunks // STEP, step, jnp.zeros((8, 128), F32))
    image_total = apply_operator(z_pad, east, north, center, from_down, image_o, None, None)
    scalars = scalar_rows([jnp.sum(smooth_total, axis=0, keepdims=True), jnp.sum(image_total, axis=0, keepdims=True)])
    sums_o[...] = jnp.broadcast_to(scalars[None], sums_o.shape)


def last_kernel(parts, scalars, forcing, z_first, image_first, z_second, image_second, solution_o, residual_o):
    tile = jnp.sum(parts[...], axis=0)
    alpha, energy = scalars[0:1, 0:1], scalars[1:2, 0:1]
    energy_next = jnp.sum(tile[0:1], axis=1, keepdims=True) + scalars[2:3, 0:1]
    beta = energy_next / energy
    alpha_next = energy_next / (jnp.sum(tile[1:2], axis=1, keepdims=True) - beta * energy_next / alpha)
    alpha, beta, alpha_next = [x.reshape(1, 1, 1, 1) for x in (alpha, beta, alpha_next)]
    z, image = z_first[...], image_first[...]
    solution_o[...] = alpha * z + alpha_next * (z_second[...] + beta * z)
    residual_o[...] = (forcing[...] - alpha * image) - alpha_next * (image_second[...] + beta * image)


def body(forcing, east, north, storage, coarse_inverse, membership, land):
    rows, width = forcing.shape
    chunks = width // 128
    basins, coarse = coarse_inverse.shape[:2]
    tile_rows = membership.shape[0]
    total_rows = tile_rows * TILE
    start = lax.axis_index(GY) * rows
    code = membership + basins * land

    def codes_of(row, inside):
        at = jnp.clip(row // TILE, 0, tile_rows - 1)
        return jnp.where(inside, lax.dynamic_slice_in_dim(code, at, 1, 0), basins)

    codes = jnp.concatenate(
        [codes_of(start, True), codes_of(start + rows, start + rows < total_rows), codes_of(start - 1, start > 0)],
        axis=0,
    )
    info = (start % TILE // 8).reshape(1)
    gather, scatter, row_lanes, row_subs, ends = [jnp.asarray(x) for x in tables()]
    inverse = jnp.transpose(coarse_inverse, (2, 1, 0))

    def blocked(x):
        return x.reshape(2, 8, chunks, 128).transpose(0, 2, 1, 3)

    forcing, east, north, storage = [blocked(x) for x in (forcing, east, north, storage)]
    devices = lax.axis_size(GY)
    upward = [(i, i + 1) for i in range(devices - 1)]
    downward = [(j, i) for i, j in upward]
    inner, outer = lax.axis_size(GY[1]) * lax.axis_size(GY[2]), lax.axis_size(GY[0])

    def everywhere(copies):
        near = lax.all_to_all(copies, GY[1:], 0, 0)
        return lax.all_to_all(jnp.broadcast_to(jnp.sum(near, axis=0)[None], (outer,) + near.shape[1:]), GY[0], 0, 0)

    def call(kernel, outs, *args, scratch=()):
        places = [pl.BlockSpec(memory_space=pltpu.SMEM if x.dtype == I32 else pltpu.VMEM) for x in args]
        return pl.pallas_call(
            kernel,
            out_shape=[jax.ShapeDtypeStruct(s, d) for s, d in outs],
            in_specs=places,
            out_specs=[pl.BlockSpec(memory_space=pltpu.VMEM) for _ in outs],
            scratch_shapes=list(scratch),
        )(*args)

    own_shape = (2, chunks, 8, 128)
    line = (chunks, 1, 128)
    hot = (chunks * 8, 128)
    pad = pltpu.VMEM((3, chunks + 2, 8, 128), F32)
    east, north, center, own, own_end, sums, down, up = call(
        first_kernel,
        [((2, chunks + 1, 8, 128), F32), (own_shape, F32), (own_shape, F32), (hot, BF16), (hot, BF16),
         ((inner, 8, 128), F32), ((2,) + line, F32), ((3,) + line, F32)],
        codes, info, forcing, east, north, storage, gather, row_lanes,
    )
    from_up = lax.ppermute(down, GY, downward)
    from_down = lax.ppermute(up, GY, upward)
    parts = everywhere(sums)
    z_first, image_first, jacobi, sums, kept, down, up = call(
        second_kernel,
        [(own_shape, F32), (own_shape, F32), ((3, chunks, 8, 128), F32), ((inner, 16, 128), F32), ((16, 128), F32),
         (line, F32), (line, F32)],
        info, parts, inverse, forcing, east, north, center, own, own_end, from_up, from_down,
        gather, scatter, row_lanes, row_subs, ends,
        scratch=(pad,),
    )
    image_up = lax.ppermute(down, GY, downward)
    image_down = lax.ppermute(up, GY, upward)
    parts = everywhere(sums)
    z_second, image_second, sums, scalars = call(
        third_kernel,
        [(own_shape, F32), (own_shape, F32), ((inner, 8, 128), F32), ((8, 128), F32)],
        info, parts, kept, inverse, forcing, image_first, jacobi, east, north, center, own, own_end,
        from_up, from_down, image_up, image_down, scatter, row_subs, ends,
        scratch=(pad,),
    )
    parts = everywhere(sums)
    fields = (forcing, z_first, image_first, z_second, image_second)
    steps = chunks // STEP
    piece = pl.BlockSpec((2, STEP, 8, 128), lambda k: (0, k, 0, 0))
    answer = pl.pallas_call(
        last_kernel,
        grid=(steps,),
        out_shape=[jax.ShapeDtypeStruct(own_shape, F32)] * 2,
        in_specs=[pl.BlockSpec(parts.shape, lambda k: (0, 0, 0)), pl.BlockSpec((8, 128), lambda k: (0, 0))]
        + [piece] * len(fields),
        out_specs=[piece] * 2,
    )(parts, scalars, *fields)
    return tuple(x.transpose(0, 2, 1, 3).reshape(rows, width) for x in answer)


def solution(mesh):
    finer = Mesh(mesh.devices.reshape(mesh.shape["ens"], 8, 8, 2), ("ens", "gy_0", "gy_1", "gy_2"))
    return jax.shard_map(
        body,
        mesh=finer,
        in_specs=(P(ENS_GY, None), P(GY, None), P(GY, None), P(GY, None), P(), P(), P()),
        out_specs=(P(ENS_GY, None), P(ENS_GY, None)),
        check_vma=False,
    )
```

```python
import jax
import jax.numpy as jnp
import numpy as np
from jax import lax
from jax.experimental import pallas as pl
from jax.experimental.pallas import tpu as pltpu
from jax.sharding import Mesh
from jax.sharding import PartitionSpec as P

TILE = 64
ORDER = 4
GY = ("gy_0", "gy_1", "gy_2")
ENS_GY = ("ens", "gy_0", "gy_1", "gy_2")
F32, BF16, I32 = jnp.float32, jnp.bfloat16, jnp.int32
STEP = 16
PIECE = 8
BLOCK = 32
GROUPS = 4
SPACES = {"R": pltpu.HBM, "V": pltpu.VMEM}
VMEM_LIMIT = 24 * 2**20


def tables():
    degree = np.arange(ORDER)[:, None]
    mode = np.cos(np.pi * degree * (np.arange(TILE)[None, :] + 0.5) / TILE)
    p_of = np.tile(np.repeat(np.arange(ORDER), ORDER), 2)
    q_of = np.tile(np.arange(ORDER), 2 * ORDER)
    half = np.repeat(np.arange(2), ORDER * ORDER)
    lane = np.arange(128)
    cols = (mode[q_of][:, lane % TILE] * (half[:, None] == lane[None, :] // TILE)).astype(np.float32)
    high = cols.astype(BF16)
    low = (cols - high.astype(np.float32)).astype(BF16)
    gather = np.concatenate([high, low], axis=0)
    scatter = np.concatenate([high, high, low, np.zeros_like(low)], axis=0)
    rows = mode[p_of].reshape(32, 8, 8).transpose(1, 0, 2).astype(np.float32)
    row_lanes = np.tile(rows, (1, 1, 16))
    row_subs = np.tile(rows.transpose(0, 2, 1), (1, 1, 4))
    ends = np.zeros((TILE // 16, 8, 128), np.float32)
    for k in range(TILE // 16):
        ends[k, :4] = row_subs[(2 * k + 2) % 8, :4]
        ends[k, 4:] = row_subs[(2 * k - 1) % 8, 4:]
    return gather, scatter, row_lanes, row_subs, ends


def iotas(n):
    return lax.broadcasted_iota(I32, (n, 8, 128), 1), lax.broadcasted_iota(I32, (n, 8, 128), 2)


def onehot(codes):
    lane = lax.broadcasted_iota(I32, codes.shape, 2)
    return jnp.where(codes == (lane % TILE).astype(F32), 1.0, 0.0).reshape(-1, 128).astype(BF16)


def dot_nt(a, b):
    return lax.dot_general(a, b, (((1,), (1,)), ((), ())), preferred_element_type=F32)


def dot_nn(a, b):
    return lax.dot_general(a, b, (((1,), (0,)), ((), ())), preferred_element_type=F32)


def split(x):
    high = x.astype(BF16)
    return high, (x - high.astype(F32)).astype(BF16)


def moments(field, codes, gather, lanes, ready=None):
    wide = [jnp.concatenate([lanes[r]] * (BLOCK * 8 // 128), axis=1) for r in range(2)]

    def step(k, total):
        first = pl.multiple_of(k * BLOCK, BLOCK)
        if ready is not None:
            ready(k)
        lifted = jnp.zeros((32, BLOCK * 8), F32)
        for r in range(2):
            high, low = split(field[r, pl.ds(first, BLOCK)].reshape(BLOCK * 8, 128))
            both = dot_nt(gather[...], high)
            lifted = lifted + wide[r] * (both[:32] + both[32:] + dot_nt(gather[0:32], low))
        own = onehot(jnp.broadcast_to(codes[0, pl.ds(first, BLOCK)], (BLOCK, 8, 128)))
        parts = dot_nn(jnp.concatenate(split(lifted), axis=0), own)
        return total + parts[:32] + parts[32:]

    total = lax.fori_loop(0, codes.shape[1] // BLOCK, step, jnp.zeros((32, 128), F32))
    sums = total[:16] + pltpu.roll(total[16:], TILE, 1)
    lane = lax.broadcasted_iota(I32, (8, 128), 1)
    return jnp.where(lane < TILE, sums[:8], pltpu.roll(sums[8:], TILE, 1))


def unpack(tile):
    return jnp.concatenate([tile, pltpu.roll(tile, TILE, 1)], axis=0)[:, :TILE]


def coarse_solve(inverse, sums):
    coef = jnp.zeros_like(sums)
    for j in range(sums.shape[0]):
        coef = coef + inverse[j] * sums[j : j + 1]
    return coef


def total_of(x):
    return jnp.sum(jnp.sum(x, axis=1, keepdims=True), axis=0, keepdims=True)


def spreader(coef, scatter, patterns):
    zero = jnp.zeros_like(coef)
    rows = [jnp.concatenate([coef, zero], axis=1), jnp.concatenate([zero, coef], axis=1)]
    high, low = split(jnp.concatenate(rows * 4, axis=0))
    lane = lax.broadcasted_iota(I32, (1, 8, 128), 2)
    middle = (lane >= 32) & (lane < 64)

    def spread(codes, ids):
        own = onehot(codes)
        per_tile = (dot_nt(own, high) + dot_nt(own, low)).reshape(-1, 8, 128)
        result = []
        for r in ids:
            scaled = per_tile * patterns[r][None]
            rounded = scaled.astype(BF16).astype(F32)
            pieces = jnp.where(middle, scaled - rounded, rounded).astype(BF16)
            result.append(dot_nn(pieces.reshape(-1, 128), scatter[...]).reshape(-1, 8, 128))
        return result

    def all_of(codes, part):
        n = part.size
        sub = iotas(n)[0]
        own = jnp.broadcast_to(codes[0, part], (n, 8, 128))
        return spread(own, (0, 1)) + spread(jnp.where(sub < 4, codes[1, part], codes[2, part]), (2,))

    return all_of


def sum_kernel(parts, out):
    out[...] = jnp.broadcast_to(jnp.sum(parts[...], axis=0)[None], out.shape)


def scalar_rows(values):
    sub = lax.broadcasted_iota(I32, (8, 128), 0)
    tile = jnp.zeros((8, 128), F32)
    for k, value in enumerate(values):
        tile = jnp.where(sub == k, value, tile)
    return tile


def part_of(k, n):
    return pl.ds(pl.multiple_of(k * n, n), n)


class Loads:
    def __init__(self, pairs, sems, chunks):
        self.pairs, self.sems, self.size = pairs, sems, chunks // GROUPS

    def copy(self, i, group):
        source, target = self.pairs[i]
        part = part_of(group, self.size)
        return pltpu.make_async_copy(source.at[:, part], target.at[:, part], self.sems.at[i, group])

    def start(self, groups=range(4)):
        for group in groups:
            for i in range(len(self.pairs)):
                self.copy(i, group).start()

    def wait(self, group):
        for i in range(len(self.pairs)):
            self.copy(i, group).wait()

    def step(self, k, per_group):
        @pl.when(lax.rem(k, per_group) == 0)
        def _():
            self.wait(lax.div(k, per_group))


def moments_kernel(codes, info, forcing, gather, scatter, row_lanes, row_subs, ends,
                   sums_o, codes_o, gather_o, scatter_o, lanes_o, patterns_o, field, sems):
    chunks = forcing.shape[1]
    loads = Loads([(forcing, field)], sems, chunks)
    loads.start()
    lane = lax.broadcasted_iota(I32, (1, 128), 1)
    block = info[0]
    gather_o[...] = gather[...]
    scatter_o[...] = scatter[...]
    for r in range(2):
        lanes_o[r] = row_lanes[block + r]
        patterns_o[r] = row_subs[block + r]
    patterns_o[2] = ends[block // 2]

    def expand(c, carry):
        for row in range(3):
            codes_o[row, c] = jnp.where(lane < TILE, codes[row, 2 * c], codes[row, 2 * c + 1]).astype(F32)
        return carry

    lax.fori_loop(0, chunks, expand, 0, unroll=8)
    tile = moments(field, codes_o, gather, lanes_o, loads.wait)
    sums_o[...] = jnp.broadcast_to(tile[None], sums_o.shape)


def faces_kernel(codes, info, forcing, east, north, storage, east_o, north_o, center_o, mate_o, other_o,
                 f_in, e_in, n_in, s_in, sems):
    chunks = forcing.shape[1]
    basins = TILE
    loads = Loads([(forcing, f_in), (east, e_in), (north, n_in), (storage, s_in)], sems, chunks)
    loads.start((3, 0, 1, 2))
    lane = lax.broadcasted_iota(I32, (8, 128), 1)
    sub = lax.broadcasted_iota(I32, (8, 128), 0)
    odd = info[1] == 1

    def wet_of(code):
        return jnp.where(code < basins, 1.0, 0.0)

    def east_of(c):
        left, right = codes[0, 2 * c], codes[0, 2 * c + 1]
        after = codes[0, lax.rem(2 * c + 2, 2 * chunks)]
        wet = wet_of(jnp.where(lane < TILE, left, right))
        other = wet_of(jnp.where(lane < TILE - 1, left, jnp.where(lane < 127, right, after)))
        mask = wet * other
        return wet, [e_in[r, c] * mask for r in range(2)]

    def rolled(pair):
        return [pltpu.roll(x, 1, 1) for x in pair]

    loads.wait(3)
    last = east_of(chunks - 1)[1]
    for r in range(2):
        east_o[r, 0] = last[r]

    def chunk(c, carry):
        wet, face = east_of(c)
        up = wet_of(jnp.where(lane < TILE, codes[1, 2 * c], codes[1, 2 * c + 1]))
        turned = rolled(face)
        west = [jnp.where(lane == 0, carry[r], turned[r]) for r in range(2)]
        norths = [n_in[0, c] * wet, n_in[1, c] * jnp.where(sub < 7, wet, wet * up)]
        shifted = [pltpu.roll(x, 1, 0) for x in norths]
        south = [jnp.where(sub == 0, 0.0, shifted[0]), jnp.where(sub == 0, shifted[0], shifted[1])]
        centers = []
        for r in range(2):
            center = (1.0 - wet) + wet * s_in[r, c] + face[r] + west[r] + norths[r] + south[r]
            east_o[r, c + 1] = face[r]
            north_o[r, c] = norths[r]
            center_o[r, c] = center
            centers.append(center)
        fields = [f_in[0, c], f_in[1, c]]
        inner = jnp.where(sub < 4, fields[0], fields[1]) / jnp.where(sub < 4, centers[0], centers[1])
        first = [x[0][0:1] for x in (fields, centers, face, norths)] + [inner[1:2], inner[1:2]]
        final = [x[1][7:8] for x in (fields, centers, face, norths)] + [inner[6:7], norths[1][6:7]]
        for j in range(6):
            mate_o[j, c] = jnp.where(odd, first[j], final[j])
            other_o[j, c] = jnp.where(odd, final[j], first[j])
        return turned

    size = chunks // GROUPS

    def step(k, carry):
        @pl.when((lax.rem(k, size // 4) == 0) & (k < 3 * (size // 4)))
        def _():
            loads.wait(lax.div(k, size // 4))

        for j in range(4):
            carry = chunk(4 * k + j, carry)
        return carry

    lax.fori_loop(0, chunks // 4, step, rolled(last))


def apply_operator(z_pad, faces, blocks, out):
    east, north, center = faces
    chunks = z_pad.shape[1] - 2
    z_pad[:, 0] = z_pad[:, chunks]
    z_pad[:, chunks + 1] = z_pad[:, 1]
    n = PIECE
    sub, lane = iotas(n)

    def step(k, total):
        c = pl.multiple_of(k * n, n)
        own = [z_pad[r, pl.ds(c + 1, n)] for r in range(3)]
        faced = [north(r, pl.ds(c, n)) for r in range(3)]
        below = [pltpu.roll(faced[r] * own[r], 1, 1) for r in range(3)]
        above = [pltpu.roll(own[r], 7, 1) for r in range(3)]
        for r in range(blocks):
            ahead = pltpu.roll(z_pad[r, pl.ds(c + 1, n + 1)], 127, 2)
            ahead = jnp.where(lane == 127, ahead[1:], ahead[:-1])
            face = east(r, pl.ds(c, n + 1))
            behind = pltpu.roll(face * z_pad[r, pl.ds(c, n + 1)], 1, 2)
            behind = jnp.where(lane == 0, behind[:-1], behind[1:])
            image = (center(r, pl.ds(c, n)) * own[r] - face[1:] * ahead - behind
                     - faced[r] * jnp.where(sub == 7, above[(r + 1) % 3], above[r])
                     - jnp.where(sub == 0, below[(r + 2) % 3], below[r]))
            out[r, pl.ds(c, n)] = image
            if r < 2:
                total = total + jnp.sum(own[r] * image, axis=0)
        return total

    return lax.fori_loop(0, chunks // n, step, jnp.zeros((8, 128), F32))


def chooser(own, end):
    return lambda r, part: own[r, part] if r < 2 else end[part]


def beyond(mate, other, odd, part):
    sub = iotas(part.size)[0]
    after = jnp.logical_xor(sub < 4, odd)
    return lambda j: jnp.where(after, mate[j, part], other[j, part])


def end_rows(rows, north_last):
    sub = iotas(north_last.shape[0])[0]
    faced = jnp.where(sub == 6, rows(5), rows(3))
    center = rows(1) + jnp.where(sub == 0, pltpu.roll(north_last, 1, 1), 0.0)
    return rows(0), jnp.where(center == 0.0, 1.0, center), faced


def second_kernel(info, parts, inverse, forcing, mate, other, codes, gather, scatter, lanes, patterns, east, north, center_in,
                  z_o, image_o, sums_o, kept_o, center, field, mate_in, other_in, z_pad, image, end_e, end_n, end_c, sems, small):
    chunks = forcing.shape[1]
    loads = Loads([(forcing, field)], sems, chunks)
    halos = [pltpu.make_async_copy(x, y, small.at[i]) for i, (x, y) in enumerate([(mate, mate_in), (other, other_in)])]
    for copy in halos:
        copy.start()
    loads.start()
    tile = jnp.sum(parts[...], axis=0)
    sums = unpack(tile)
    coef = coarse_solve(inverse, sums)
    kept_o[0:8] = tile
    kept_o[8:16] = jnp.broadcast_to(total_of(sums * coef), (8, 128))
    spread = spreader(coef, scatter, patterns)
    sub = iotas(STEP)[0]
    odd = info[1] == 1
    for copy in halos:
        copy.wait()

    def step(k, total):
        part = part_of(k, STEP)
        loads.step(k, chunks // GROUPS // STEP)
        added = spread(codes, part)
        rows = beyond(mate_in, other_in, odd, part)
        end_f, end_center, end_north = end_rows(rows, north[1, part])
        end_n[part] = end_north
        end_c[part] = end_center
        end_e[pl.ds(k * STEP + 1, STEP)] = rows(2)
        first = center_in[0, part] + jnp.where(sub == 0, pltpu.roll(end_north, 1, 1), 0.0)
        center[0, part] = first
        center[1, part] = center_in[1, part]
        fields = [field[0, part], field[1, part], end_f]
        centers = [first, center[1, part], end_center]
        for r in range(3):
            smooth = fields[r] / centers[r]
            if r == 2:
                smooth = jnp.where((sub == 1) | (sub == 6), rows(4), smooth)
            z_pad[r, pl.ds(k * STEP + 1, STEP)] = smooth + added[r]
            if r < 2:
                total = total + jnp.sum(fields[r] * smooth, axis=0)
        return total

    smooth_total = lax.fori_loop(0, chunks // STEP, step, jnp.zeros((8, 128), F32))
    end_e[0] = end_e[chunks]
    save_z = pltpu.make_async_copy(z_pad.at[0:2, 1 : chunks + 1], z_o, small.at[2])
    save_z.start()
    faces = chooser(east, end_e), chooser(north, end_n), chooser(center, end_c)
    image_total = apply_operator(z_pad, faces, 3, image)
    save_image = pltpu.make_async_copy(image, image_o, small.at[3])
    save_image.start()
    tile = moments(image, codes, gather, lanes)
    scalars = scalar_rows([jnp.sum(smooth_total, axis=0, keepdims=True), jnp.sum(image_total, axis=0, keepdims=True)])
    sums_o[...] = jnp.broadcast_to(jnp.concatenate([tile, scalars], axis=0)[None], sums_o.shape)
    save_z.wait()
    save_image.wait()


def third_kernel(info, parts, kept, inverse, forcing, image, mate, other, codes, scatter, patterns, east, north, center,
                 z_o, image_o, sums_o, scalars_o, field, image_in, mate_in, other_in, z_pad, end_n, sems, small):
    chunks = forcing.shape[1]
    loads = Loads([(forcing, field), (image, image_in)], sems, chunks)
    halos = [pltpu.make_async_copy(x, y, small.at[i]) for i, (x, y) in enumerate([(mate, mate_in), (other, other_in)])]
    for copy in halos:
        copy.start()
    loads.start()
    tile = jnp.sum(parts[...], axis=0)
    energy = jnp.sum(tile[8:9], axis=1, keepdims=True) + kept[8:9, 0:1]
    alpha = energy / jnp.sum(tile[9:10], axis=1, keepdims=True)
    sums = unpack(kept[0:8] - alpha * tile[0:8])
    coef = coarse_solve(inverse, sums)
    scalars_o[...] = scalar_rows([alpha, energy, total_of(sums * coef)])
    spread = spreader(coef, scatter, patterns)
    factor = alpha.reshape(1, 1, 1)
    odd = info[1] == 1
    for copy in halos:
        copy.wait()

    def step(k, total):
        part = part_of(k, STEP)
        loads.step(k, chunks // GROUPS // STEP)
        added = spread(codes, part)
        end_f, end_center, end_n[part] = end_rows(beyond(mate_in, other_in, odd, part), north[1, part])
        fields = [field[0, part], field[1, part], end_f]
        centers = [center[0, part], center[1, part], end_center]
        for r in range(3):
            residual = fields[r] - factor * image_in[r, part]
            smooth = residual / centers[r]
            z = smooth + added[r]
            z_pad[r, pl.ds(k * STEP + 1, STEP)] = z
            if r < 2:
                z_o[r, part] = z
                total = total + jnp.sum(residual * smooth, axis=0)
        return total

    smooth_total = lax.fori_loop(0, chunks // STEP, step, jnp.zeros((8, 128), F32))
    faces = chooser(east, None), chooser(north, end_n), chooser(center, None)
    image_total = apply_operator(z_pad, faces, 2, image_o)
    scalars = scalar_rows([jnp.sum(smooth_total, axis=0, keepdims=True), jnp.sum(image_total, axis=0, keepdims=True)])
    sums_o[...] = jnp.broadcast_to(scalars[None], sums_o.shape)


def last_kernel(parts, scalars, forcing, z_first, image_first, z_second, image_second, solution_o, residual_o,
                f_in, z_in, image_in, solution_v, residual_v, sems, out_sems):
    chunks = forcing.shape[1]
    loads = Loads([(forcing, f_in), (z_first, z_in), (image_first.at[0:2], image_in)], sems, chunks)
    saves = Loads([(solution_v, solution_o), (residual_v, residual_o)], out_sems, chunks)
    loads.start()
    tile = jnp.sum(parts[...], axis=0)
    alpha, energy = scalars[0:1, 0:1], scalars[1:2, 0:1]
    energy_next = jnp.sum(tile[0:1], axis=1, keepdims=True) + scalars[2:3, 0:1]
    beta = energy_next / energy
    alpha_next = energy_next / (jnp.sum(tile[1:2], axis=1, keepdims=True) - beta * energy_next / alpha)
    alpha, beta, alpha_next = [x.reshape(1, 1, 1) for x in (alpha, beta, alpha_next)]
    per_group = chunks // GROUPS // PIECE

    def step(k, carry):
        loads.step(k, per_group)
        part = part_of(k, PIECE)
        for r in range(2):
            z, image = z_in[r, part], image_in[r, part]
            solution_v[r, part] = alpha * z + alpha_next * (z_second[r, part] + beta * z)
            residual_v[r, part] = (f_in[r, part] - alpha * image) - alpha_next * (image_second[r, part] + beta * image)

        @pl.when(lax.rem(k, per_group) == per_group - 1)
        def _():
            for i in range(2):
                saves.copy(i, lax.div(k, per_group)).start()

        return carry

    lax.fori_loop(0, chunks // PIECE, step, 0)
    for group in range(GROUPS):
        saves.wait(group)


def body(forcing, east, north, storage, coarse_inverse, membership, land):
    rows, width = forcing.shape
    chunks = width // 128
    basins = coarse_inverse.shape[0]
    tile_rows = membership.shape[0]
    total_rows = tile_rows * TILE
    index = lax.axis_index(GY)
    start = index * rows
    code = membership + basins * land

    def codes_of(row, inside):
        at = jnp.clip(row // TILE, 0, tile_rows - 1)
        return jnp.where(inside, lax.dynamic_slice_in_dim(code, at, 1, 0), basins)

    codes = jnp.concatenate(
        [codes_of(start, True), codes_of(start + rows, start + rows < total_rows), codes_of(start - 1, start > 0)],
        axis=0,
    )
    info = jnp.stack([start % TILE // 8, index % 2])
    inverse, codes = lax.optimization_barrier((jnp.transpose(coarse_inverse, (2, 1, 0)), codes))

    def blocked(x):
        return x.reshape(2, 8, chunks, 128).transpose(0, 2, 1, 3)

    forcing, east, north, storage = [blocked(x) for x in (forcing, east, north, storage)]
    devices = lax.axis_size(GY)
    mates = [(i, i ^ 1) for i in range(devices)]
    others = [(i, j) for i in range(devices) if (j := ((i + 1) ^ 1) - 1) in range(devices)]
    inner, outer = lax.axis_size(GY[1]) * lax.axis_size(GY[2]), lax.axis_size(GY[0])

    def call(kernel, outs, *args, scratch=(), label=""):
        places, values = [], []
        for x in args:
            kind = ""
            if isinstance(x, tuple):
                kind, x = x
            if x.dtype == I32:
                places.append(pl.BlockSpec(memory_space=pltpu.SMEM))
            elif kind in ("H", "R"):
                places.append(pl.BlockSpec(memory_space=pltpu.HBM if kind == "R" else pl.ANY))
            else:
                places.append(pl.BlockSpec(memory_space=pltpu.VMEM))
            values.append(pltpu.with_memory_space_constraint(x, SPACES[kind]) if kind in SPACES else x)
        shapes = [pltpu.VMEM(s, d) if k == "V" else jax.ShapeDtypeStruct(s, d) for k, s, d in outs]
        return pl.pallas_call(
            kernel,
            out_shape=shapes,
            in_specs=places,
            out_specs=[pl.BlockSpec(memory_space=pl.ANY if k == "H" else pltpu.VMEM) for k, _, _ in outs],
            scratch_shapes=list(scratch),
            compiler_params=pltpu.CompilerParams(vmem_limit_bytes=VMEM_LIMIT),
            name=label,
        )(*values)

    def everywhere(copies):
        near = lax.all_to_all(copies, GY[1:], 0, 0)
        (copies,) = call(sum_kernel, [("", (outer,) + near.shape[1:], F32)], near, label="middle")
        return lax.all_to_all(copies, GY[0], 0, 0)

    own_shape = (2, chunks, 8, 128)
    all_shape = (3, chunks, 8, 128)
    end_shape = (chunks, 8, 128)
    halo = (6, chunks, 1, 128)
    own_v, all_v, end_v, halo_v = [pltpu.VMEM(s, F32) for s in (own_shape, all_shape, end_shape, halo)]
    pad = pltpu.VMEM((3, chunks + 2, 8, 128), F32)

    def dma(*shape):
        return pltpu.SemaphoreType.DMA(shape)

    sums, lane_codes, gather, scatter, lanes, patterns = call(
        moments_kernel,
        [("", (inner, 8, 128), F32), ("V", (3, chunks, 1, 128), F32), ("V", (64, 128), BF16), ("V", (128, 128), BF16),
         ("V", (2, 32, 128), F32), ("V", (3, 8, 128), F32)],
        codes, info, ("R", forcing), *[jnp.asarray(x) for x in tables()],
        scratch=(own_v, dma(1, GROUPS)), label="moments",
    )
    parts = everywhere(sums)
    east, north, center, mate, other = call(
        faces_kernel,
        [("V", (2, chunks + 1, 8, 128), F32), ("V", own_shape, F32), ("V", own_shape, F32), ("", halo, F32), ("", halo, F32)],
        codes, info, ("R", forcing), ("R", east), ("R", north), ("R", storage),
        scratch=(own_v,) * 4 + (dma(4, GROUPS),), label="faces",
    )
    mate = lax.ppermute(mate, GY, mates)
    other = lax.ppermute(other, GY, others)
    kept_tables = [("V", x) for x in (gather, scatter, lanes, patterns)]
    z_first, image_first, sums, kept, center = call(
        second_kernel,
        [("H", own_shape, F32), ("H", all_shape, F32), ("", (inner, 16, 128), F32), ("", (16, 128), F32), ("V", own_shape, F32)],
        info, parts, inverse, ("H", forcing), ("H", mate), ("H", other), ("V", lane_codes), *kept_tables,
        ("V", east), ("V", north), ("V", center),
        scratch=(own_v, halo_v, halo_v, pad, all_v, pltpu.VMEM((chunks + 1, 8, 128), F32), end_v, end_v,
                 dma(1, GROUPS), dma(4)), label="second",
    )
    parts = everywhere(sums)
    z_second, image_second, sums, scalars = call(
        third_kernel,
        [("V", own_shape, F32), ("V", own_shape, F32), ("", (inner, 8, 128), F32), ("", (8, 128), F32)],
        info, parts, kept, inverse, ("H", forcing), ("H", image_first), ("H", mate), ("H", other), ("V", lane_codes),
        ("V", scatter), ("V", patterns), ("V", east), ("V", north), ("V", center),
        scratch=(own_v, all_v, halo_v, halo_v, pad, end_v, dma(2, GROUPS), dma(2)), label="third",
    )
    parts = everywhere(sums)
    answer = call(
        last_kernel,
        [("H", own_shape, F32)] * 2,
        parts, scalars, ("H", forcing), ("H", z_first), ("H", image_first), ("V", z_second), ("V", image_second),
        scratch=(own_v,) * 5 + (dma(3, GROUPS), dma(2, GROUPS)), label="last",
    )
    return tuple(x.transpose(0, 2, 1, 3).reshape(rows, width) for x in answer)


def solution(mesh):
    finer = Mesh(mesh.devices.reshape(mesh.shape["ens"], 8, 8, 2), ("ens", "gy_0", "gy_1", "gy_2"))
    return jax.shard_map(
        body,
        mesh=finer,
        in_specs=(P(ENS_GY, None), P(GY, None), P(GY, None), P(GY, None), P(), P(), P()),
        out_specs=(P(ENS_GY, None), P(ENS_GY, None)),
        check_vma=False,
    )
```

```python
import jax
import jax.numpy as jnp
import numpy as np
from jax import lax
from jax.experimental import pallas as pl
from jax.experimental.pallas import tpu as pltpu
from jax.sharding import Mesh
from jax.sharding import PartitionSpec as P


TILE = 64
ORDER = 4
GY = ("gy_0", "gy_1", "gy_2")
ENS_GY = ("ens", "gy_0", "gy_1", "gy_2")
F32, BF16, I32 = jnp.float32, jnp.bfloat16, jnp.int32
ROWS = 8
PIECE = 8
BLOCK = 32
GROUPS = 4
VMEM_LIMIT = 24 * 2**20


def tables():
    degree = np.arange(ORDER)[:, None]
    mode = np.cos(np.pi * degree * (np.arange(TILE)[None, :] + 0.5) / TILE)
    p_of = np.tile(np.repeat(np.arange(ORDER), ORDER), 2)
    q_of = np.tile(np.arange(ORDER), 2 * ORDER)
    half = np.repeat(np.arange(2), ORDER * ORDER)
    lane = np.arange(128)
    cols = (mode[q_of][:, lane % TILE] * (half[:, None] == lane[None, :] // TILE)).astype(np.float32)
    high = cols.astype(BF16)
    low = (cols - high.astype(np.float32)).astype(BF16)
    gather = np.concatenate([high, low], axis=0)
    scatter = np.concatenate([high, high, low, np.zeros_like(low)], axis=0)
    rows = mode[p_of].reshape(32, 8, 8).transpose(1, 0, 2).astype(np.float32)
    row_lanes = np.tile(rows, (1, 1, 16))
    row_subs = np.broadcast_to(mode.reshape(ORDER, 8, 8, 1).transpose(1, 0, 2, 3), (8, ORDER, 8, 128)).astype(np.float32)
    ends = np.zeros((TILE // 16, ORDER, 8, 128), np.float32)
    for k in range(TILE // 16):
        ends[k, :, :4] = row_subs[(2 * k + 2) % 8, :, :4]
        ends[k, :, 4:] = row_subs[(2 * k - 1) % 8, :, 4:]
    return gather, scatter, row_lanes, row_subs, ends


def iota(shape, dim):
    return lax.broadcasted_iota(I32, shape, dim)


def onehot(codes):
    return jnp.where(codes == (iota(codes.shape, 1) % TILE).astype(F32), 1.0, 0.0).astype(BF16)


def spread_row(ref, row):
    return jnp.broadcast_to(ref[pl.ds(row, 1)], (8, 128))


def dot_nt(a, b):
    return lax.dot_general(a, b, (((1,), (1,)), ((), ())), preferred_element_type=F32)


def dot_nn(a, b):
    return lax.dot_general(a, b, (((1,), (0,)), ((), ())), preferred_element_type=F32)


def split(x):
    high = x.astype(BF16)
    return high, (x - high.astype(F32)).astype(BF16)


def expand(codes_small, out):
    chunks, tiles = out.shape[1], codes_small.shape[1]
    mine = iota((chunks, tiles), 1) // 2 == iota((chunks, tiles), 0)
    halves = jnp.where(iota((tiles, 128), 0) % 2 == iota((tiles, 128), 1) // TILE, 1.0, 0.0).astype(BF16)
    for k in range(3):
        out[k] = dot_nn(jnp.where(mine, codes_small[k : k + 1], 0.0).astype(BF16), halves)


def moments(field, codes, gather, lanes, ready=None):
    wide = [jnp.concatenate([lanes[r]] * (BLOCK * 8 // 128), axis=1) for r in range(2)]

    def step(k, total):
        first = pl.multiple_of(k * BLOCK, BLOCK)
        if ready is not None:
            ready(k)
        lifted = jnp.zeros((32, BLOCK * 8), F32)
        for r in range(2):
            high, low = split(field[r, pl.ds(first, BLOCK)].reshape(BLOCK * 8, 128))
            both = dot_nt(gather[...], high)
            lifted = lifted + wide[r] * (both[:32] + both[32:] + dot_nt(gather[0:32], low))
        own = onehot(jnp.concatenate([spread_row(codes.at[0], first + j) for j in range(BLOCK)], axis=0))
        parts = dot_nn(jnp.concatenate(split(lifted), axis=0), own)
        return total + parts[:32] + parts[32:]

    total = lax.fori_loop(0, codes.shape[1] // BLOCK, step, jnp.zeros((32, 128), F32))
    sums = total[:16] + pltpu.roll(total[16:], TILE, 1)
    return jnp.where(iota((8, 128), 1) < TILE, sums[:8], pltpu.roll(sums[8:], TILE, 1))


def unpack(tile):
    return jnp.concatenate([tile, pltpu.roll(tile, TILE, 1)], axis=0)[:, :TILE]


def coarse_solve(inverse, sums):
    coef = jnp.zeros_like(sums)
    for j in range(sums.shape[0]):
        coef = coef + inverse[j] * sums[j : j + 1]
    return coef


def total_of(x):
    return jnp.sum(jnp.sum(x, axis=1, keepdims=True), axis=0, keepdims=True)


def column_tables(coef, codes, scatter, out):
    zero = jnp.zeros_like(coef)
    rows = [jnp.concatenate([coef, zero], axis=1), jnp.concatenate([zero, coef], axis=1)]
    high, low = split(jnp.concatenate(rows * 4, axis=0))
    for row in range(3):
        own = onehot(codes[row])
        per_tile = dot_nt(own, high) + dot_nt(own, low)
        lane = iota(per_tile.shape, 1)
        rounded = per_tile.astype(BF16).astype(F32)
        pieces = jnp.where(lane // 32 == 1, per_tile - rounded, rounded)
        split_p = [jnp.where(lane // ORDER % ORDER == p, pieces, 0.0).astype(BF16) for p in range(ORDER)]
        columns = dot_nn(jnp.concatenate(split_p, axis=0), scatter[...])
        for p in range(ORDER):
            out[row, p] = columns[p * codes.shape[1] : (p + 1) * codes.shape[1]]


def sum_kernel(parts, out):
    out[...] = jnp.broadcast_to(jnp.sum(parts[...], axis=0)[None], out.shape)


def scalar_rows(values):
    tile = jnp.zeros((8, 128), F32)
    for k, value in enumerate(values):
        tile = jnp.where(iota((8, 128), 0) == k, value, tile)
    return tile


class Loads:
    def __init__(self, pairs, sems, chunks):
        self.pairs, self.sems, self.size = pairs, sems, chunks // GROUPS

    def copy(self, i, group):
        source, target = self.pairs[i]
        part = pl.ds(pl.multiple_of(group * self.size, self.size), self.size)
        return pltpu.make_async_copy(source.at[:, part], target.at[:, part], self.sems.at[i, group])

    def start(self, groups=range(GROUPS)):
        for group in groups:
            for i in range(len(self.pairs)):
                self.copy(i, group).start()

    def wait(self, group):
        for i in range(len(self.pairs)):
            self.copy(i, group).wait()


def moments_kernel(info, forcing, membership, land, gather, scatter, row_lanes, row_subs, ends,
                   sums_o, codes_o, gather_o, scatter_o, lanes_o, patterns_o, field, codes, member_in, land_in, sems, small):
    chunks = forcing.shape[1]
    block = info[0]
    pairs = [(membership, member_in), (land, land_in), (gather, gather_o), (row_lanes.at[pl.ds(block, 2)], lanes_o),
             (scatter, scatter_o), (row_subs.at[pl.ds(block, 2)], patterns_o.at[0:2]), (ends.at[lax.div(block, 2)], patterns_o.at[2])]
    copies = [pltpu.make_async_copy(x, y, small.at[i]) for i, (x, y) in enumerate(pairs)]
    for copy in copies:
        copy.start()
    loads = Loads([(forcing, field)], sems, chunks)
    loads.start()
    for copy in copies:
        copy.wait()
    for k in range(3):
        row = pl.ds(jnp.maximum(info[2 + k], 0), 1)
        dry = (land_in[row] == 1) | (info[2 + k] < 0)
        codes_o[k : k + 1] = jnp.where(dry, TILE, member_in[row]).astype(F32)
    expand(codes_o, codes)
    tile = moments(field, codes, gather_o, lanes_o, loads.wait)
    sums_o[...] = jnp.broadcast_to(tile[None], sums_o.shape)


def faces_kernel(info, codes_small, forcing, east, north, storage, east_o, north_o, center_o, mate_h, other_h,
                 mate_o, other_o, codes, f_in, e_in, n_in, s_in, sems, small):
    chunks = forcing.shape[1]
    loads = Loads([(east, e_in), (north, n_in), (storage, s_in), (forcing, f_in)], sems, chunks)
    loads.start((3, 0, 1, 2))
    expand(codes_small, codes)
    lane, sub = iota((8, 128), 1), iota((8, 128), 0)
    odd = info[1] == 1

    def rolled(x):
        return pltpu.roll(x, 1, 1)

    def after_of(row):
        code = spread_row(codes.at[0], row)
        return code, pltpu.roll(code, 127, 1)

    def east_of(c, here, turned, turned_next):
        mask = (here < TILE) & (jnp.where(lane == 127, turned_next, turned) < TILE)
        return [jnp.where(mask, e_in[r, c], 0.0) for r in range(2)]

    first_code, first_turned = after_of(0)
    loads.wait(3)
    last = east_of(chunks - 1, *after_of(chunks - 1), first_turned)
    for r in range(2):
        east_o[r, 0] = last[r]

    def chunk(k, j, carry):
        west_before, here, turned = carry
        c = k * ROWS + j
        ahead = k * ROWS + j + 1 if j + 1 < ROWS else lax.rem(k * ROWS + ROWS, chunks)
        coming, coming_turned = after_of(ahead)
        face = east_of(c, here, turned, coming_turned)
        wet = here < TILE
        open_north = wet & ((sub < 7) | (spread_row(codes.at[1], c) < TILE))
        west_next = [rolled(x) for x in face]
        west = [jnp.where(lane == 0, west_before[r], west_next[r]) for r in range(2)]
        norths = [jnp.where(wet, n_in[0, c], 0.0), jnp.where(open_north, n_in[1, c], 0.0)]
        shifted = [pltpu.roll(x, 1, 0) for x in norths]
        south = [jnp.where(sub == 0, 0.0, shifted[0]), jnp.where(sub == 0, shifted[0], shifted[1])]
        fields, centers = [f_in[0, c], f_in[1, c]], []
        for r in range(2):
            center = jnp.where(wet, s_in[r, c], 1.0) + face[r] + west[r] + norths[r] + south[r]
            east_o[r, c + 1] = face[r]
            north_o[r, c] = norths[r]
            center_o[r, c] = center
            centers.append(center)
        smooth = jnp.where(sub < 4, fields[0], fields[1]) / jnp.where(sub < 4, centers[0], centers[1])
        first = [x[0][0:1] for x in (fields, centers, face, norths)] + [smooth[1:2]] * 2
        final = [x[1][7:8] for x in (fields, centers, face, norths)] + [smooth[6:7], norths[1][6:7]]
        for j in range(6):
            mate_o[j, c] = jnp.where(odd, first[j], final[j])
            other_o[j, c] = jnp.where(odd, final[j], first[j])
        return west_next, coming, coming_turned

    size = chunks // GROUPS // ROWS

    def step(k, carry):
        @pl.when((lax.rem(k, size) == 0) & (k < (GROUPS - 1) * size))
        def _():
            loads.wait(lax.div(k, size))

        for j in range(ROWS):
            carry = chunk(k, j, carry)
        return carry

    lax.fori_loop(0, chunks // ROWS, step, ([rolled(x) for x in last], first_code, first_turned))
    saves = [pltpu.make_async_copy(x, y, small.at[i]) for i, (x, y) in enumerate([(mate_o, mate_h), (other_o, other_h)])]
    for copy in saves:
        copy.start()
    for copy in saves:
        copy.wait()


def apply_operator(z_pad, faces, blocks, out):
    east, north, center = faces
    chunks = z_pad.shape[1] - 2
    z_pad[:, 0] = z_pad[:, chunks]
    z_pad[:, chunks + 1] = z_pad[:, 1]
    n = PIECE
    sub, lane = iota((n, 8, 128), 1), iota((n, 8, 128), 2)

    def step(k, total):
        c = pl.multiple_of(k * n, n)
        own = [z_pad[r, pl.ds(c + 1, n)] for r in range(3)]
        faced = [north(r, pl.ds(c, n)) for r in range(3)]
        below = [pltpu.roll(faced[r] * own[r], 1, 1) for r in range(3)]
        above = [pltpu.roll(own[r], 7, 1) for r in range(3)]
        for r in range(blocks):
            ahead = pltpu.roll(z_pad[r, pl.ds(c + 1, n + 1)], 127, 2)
            ahead = jnp.where(lane == 127, ahead[1:], ahead[:-1])
            face = east(r, pl.ds(c, n + 1))
            behind = pltpu.roll(face * z_pad[r, pl.ds(c, n + 1)], 1, 2)
            behind = jnp.where(lane == 0, behind[:-1], behind[1:])
            image = (center(r, pl.ds(c, n)) * own[r] - face[1:] * ahead - behind
                     - faced[r] * jnp.where(sub == 7, above[(r + 1) % 3], above[r])
                     - jnp.where(sub == 0, below[(r + 2) % 3], below[r]))
            out[r, pl.ds(c, n)] = image
            if r < 2:
                total = total + jnp.sum(own[r] * image, axis=0)
        return total

    return lax.fori_loop(0, chunks // n, step, jnp.zeros((8, 128), F32))


def chooser(*views):
    return lambda r, part: views[r][part]


class Spread:
    def __init__(self, columns, patterns):
        self.columns = columns
        self.patterns = [[patterns[r, p] for p in range(ORDER)] for r in range(3)]
        self.sub = iota((8, 128), 0)

    def at(self, c):
        def row(k, p):
            return spread_row(self.columns.at[k, p], c)

        own = [row(0, p) for p in range(ORDER)]
        end = [jnp.where(self.sub < 4, row(1, p), row(2, p)) for p in range(ORDER)]
        return [sum(self.patterns[r][p] * x[p] for p in range(ORDER)) for r, x in enumerate((own, own, end))]


def second_kernel(info, parts, forcing, mate_h, other_h, inverse, codes_small, gather, scatter, lanes, patterns, east, north, center,
                  field, z_pad, image_o, sums_o, kept_o, center_o, jacobi_o, end_f, end_n,
                  mate, other, codes, end_e, end_c, columns, sems, small):
    chunks = forcing.shape[1]
    halos = [pltpu.make_async_copy(x, y, small.at[i]) for i, (x, y) in enumerate([(mate_h, mate), (other_h, other)])]
    for copy in halos:
        copy.start()
    loads = Loads([(forcing, field)], sems, chunks)
    loads.start()
    expand(codes_small, codes)
    tile = jnp.sum(parts[...], axis=0)
    sums = unpack(tile)
    coef = coarse_solve(inverse, sums)
    kept_o[0:8] = tile
    kept_o[8:16] = jnp.broadcast_to(total_of(sums * coef), (8, 128))
    column_tables(coef, codes, scatter, columns)
    spread = Spread(columns, patterns)
    sub = iota((8, 128), 0)
    after = jnp.logical_xor(sub < 4, info[1] == 1)

    def chunk(c, total):
        added = spread.at(c)

        def rows(j):
            return jnp.where(after, mate[j, c], other[j, c])

        faced = jnp.where(sub == 6, rows(5), rows(3))
        far = rows(0)
        beyond = rows(1) + jnp.where(sub == 0, pltpu.roll(north[1, c], 1, 0), 0.0)
        first = center[0, c] + jnp.where(sub == 0, pltpu.roll(faced, 1, 0), 0.0)
        both = jnp.where(sub == 3, pltpu.roll(first, 3, 0), jnp.where(beyond == 0.0, 1.0, beyond))
        inverted = 1.0 / both
        own = [jnp.where(sub == 0, pltpu.roll(inverted, 5, 0), 1.0 / center[0, c]), 1.0 / center[1, c]]
        end_f[c] = far
        end_n[c] = faced
        end_e[c + 1] = rows(2)
        end_c[c] = both
        center_o[c] = first
        jacobi_o[0, c] = own[0]
        jacobi_o[1, c] = own[1]
        jacobi_o[2, c] = inverted
        smooth = [field[0, c] * own[0], field[1, c] * own[1],
                  jnp.where((sub == 1) | (sub == 6), rows(4), far * inverted)]
        for r in range(3):
            z_pad[r, c + 1] = smooth[r] + added[r]
        return total + (field[0, c] * smooth[0] + field[1, c] * smooth[1])

    size = chunks // GROUPS // ROWS
    for copy in halos:
        copy.wait()

    def step(k, total):
        @pl.when(lax.rem(k, size) == 0)
        def _():
            loads.wait(lax.div(k, size))

        for j in range(ROWS):
            total = chunk(k * ROWS + j, total)
        return total

    smooth_total = lax.fori_loop(0, chunks // ROWS, step, jnp.zeros((8, 128), F32))
    end_e[0] = end_e[chunks]
    faces = (chooser(east.at[0], east.at[1], end_e), chooser(north.at[0], north.at[1], end_n),
             chooser(center_o, center.at[1], end_c))
    image_total = apply_operator(z_pad, faces, 3, image_o)
    tile = moments(image_o, codes, gather, lanes)
    scalars = scalar_rows([jnp.sum(smooth_total, axis=0, keepdims=True), jnp.sum(image_total, axis=0, keepdims=True)])
    sums_o[...] = jnp.broadcast_to(jnp.concatenate([tile, scalars], axis=0)[None], sums_o.shape)


def third_kernel(parts, kept, inverse, forcing, image, codes_small, scatter, patterns, east, north, center,
                 first_center, jacobi, end_f, end_n, z_pad, image_o, sums_o, scalars_o, codes, columns):
    chunks = forcing.shape[1]
    expand(codes_small, codes)
    tile = jnp.sum(parts[...], axis=0)
    energy = jnp.sum(tile[8:9], axis=1, keepdims=True) + kept[8:9, 0:1]
    alpha = energy / jnp.sum(tile[9:10], axis=1, keepdims=True)
    sums = unpack(kept[0:8] - alpha * tile[0:8])
    coef = coarse_solve(inverse, sums)
    scalars_o[...] = scalar_rows([alpha, energy, total_of(sums * coef)])
    column_tables(coef, codes, scatter, columns)
    spread = Spread(columns, patterns)
    factor = jnp.broadcast_to(alpha, (8, 128))

    def chunk(c, total):
        added = spread.at(c)
        fields = [forcing[0, c], forcing[1, c], end_f[c]]
        for r in range(3):
            residual = fields[r] - factor * image[r, c]
            smooth = jacobi[r, c] * residual
            z_pad[r, c + 1] = smooth + added[r]
            if r < 2:
                total = total + residual * smooth
        return total

    def step(k, total):
        for j in range(ROWS):
            total = chunk(k * ROWS + j, total)
        return total

    smooth_total = lax.fori_loop(0, chunks // ROWS, step, jnp.zeros((8, 128), F32))
    faces = (chooser(east.at[0], east.at[1]), chooser(north.at[0], north.at[1], end_n), chooser(first_center, center.at[1]))
    image_total = apply_operator(z_pad, faces, 2, image_o)
    scalars = scalar_rows([jnp.sum(smooth_total, axis=0, keepdims=True), jnp.sum(image_total, axis=0, keepdims=True)])
    sums_o[...] = jnp.broadcast_to(scalars[None], sums_o.shape)


def last_kernel(parts, scalars, forcing, z_first, image_first, z_second, image_second, solution_o, residual_o,
                solution_v, residual_v, out_sems):
    chunks = forcing.shape[1]
    saves = Loads([(solution_v, solution_o), (residual_v, residual_o)], out_sems, chunks)
    tile = jnp.sum(parts[...], axis=0)
    alpha, energy = scalars[0:1, 0:1], scalars[1:2, 0:1]
    energy_next = jnp.sum(tile[0:1], axis=1, keepdims=True) + scalars[2:3, 0:1]
    beta = energy_next / energy
    alpha_next = energy_next / (jnp.sum(tile[1:2], axis=1, keepdims=True) - beta * energy_next / alpha)
    alpha, beta, alpha_next = [x.reshape(1, 1, 1) for x in (alpha, beta, alpha_next)]
    per_group = chunks // GROUPS // PIECE

    def step(k, carry):
        c = pl.multiple_of(k * PIECE, PIECE)
        part, shifted = pl.ds(c, PIECE), pl.ds(c + 1, PIECE)
        for r in range(2):
            z, image = z_first[r, shifted], image_first[r, part]
            solution_v[r, part] = alpha * z + alpha_next * (z_second[r, shifted] + beta * z)
            residual_v[r, part] = (forcing[r, part] - alpha * image) - alpha_next * (image_second[r, part] + beta * image)

        @pl.when(lax.rem(k, per_group) == per_group - 1)
        def _():
            for i in range(2):
                saves.copy(i, lax.div(k, per_group)).start()

        return carry

    lax.fori_loop(0, chunks // PIECE, step, 0)
    for group in range(GROUPS):
        saves.wait(group)


def body(forcing, east, north, storage, coarse_inverse, membership, land):
    rows, width = forcing.shape
    chunks = width // 128
    tile_rows = membership.shape[0]
    total_rows = tile_rows * TILE
    index = lax.axis_index(GY)
    start = index * rows
    info = jnp.stack([
        start % TILE // 8, index % 2, start // TILE,
        jnp.where(start + rows < total_rows, (start + rows) // TILE, -1), jnp.where(start > 0, (start - 1) // TILE, -1),
    ])
    inverse = jnp.transpose(coarse_inverse, (1, 2, 0))

    def blocked(x):
        return x.reshape(2, 8, chunks, 128).transpose(0, 2, 1, 3)

    forcing, east, north, storage = [blocked(x) for x in (forcing, east, north, storage)]
    devices = lax.axis_size(GY)
    mates = [(i, i ^ 1) for i in range(devices)]
    others = [(i, j) for i in range(devices) if (j := ((i + 1) ^ 1) - 1) in range(devices)]
    inner, outer = lax.axis_size(GY[1]) * lax.axis_size(GY[2]), lax.axis_size(GY[0])

    def call(kernel, outs, *args, scratch=()):
        places, kept_in = {"S": pltpu.SMEM, "H": pltpu.HBM}, {"V": pltpu.VMEM, "H": pltpu.HBM}
        kinds, values = [], []
        for kind, items in args:
            for x in items:
                kinds.append(kind)
                space = kept_in.get(kind)
                values.append(pltpu.with_memory_space_constraint(x, space) if space is not None else x)
        return pl.pallas_call(
            kernel,
            out_shape=[kept_in[k](s, d) if k in kept_in else jax.ShapeDtypeStruct(s, d) for k, s, d in outs],
            in_specs=[pl.BlockSpec(memory_space=places.get(k, pltpu.VMEM)) for k in kinds],
            out_specs=[pl.BlockSpec(memory_space=places.get(k, pltpu.VMEM)) for k, _, _ in outs],
            scratch_shapes=list(scratch),
            compiler_params=pltpu.CompilerParams(vmem_limit_bytes=VMEM_LIMIT),
        )(*values)

    def everywhere(copies):
        near = lax.all_to_all(copies, GY[1:], 0, 0)
        (copies,) = call(sum_kernel, [("", (outer,) + near.shape[1:], F32)], ("", [near]))
        return lax.all_to_all(copies, GY[0], 0, 0)

    own_shape, all_shape, end_shape = (2, chunks, 8, 128), (3, chunks, 8, 128), (chunks, 8, 128)
    halo, pad_shape = (6, chunks, 1, 128), (3, chunks + 2, 8, 128)
    own_v, halo_v = pltpu.VMEM(own_shape, F32), pltpu.VMEM(halo, F32)
    codes_v, columns = pltpu.VMEM((3, chunks, 128), F32), pltpu.VMEM((3, ORDER, chunks, 128), F32)

    def dma(*shape):
        return pltpu.SemaphoreType.DMA(shape)

    sums, codes, gather, scatter, lanes, patterns = call(
        moments_kernel,
        [("", (inner, 8, 128), F32), ("V", (8, membership.shape[1]), F32), ("V", (64, 128), BF16), ("V", (128, 128), BF16),
         ("V", (2, 32, 128), F32), ("V", (3, ORDER, 8, 128), F32)],
        ("S", [info]), ("H", [forcing, membership, land, *[jnp.asarray(x) for x in tables()]]),
        scratch=(own_v, codes_v, pltpu.VMEM(membership.shape, I32), pltpu.VMEM(land.shape, I32), dma(1, GROUPS), dma(7)),
    )
    parts = everywhere(sums)
    east, north, center, mate, other = call(
        faces_kernel,
        [("V", (2, chunks + 1, 8, 128), F32)] + [("V", own_shape, F32)] * 2 + [("H", halo, F32)] * 2,
        ("S", [info]), ("V", [codes]), ("H", [forcing, east, north, storage]),
        scratch=(halo_v, halo_v, codes_v) + (own_v,) * 4 + (dma(4, GROUPS), dma(2)),
    )
    mate = lax.ppermute(mate, GY, mates)
    other = lax.ppermute(other, GY, others)
    field, z_first, image_first, sums, kept, first_center, jacobi, end_f, end_n = call(
        second_kernel,
        [("V", own_shape, F32), ("V", pad_shape, F32), ("V", all_shape, F32), ("", (inner, 16, 128), F32), ("V", (16, 128), F32),
         ("V", end_shape, F32), ("V", all_shape, F32), ("V", end_shape, F32), ("V", end_shape, F32)],
        ("S", [info]), ("", [parts]), ("H", [forcing, mate, other]),
        ("V", [inverse, codes, gather, scatter, lanes, patterns, east, north, center]),
        scratch=(halo_v, halo_v, codes_v, pltpu.VMEM((chunks + 1, 8, 128), F32), pltpu.VMEM(end_shape, F32), columns,
                 dma(1, GROUPS), dma(2)),
    )
    parts = everywhere(sums)
    z_second, image_second, sums, scalars = call(
        third_kernel,
        [("V", pad_shape, F32), ("V", own_shape, F32), ("", (inner, 8, 128), F32), ("V", (8, 128), F32)],
        ("", [parts]),
        ("V", [kept, inverse, field, image_first, codes, scatter, patterns, east, north, center, first_center, jacobi, end_f, end_n]),
        scratch=(codes_v, columns),
    )
    parts = everywhere(sums)
    answer = call(
        last_kernel,
        [("H", own_shape, F32)] * 2,
        ("", [parts]), ("V", [scalars, field, z_first, image_first, z_second, image_second]),
        scratch=(own_v,) * 2 + (dma(2, GROUPS),),
    )
    return tuple(x.transpose(0, 2, 1, 3).reshape(rows, width) for x in answer)


def solution(mesh):
    finer = Mesh(mesh.devices.reshape(mesh.shape["ens"], 8, 8, 2), ("ens", "gy_0", "gy_1", "gy_2"))
    return jax.shard_map(
        body,
        mesh=finer,
        in_specs=(P(ENS_GY, None), P(GY, None), P(GY, None), P(GY, None), P(), P(), P()),
        out_specs=(P(ENS_GY, None), P(ENS_GY, None)),
        check_vma=False,
    )
```

```python
import jax
import jax.numpy as jnp
import numpy as np
from jax import lax
from jax.experimental import pallas as pl
from jax.experimental.pallas import tpu as pltpu
from jax.sharding import Mesh
from jax.sharding import PartitionSpec as P


TILE = 64
ORDER = 4
GY = ("gy_0", "gy_1", "gy_2")
ENS_GY = ("ens", "gy_0", "gy_1", "gy_2")
F32, BF16, I32 = jnp.float32, jnp.bfloat16, jnp.int32
ROWS = 8
PIECE = 8
BLOCK = 32
GROUPS = 4
VMEM_LIMIT = 24 * 2**20


def tables():
    degree = np.arange(ORDER)[:, None]
    mode = np.cos(np.pi * degree * (np.arange(TILE)[None, :] + 0.5) / TILE)
    p_of = np.tile(np.repeat(np.arange(ORDER), ORDER), 2)
    q_of = np.tile(np.arange(ORDER), 2 * ORDER)
    half = np.repeat(np.arange(2), ORDER * ORDER)
    lane = np.arange(128)
    cols = (mode[q_of][:, lane % TILE] * (half[:, None] == lane[None, :] // TILE)).astype(np.float32)
    high = cols.astype(BF16)
    low = (cols - high.astype(np.float32)).astype(BF16)
    gather = np.concatenate([high, low], axis=0)
    scatter = np.concatenate([high, high, low, np.zeros_like(low)], axis=0)
    rows = mode[p_of].reshape(32, 8, 8).transpose(1, 0, 2).astype(np.float32)
    row_lanes = np.tile(rows, (1, 1, 16))
    row_subs = np.broadcast_to(mode.reshape(ORDER, 8, 8, 1).transpose(1, 0, 2, 3), (8, ORDER, 8, 128)).astype(np.float32)
    ends = np.zeros((TILE // 16, ORDER, 8, 128), np.float32)
    for k in range(TILE // 16):
        ends[k, :, :4] = row_subs[(2 * k + 2) % 8, :, :4]
        ends[k, :, 4:] = row_subs[(2 * k - 1) % 8, :, 4:]
    return gather, scatter, row_lanes, row_subs, ends


def iota(shape, dim):
    return lax.broadcasted_iota(I32, shape, dim)


def onehot(codes):
    return jnp.where(codes == (iota(codes.shape, 1) % TILE).astype(F32), 1.0, 0.0).astype(BF16)


def spread_row(ref, row):
    return jnp.broadcast_to(ref[pl.ds(row, 1)], (8, 128))


def dot_nt(a, b):
    return lax.dot_general(a, b, (((1,), (1,)), ((), ())), preferred_element_type=F32)


def dot_nn(a, b):
    return lax.dot_general(a, b, (((1,), (0,)), ((), ())), preferred_element_type=F32)


def split(x):
    high = x.astype(BF16)
    return high, (x - high.astype(F32)).astype(BF16)


def expand(codes_small, out):
    chunks, tiles = out.shape[1], codes_small.shape[1]
    mine = iota((chunks, tiles), 1) // 2 == iota((chunks, tiles), 0)
    halves = jnp.where(iota((tiles, 128), 0) % 2 == iota((tiles, 128), 1) // TILE, 1.0, 0.0).astype(BF16)
    for k in range(3):
        out[k] = dot_nn(jnp.where(mine, codes_small[k : k + 1], 0.0).astype(BF16), halves)


def moments(field, codes, gather, lanes, ready=None):
    wide = [jnp.concatenate([lanes[r]] * (BLOCK * 8 // 128), axis=1) for r in range(2)]

    def step(k, total):
        first = pl.multiple_of(k * BLOCK, BLOCK)
        if ready is not None:
            ready(k)
        lifted = jnp.zeros((32, BLOCK * 8), F32)
        for r in range(2):
            high, low = split(field[r, pl.ds(first, BLOCK)].reshape(BLOCK * 8, 128))
            both = dot_nt(gather[...], high)
            lifted = lifted + wide[r] * (both[:32] + both[32:] + dot_nt(gather[0:32], low))
        own = onehot(jnp.concatenate([spread_row(codes.at[0], first + j) for j in range(BLOCK)], axis=0))
        parts = dot_nn(jnp.concatenate(split(lifted), axis=0), own)
        return total + parts[:32] + parts[32:]

    total = lax.fori_loop(0, codes.shape[1] // BLOCK, step, jnp.zeros((32, 128), F32))
    sums = total[:16] + pltpu.roll(total[16:], TILE, 1)
    return jnp.where(iota((8, 128), 1) < TILE, sums[:8], pltpu.roll(sums[8:], TILE, 1))


def unpack(tile):
    return jnp.concatenate([tile, pltpu.roll(tile, TILE, 1)], axis=0)[:, :TILE]


def coarse_solve(inverse, sums):
    coef = jnp.zeros_like(sums)
    for j in range(sums.shape[0]):
        coef = coef + inverse[j] * sums[j : j + 1]
    return coef


def total_of(x):
    return jnp.sum(jnp.sum(x, axis=1, keepdims=True), axis=0, keepdims=True)


def column_tables(coef, codes, scatter, out):
    zero = jnp.zeros_like(coef)
    rows = [jnp.concatenate([coef, zero], axis=1), jnp.concatenate([zero, coef], axis=1)]
    high, low = split(jnp.concatenate(rows * 4, axis=0))
    for row in range(3):
        own = onehot(codes[row])
        per_tile = dot_nt(own, high) + dot_nt(own, low)
        lane = iota(per_tile.shape, 1)
        rounded = per_tile.astype(BF16).astype(F32)
        pieces = jnp.where(lane // 32 == 1, per_tile - rounded, rounded)
        split_p = [jnp.where(lane // ORDER % ORDER == p, pieces, 0.0).astype(BF16) for p in range(ORDER)]
        columns = dot_nn(jnp.concatenate(split_p, axis=0), scatter[...])
        for p in range(ORDER):
            out[row, p] = columns[p * codes.shape[1] : (p + 1) * codes.shape[1]]


def sum_kernel(parts, out):
    out[...] = jnp.broadcast_to(jnp.sum(parts[...], axis=0)[None], out.shape)


def scalar_rows(values):
    tile = jnp.zeros((8, 128), F32)
    for k, value in enumerate(values):
        tile = jnp.where(iota((8, 128), 0) == k, value, tile)
    return tile


class Loads:
    def __init__(self, pairs, sems, chunks):
        self.pairs, self.sems, self.size = pairs, sems, chunks // GROUPS

    def copy(self, i, group):
        source, target = self.pairs[i]
        part = pl.ds(pl.multiple_of(group * self.size, self.size), self.size)
        return pltpu.make_async_copy(source.at[:, part], target.at[:, part], self.sems.at[i, group])

    def start(self, groups=range(GROUPS)):
        for group in groups:
            for i in range(len(self.pairs)):
                self.copy(i, group).start()

    def wait(self, group):
        for i in range(len(self.pairs)):
            self.copy(i, group).wait()


def moments_kernel(info, forcing, membership, land, gather, scatter, row_lanes, row_subs, ends,
                   sums_o, codes_o, gather_o, scatter_o, lanes_o, patterns_o, field, codes, member_in, land_in, sems, small):
    chunks = forcing.shape[1]
    block = info[0]
    pairs = [(membership, member_in), (land, land_in), (gather, gather_o), (row_lanes.at[pl.ds(block, 2)], lanes_o),
             (scatter, scatter_o), (row_subs.at[pl.ds(block, 2)], patterns_o.at[0:2]), (ends.at[lax.div(block, 2)], patterns_o.at[2])]
    copies = [pltpu.make_async_copy(x, y, small.at[i]) for i, (x, y) in enumerate(pairs)]
    for copy in copies:
        copy.start()
    loads = Loads([(forcing, field)], sems, chunks)
    loads.start()
    for copy in copies:
        copy.wait()
    for k in range(3):
        row = pl.ds(jnp.maximum(info[2 + k], 0), 1)
        dry = (land_in[row] == 1) | (info[2 + k] < 0)
        codes_o[k : k + 1] = jnp.where(dry, TILE, member_in[row]).astype(F32)
    expand(codes_o, codes)
    tile = moments(field, codes, gather_o, lanes_o, loads.wait)
    sums_o[...] = jnp.broadcast_to(tile[None], sums_o.shape)


def faces_kernel(info, codes_small, forcing, east, north, storage, east_o, north_h, center_h, mate_o, other_o,
                 north_o, center_o, codes, f_in, e_in, n_in, s_in, sems, out_sems):
    chunks = forcing.shape[1]
    loads = Loads([(east, e_in), (north, n_in), (storage, s_in), (forcing, f_in)], sems, chunks)
    loads.start((3, 0, 1, 2))
    saves = Loads([(north_o, north_h), (center_o, center_h)], out_sems, chunks)
    expand(codes_small, codes)
    lane, sub = iota((8, 128), 1), iota((8, 128), 0)
    odd = info[1] == 1

    def rolled(x):
        return pltpu.roll(x, 1, 1)

    def after_of(row):
        code = spread_row(codes.at[0], row)
        return code, pltpu.roll(code, 127, 1)

    def east_of(c, here, turned, turned_next):
        mask = (here < TILE) & (jnp.where(lane == 127, turned_next, turned) < TILE)
        return [jnp.where(mask, e_in[r, c], 0.0) for r in range(2)]

    first_code, first_turned = after_of(0)
    loads.wait(3)
    last = east_of(chunks - 1, *after_of(chunks - 1), first_turned)
    for r in range(2):
        east_o[r, 0] = last[r]

    def chunk(k, j, carry):
        west_before, here, turned = carry
        c = k * ROWS + j
        ahead = k * ROWS + j + 1 if j + 1 < ROWS else lax.rem(k * ROWS + ROWS, chunks)
        coming, coming_turned = after_of(ahead)
        face = east_of(c, here, turned, coming_turned)
        wet = here < TILE
        open_north = wet & ((sub < 7) | (spread_row(codes.at[1], c) < TILE))
        west_next = [rolled(x) for x in face]
        west = [jnp.where(lane == 0, west_before[r], west_next[r]) for r in range(2)]
        norths = [jnp.where(wet, n_in[0, c], 0.0), jnp.where(open_north, n_in[1, c], 0.0)]
        shifted = [pltpu.roll(x, 1, 0) for x in norths]
        south = [jnp.where(sub == 0, 0.0, shifted[0]), jnp.where(sub == 0, shifted[0], shifted[1])]
        fields, centers = [f_in[0, c], f_in[1, c]], []
        for r in range(2):
            center = jnp.where(wet, s_in[r, c], 1.0) + face[r] + west[r] + norths[r] + south[r]
            east_o[r, c + 1] = face[r]
            north_o[r, c] = norths[r]
            center_o[r, c] = center
            centers.append(center)
        smooth = jnp.where(sub < 4, fields[0], fields[1]) / jnp.where(sub < 4, centers[0], centers[1])
        first = [x[0][0:1] for x in (fields, centers, face, norths)] + [smooth[1:2]] * 2
        final = [x[1][7:8] for x in (fields, centers, face, norths)] + [smooth[6:7], norths[1][6:7]]
        for j in range(6):
            mate_o[j, c] = jnp.where(odd, first[j], final[j])
            other_o[j, c] = jnp.where(odd, final[j], first[j])
        return west_next, coming, coming_turned

    size = chunks // GROUPS // ROWS

    def step(k, carry):
        @pl.when((lax.rem(k, size) == 0) & (k < (GROUPS - 1) * size))
        def _():
            loads.wait(lax.div(k, size))

        for j in range(ROWS):
            carry = chunk(k, j, carry)

        @pl.when(lax.rem(k, size) == size - 1)
        def _():
            for i in range(2):
                saves.copy(i, lax.div(k, size)).start()

        return carry

    lax.fori_loop(0, chunks // ROWS, step, ([rolled(x) for x in last], first_code, first_turned))
    for group in range(GROUPS):
        saves.wait(group)


def apply_operator(z_pad, faces, blocks, out):
    east, north, center = faces
    chunks = z_pad.shape[1] - 2
    z_pad[:, 0] = z_pad[:, chunks]
    z_pad[:, chunks + 1] = z_pad[:, 1]
    n = PIECE
    sub, lane = iota((n, 8, 128), 1), iota((n, 8, 128), 2)

    def step(k, total):
        c = pl.multiple_of(k * n, n)
        own = [z_pad[r, pl.ds(c + 1, n)] for r in range(3)]
        faced = [north(r, pl.ds(c, n)) for r in range(3)]
        below = [pltpu.roll(faced[r] * own[r], 1, 1) for r in range(3)]
        above = [pltpu.roll(own[r], 7, 1) for r in range(3)]
        for r in range(blocks):
            ahead = pltpu.roll(z_pad[r, pl.ds(c + 1, n + 1)], 127, 2)
            ahead = jnp.where(lane == 127, ahead[1:], ahead[:-1])
            face = east(r, pl.ds(c, n + 1))
            behind = pltpu.roll(face * z_pad[r, pl.ds(c, n + 1)], 1, 2)
            behind = jnp.where(lane == 0, behind[:-1], behind[1:])
            image = (center(r, pl.ds(c, n)) * own[r] - face[1:] * ahead - behind
                     - faced[r] * jnp.where(sub == 7, above[(r + 1) % 3], above[r])
                     - jnp.where(sub == 0, below[(r + 2) % 3], below[r]))
            out[r, pl.ds(c, n)] = image
            if r < 2:
                total = total + jnp.sum(own[r] * image, axis=0)
        return total

    return lax.fori_loop(0, chunks // n, step, jnp.zeros((8, 128), F32))


def chooser(*views):
    return lambda r, part: views[r][part]


class Spread:
    def __init__(self, columns, patterns):
        self.columns = columns
        self.patterns = [[patterns[r, p] for p in range(ORDER)] for r in range(3)]
        self.sub = iota((8, 128), 0)

    def at(self, c):
        def row(k, p):
            return spread_row(self.columns.at[k, p], c)

        own = [row(0, p) for p in range(ORDER)]
        end = [jnp.where(self.sub < 4, row(1, p), row(2, p)) for p in range(ORDER)]
        return [sum(self.patterns[r][p] * x[p] for p in range(ORDER)) for r, x in enumerate((own, own, end))]


def second_kernel(info, parts, forcing, north_h, center_h, mate, other, inverse, codes_small, gather, scatter, lanes, patterns, east,
                  field, north, center, z_pad, image_o, sums_o, kept_o, jacobi_o, end_f, end_n,
                  codes, end_e, end_c, columns, sems):
    chunks = forcing.shape[1]
    loads = Loads([(forcing, field), (north_h, north), (center_h, center)], sems, chunks)
    loads.start()
    expand(codes_small, codes)
    tile = jnp.sum(parts[...], axis=0)
    sums = unpack(tile)
    coef = coarse_solve(inverse, sums)
    kept_o[0:8] = tile
    kept_o[8:16] = jnp.broadcast_to(total_of(sums * coef), (8, 128))
    column_tables(coef, codes, scatter, columns)
    spread = Spread(columns, patterns)
    sub = iota((8, 128), 0)
    after = jnp.logical_xor(sub < 4, info[1] == 1)

    def chunk(c, total):
        added = spread.at(c)

        def rows(j):
            return jnp.where(after, mate[j, c], other[j, c])

        faced = jnp.where(sub == 6, rows(5), rows(3))
        far = rows(0)
        beyond = rows(1) + jnp.where(sub == 0, pltpu.roll(north[1, c], 1, 0), 0.0)
        first = center[0, c] + jnp.where(sub == 0, pltpu.roll(faced, 1, 0), 0.0)
        both = jnp.where(sub == 3, pltpu.roll(first, 3, 0), jnp.where(beyond == 0.0, 1.0, beyond))
        inverted = 1.0 / both
        own = [jnp.where(sub == 0, pltpu.roll(inverted, 5, 0), 1.0 / first), 1.0 / center[1, c]]
        end_f[c] = far
        end_n[c] = faced
        end_e[c + 1] = rows(2)
        end_c[c] = both
        center[0, c] = first
        jacobi_o[0, c] = own[0]
        jacobi_o[1, c] = own[1]
        jacobi_o[2, c] = inverted
        smooth = [field[0, c] * own[0], field[1, c] * own[1],
                  jnp.where((sub == 1) | (sub == 6), rows(4), far * inverted)]
        for r in range(3):
            z_pad[r, c + 1] = smooth[r] + added[r]
        return total + (field[0, c] * smooth[0] + field[1, c] * smooth[1])

    size = chunks // GROUPS // ROWS

    def step(k, total):
        @pl.when(lax.rem(k, size) == 0)
        def _():
            loads.wait(lax.div(k, size))

        for j in range(ROWS):
            total = chunk(k * ROWS + j, total)
        return total

    smooth_total = lax.fori_loop(0, chunks // ROWS, step, jnp.zeros((8, 128), F32))
    end_e[0] = end_e[chunks]
    faces = (chooser(east.at[0], east.at[1], end_e), chooser(north.at[0], north.at[1], end_n),
             chooser(center.at[0], center.at[1], end_c))
    image_total = apply_operator(z_pad, faces, 3, image_o)
    tile = moments(image_o, codes, gather, lanes)
    scalars = scalar_rows([jnp.sum(smooth_total, axis=0, keepdims=True), jnp.sum(image_total, axis=0, keepdims=True)])
    sums_o[...] = jnp.broadcast_to(jnp.concatenate([tile, scalars], axis=0)[None], sums_o.shape)


def third_kernel(parts, kept, inverse, forcing, image, codes_small, scatter, patterns, east, north, center,
                 jacobi, end_f, end_n, z_pad, image_o, sums_o, scalars_o, codes, columns):
    chunks = forcing.shape[1]
    expand(codes_small, codes)
    tile = jnp.sum(parts[...], axis=0)
    energy = jnp.sum(tile[8:9], axis=1, keepdims=True) + kept[8:9, 0:1]
    alpha = energy / jnp.sum(tile[9:10], axis=1, keepdims=True)
    sums = unpack(kept[0:8] - alpha * tile[0:8])
    coef = coarse_solve(inverse, sums)
    scalars_o[...] = scalar_rows([alpha, energy, total_of(sums * coef)])
    column_tables(coef, codes, scatter, columns)
    spread = Spread(columns, patterns)
    factor = jnp.broadcast_to(alpha, (8, 128))

    def chunk(c, total):
        added = spread.at(c)
        fields = [forcing[0, c], forcing[1, c], end_f[c]]
        for r in range(3):
            residual = fields[r] - factor * image[r, c]
            smooth = jacobi[r, c] * residual
            z_pad[r, c + 1] = smooth + added[r]
            if r < 2:
                total = total + residual * smooth
        return total

    def step(k, total):
        for j in range(ROWS):
            total = chunk(k * ROWS + j, total)
        return total

    smooth_total = lax.fori_loop(0, chunks // ROWS, step, jnp.zeros((8, 128), F32))
    faces = (chooser(east.at[0], east.at[1]), chooser(north.at[0], north.at[1], end_n), chooser(center.at[0], center.at[1]))
    image_total = apply_operator(z_pad, faces, 2, image_o)
    smooth_row, image_row = [x + pltpu.roll(x, TILE, 1) for x in (smooth_total, image_total)]
    packed = jnp.where(iota((8, 128), 1) < TILE, smooth_row, image_row)
    sums_o[...] = jnp.sum(packed, axis=0, keepdims=True)


def pair_kernel(mine, mates, out):
    out[...] = jnp.broadcast_to((mine[...] + mates[...])[None], out.shape)


def last_kernel(parts, scalars, forcing, z_first, image_first, z_second, image_second, solution_o, residual_o,
                solution_v, residual_v, out_sems):
    chunks = forcing.shape[1]
    saves = Loads([(solution_v, solution_o), (residual_v, residual_o)], out_sems, chunks)
    row = jnp.sum(parts[...], axis=0)
    left = iota(row.shape, 1) < TILE
    alpha, energy = scalars[0:1, 0:1], scalars[1:2, 0:1]
    energy_next = jnp.sum(jnp.where(left, row, 0.0), axis=1, keepdims=True) + scalars[2:3, 0:1]
    beta = energy_next / energy
    alpha_next = energy_next / (jnp.sum(jnp.where(left, 0.0, row), axis=1, keepdims=True) - beta * energy_next / alpha)
    alpha, beta, alpha_next = [x.reshape(1, 1, 1) for x in (alpha, beta, alpha_next)]
    per_group = chunks // GROUPS // PIECE

    def step(k, carry):
        c = pl.multiple_of(k * PIECE, PIECE)
        part, shifted = pl.ds(c, PIECE), pl.ds(c + 1, PIECE)
        for r in range(2):
            z, image = z_first[r, shifted], image_first[r, part]
            solution_v[r, part] = alpha * z + alpha_next * (z_second[r, shifted] + beta * z)
            residual_v[r, part] = (forcing[r, part] - alpha * image) - alpha_next * (image_second[r, part] + beta * image)

        @pl.when(lax.rem(k, per_group) == per_group - 1)
        def _():
            for i in range(2):
                saves.copy(i, lax.div(k, per_group)).start()

        return carry

    lax.fori_loop(0, chunks // PIECE, step, 0)
    for group in range(GROUPS):
        saves.wait(group)


def body(forcing, east, north, storage, coarse_inverse, membership, land):
    rows, width = forcing.shape
    chunks = width // 128
    tile_rows = membership.shape[0]
    total_rows = tile_rows * TILE
    index = lax.axis_index(GY)
    start = index * rows
    info = jnp.stack([
        start % TILE // 8, index % 2, start // TILE,
        jnp.where(start + rows < total_rows, (start + rows) // TILE, -1), jnp.where(start > 0, (start - 1) // TILE, -1),
    ])
    inverse = jnp.transpose(coarse_inverse, (1, 2, 0))

    def blocked(x):
        return x.reshape(2, 8, chunks, 128).transpose(0, 2, 1, 3)

    forcing, east, north, storage = [blocked(x) for x in (forcing, east, north, storage)]
    devices = lax.axis_size(GY)
    mates = [(i, i ^ 1) for i in range(devices)]
    others = [(i, j) for i in range(devices) if (j := ((i + 1) ^ 1) - 1) in range(devices)]
    inner, outer = lax.axis_size(GY[1]) * lax.axis_size(GY[2]), lax.axis_size(GY[0])

    def call(kernel, outs, *args, scratch=()):
        places, kept_in = {"S": pltpu.SMEM, "H": pltpu.HBM}, {"V": pltpu.VMEM, "H": pltpu.HBM}
        kinds, values = [], []
        for kind, items in args:
            for x in items:
                kinds.append(kind)
                space = kept_in.get(kind)
                values.append(pltpu.with_memory_space_constraint(x, space) if space is not None else x)
        return pl.pallas_call(
            kernel,
            out_shape=[kept_in[k](s, d) if k in kept_in else jax.ShapeDtypeStruct(s, d) for k, s, d in outs],
            in_specs=[pl.BlockSpec(memory_space=places.get(k, pltpu.VMEM)) for k in kinds],
            out_specs=[pl.BlockSpec(memory_space=places.get(k, pltpu.VMEM)) for k, _, _ in outs],
            scratch_shapes=list(scratch),
            compiler_params=pltpu.CompilerParams(vmem_limit_bytes=VMEM_LIMIT),
        )(*values)

    def everywhere(copies):
        near = lax.all_to_all(copies, GY[1:], 0, 0)
        (copies,) = call(sum_kernel, [("", (outer,) + near.shape[1:], F32)], ("", [near]))
        return lax.all_to_all(copies, GY[0], 0, 0)

    own_shape, all_shape, end_shape = (2, chunks, 8, 128), (3, chunks, 8, 128), (chunks, 8, 128)
    halo, pad_shape = (6, chunks, 1, 128), (3, chunks + 2, 8, 128)
    own_v = pltpu.VMEM(own_shape, F32)
    codes_v, columns = pltpu.VMEM((3, chunks, 128), F32), pltpu.VMEM((3, ORDER, chunks, 128), F32)

    def dma(*shape):
        return pltpu.SemaphoreType.DMA(shape)

    sums, codes, gather, scatter, lanes, patterns = call(
        moments_kernel,
        [("", (inner, 8, 128), F32), ("V", (8, membership.shape[1]), F32), ("V", (64, 128), BF16), ("V", (128, 128), BF16),
         ("V", (2, 32, 128), F32), ("V", (3, ORDER, 8, 128), F32)],
        ("S", [info]), ("H", [forcing, membership, land, *[jnp.asarray(x) for x in tables()]]),
        scratch=(own_v, codes_v, pltpu.VMEM(membership.shape, I32), pltpu.VMEM(land.shape, I32), dma(1, GROUPS), dma(7)),
    )
    parts = everywhere(sums)
    east, north, center, mate, other = call(
        faces_kernel,
        [("V", (2, chunks + 1, 8, 128), F32)] + [("H", own_shape, F32)] * 2 + [("V", halo, F32)] * 2,
        ("S", [info]), ("V", [codes]), ("H", [forcing, east, north, storage]),
        scratch=(own_v, own_v, codes_v) + (own_v,) * 4 + (dma(4, GROUPS), dma(2, GROUPS)),
    )
    mate = lax.ppermute(mate, GY, mates)
    other = lax.ppermute(other, GY, others)
    field, north, center, z_first, image_first, sums, kept, jacobi, end_f, end_n = call(
        second_kernel,
        [("V", own_shape, F32)] * 3 + [("V", pad_shape, F32), ("V", all_shape, F32), ("", (inner, 16, 128), F32), ("V", (16, 128), F32),
         ("V", all_shape, F32), ("V", end_shape, F32), ("V", end_shape, F32)],
        ("S", [info]), ("", [parts]), ("H", [forcing, north, center]),
        ("V", [mate, other, inverse, codes, gather, scatter, lanes, patterns, east]),
        scratch=(codes_v, pltpu.VMEM((chunks + 1, 8, 128), F32), pltpu.VMEM(end_shape, F32), columns, dma(3, GROUPS)),
    )
    parts = everywhere(sums)
    z_second, image_second, sums, scalars = call(
        third_kernel,
        [("V", pad_shape, F32), ("V", own_shape, F32), ("", (1, 128), F32), ("V", (8, 128), F32)],
        ("", [parts]),
        ("V", [kept, inverse, field, image_first, codes, scatter, patterns, east, north, center, jacobi, end_f, end_n]),
        scratch=(codes_v, columns),
    )
    chips = lax.axis_size(GY[:2])
    swapped = lax.ppermute(sums, GY[2], [(0, 1), (1, 0)])
    (sums,) = call(pair_kernel, [("", (chips, 1, 128), F32)], ("", [sums, swapped]))
    parts = lax.all_to_all(sums, GY[:2], 0, 0)
    answer = call(
        last_kernel,
        [("H", own_shape, F32)] * 2,
        ("", [parts]), ("V", [scalars, field, z_first, image_first, z_second, image_second]),
        scratch=(own_v,) * 2 + (dma(2, GROUPS),),
    )
    return tuple(x.transpose(0, 2, 1, 3).reshape(rows, width) for x in answer)


def solution(mesh):
    finer = Mesh(mesh.devices.reshape(mesh.shape["ens"], 8, 8, 2), ("ens", "gy_0", "gy_1", "gy_2"))
    return jax.shard_map(
        body,
        mesh=finer,
        in_specs=(P(ENS_GY, None), P(GY, None), P(GY, None), P(GY, None), P(), P(), P()),
        out_specs=(P(ENS_GY, None), P(ENS_GY, None)),
        check_vma=False,
    )
```

```python
import jax
import jax.numpy as jnp
import numpy as np
from jax import lax
from jax.experimental import pallas as pl
from jax.experimental.pallas import tpu as pltpu
from jax.sharding import Mesh
from jax.sharding import PartitionSpec as P


TILE = 64
ORDER = 4
GY = ("gy_0", "gy_1", "gy_2")
ENS_GY = ("ens", "gy_0", "gy_1", "gy_2")
F32, BF16, I32 = jnp.float32, jnp.bfloat16, jnp.int32
ROWS = 8
PIECE = 8
BLOCK = 32
GROUPS = 4
VMEM_LIMIT = 24 * 2**20


def tables():
    degree = np.arange(ORDER)[:, None]
    mode = np.cos(np.pi * degree * (np.arange(TILE)[None, :] + 0.5) / TILE)
    p_of = np.tile(np.repeat(np.arange(ORDER), ORDER), 2)
    q_of = np.tile(np.arange(ORDER), 2 * ORDER)
    half = np.repeat(np.arange(2), ORDER * ORDER)
    lane = np.arange(128)
    cols = (mode[q_of][:, lane % TILE] * (half[:, None] == lane[None, :] // TILE)).astype(np.float32)
    high = cols.astype(BF16)
    low = (cols - high.astype(np.float32)).astype(BF16)
    gather = np.concatenate([high, low], axis=0)
    scatter = np.concatenate([high, high, low, np.zeros_like(low)], axis=0)
    rows = mode[p_of].reshape(32, 8, 8).transpose(1, 0, 2).astype(np.float32)
    row_lanes = np.tile(rows, (1, 1, 16))
    row_subs = np.broadcast_to(mode.reshape(ORDER, 8, 8, 1).transpose(1, 0, 2, 3), (8, ORDER, 8, 128)).astype(np.float32)
    ends = np.zeros((TILE // 16, ORDER, 8, 128), np.float32)
    for k in range(TILE // 16):
        ends[k, :, :4] = row_subs[(2 * k + 2) % 8, :, :4]
        ends[k, :, 4:] = row_subs[(2 * k - 1) % 8, :, 4:]
    return gather, scatter, row_lanes, row_subs, ends


def iota(shape, dim):
    return lax.broadcasted_iota(I32, shape, dim)


def onehot(codes):
    return jnp.where(codes == (iota(codes.shape, 1) % TILE).astype(F32), 1.0, 0.0).astype(BF16)


def spread_row(ref, row):
    return jnp.broadcast_to(ref[pl.ds(row, 1)], (8, 128))


def dot_nt(a, b):
    return lax.dot_general(a, b, (((1,), (1,)), ((), ())), preferred_element_type=F32)


def dot_nn(a, b):
    return lax.dot_general(a, b, (((1,), (0,)), ((), ())), preferred_element_type=F32)


def split(x):
    high = x.astype(BF16)
    return high, (x - high.astype(F32)).astype(BF16)


def expand(codes_small, out):
    chunks, tiles = out.shape[1], codes_small.shape[1]
    mine = iota((chunks, tiles), 1) // 2 == iota((chunks, tiles), 0)
    halves = jnp.where(iota((tiles, 128), 0) % 2 == iota((tiles, 128), 1) // TILE, 1.0, 0.0).astype(BF16)
    for k in range(3):
        out[k] = dot_nn(jnp.where(mine, codes_small[k : k + 1], 0.0).astype(BF16), halves)


def moments(field, codes, gather, lanes, ready=None):
    wide = [jnp.concatenate([lanes[r]] * (BLOCK * 8 // 128), axis=1) for r in range(2)]

    def step(k, total):
        first = pl.multiple_of(k * BLOCK, BLOCK)
        if ready is not None:
            ready(k)
        lifted = jnp.zeros((32, BLOCK * 8), F32)
        for r in range(2):
            high, low = split(field[r, pl.ds(first, BLOCK)].reshape(BLOCK * 8, 128))
            both = dot_nt(gather[...], high)
            lifted = lifted + wide[r] * (both[:32] + both[32:] + dot_nt(gather[0:32], low))
        own = onehot(jnp.concatenate([spread_row(codes.at[0], first + j) for j in range(BLOCK)], axis=0))
        parts = dot_nn(jnp.concatenate(split(lifted), axis=0), own)
        return total + parts[:32] + parts[32:]

    total = lax.fori_loop(0, codes.shape[1] // BLOCK, step, jnp.zeros((32, 128), F32))
    sums = total[:16] + pltpu.roll(total[16:], TILE, 1)
    return jnp.where(iota((8, 128), 1) < TILE, sums[:8], pltpu.roll(sums[8:], TILE, 1))


def unpack(tile):
    return jnp.concatenate([tile, pltpu.roll(tile, TILE, 1)], axis=0)[:, :TILE]


def coarse_solve(inverse, sums):
    coef = jnp.zeros_like(sums)
    for j in range(sums.shape[0]):
        coef = coef + inverse[j] * sums[j : j + 1]
    return coef


def total_of(x):
    return jnp.sum(jnp.sum(x, axis=1, keepdims=True), axis=0, keepdims=True)


def column_tables(coef, codes, scatter, out):
    zero = jnp.zeros_like(coef)
    rows = [jnp.concatenate([coef, zero], axis=1), jnp.concatenate([zero, coef], axis=1)]
    high, low = split(jnp.concatenate(rows * 4, axis=0))
    for row in range(3):
        own = onehot(codes[row])
        per_tile = dot_nt(own, high) + dot_nt(own, low)
        lane = iota(per_tile.shape, 1)
        rounded = per_tile.astype(BF16).astype(F32)
        pieces = jnp.where(lane // 32 == 1, per_tile - rounded, rounded)
        split_p = [jnp.where(lane // ORDER % ORDER == p, pieces, 0.0).astype(BF16) for p in range(ORDER)]
        columns = dot_nn(jnp.concatenate(split_p, axis=0), scatter[...])
        for p in range(ORDER):
            out[row, p] = columns[p * codes.shape[1] : (p + 1) * codes.shape[1]]


def two_sums(left, right):
    left, right = [x + pltpu.roll(x, TILE, 1) for x in (left, right)]
    return jnp.sum(jnp.where(iota((8, 128), 1) < TILE, left, right), axis=0, keepdims=True)


def sums_of(row):
    left = iota(row.shape, 1) < TILE
    return [jnp.sum(jnp.where(x, row, 0.0), axis=1, keepdims=True) for x in (left, jnp.logical_not(left))]


def scalar_rows(values):
    tile = jnp.zeros((8, 128), F32)
    for k, value in enumerate(values):
        tile = jnp.where(iota((8, 128), 0) == k, value, tile)
    return tile


class Loads:
    def __init__(self, pairs, sems, chunks):
        self.pairs, self.sems, self.size = pairs, sems, chunks // GROUPS

    def copy(self, i, group):
        source, target = self.pairs[i]
        part = pl.ds(pl.multiple_of(group * self.size, self.size), self.size)
        return pltpu.make_async_copy(source.at[:, part], target.at[:, part], self.sems.at[i, group])

    def start(self, groups=range(GROUPS)):
        for group in groups:
            for i in range(len(self.pairs)):
                self.copy(i, group).start()

    def wait(self, group):
        for i in range(len(self.pairs)):
            self.copy(i, group).wait()


def moments_kernel(info, forcing, membership, land, gather, scatter, row_lanes, row_subs, ends,
                   sums_o, codes_o, gather_o, scatter_o, lanes_o, patterns_o, field, codes, member_in, land_in, sems, small):
    chunks = forcing.shape[1]
    block = info[0]
    pairs = [(membership, member_in), (land, land_in), (gather, gather_o), (row_lanes.at[pl.ds(block, 2)], lanes_o),
             (scatter, scatter_o), (row_subs.at[pl.ds(block, 2)], patterns_o.at[0:2]), (ends.at[lax.div(block, 2)], patterns_o.at[2])]
    copies = [pltpu.make_async_copy(x, y, small.at[i]) for i, (x, y) in enumerate(pairs)]
    for copy in copies:
        copy.start()
    loads = Loads([(forcing, field)], sems, chunks)
    loads.start()
    for copy in copies:
        copy.wait()
    for k in range(3):
        row = pl.ds(jnp.maximum(info[2 + k], 0), 1)
        dry = (land_in[row] == 1) | (info[2 + k] < 0)
        codes_o[k : k + 1] = jnp.where(dry, TILE, member_in[row]).astype(F32)
    expand(codes_o, codes)
    tile = moments(field, codes, gather_o, lanes_o, loads.wait)
    sums_o[...] = tile


def faces_kernel(info, codes_small, forcing, east, north, storage, east_o, north_h, center_h, mate_o, other_o,
                 north_o, center_o, codes, f_in, e_in, n_in, s_in, sems, out_sems):
    chunks = forcing.shape[1]
    loads = Loads([(east, e_in), (north, n_in), (storage, s_in), (forcing, f_in)], sems, chunks)
    loads.start((3, 0, 1, 2))
    saves = Loads([(north_o, north_h), (center_o, center_h)], out_sems, chunks)
    expand(codes_small, codes)
    lane, sub = iota((8, 128), 1), iota((8, 128), 0)
    odd = info[1] == 1

    def rolled(x):
        return pltpu.roll(x, 1, 1)

    def after_of(row):
        code = spread_row(codes.at[0], row)
        return code, pltpu.roll(code, 127, 1)

    def east_of(c, here, turned, turned_next):
        mask = (here < TILE) & (jnp.where(lane == 127, turned_next, turned) < TILE)
        return [jnp.where(mask, e_in[r, c], 0.0) for r in range(2)]

    first_code, first_turned = after_of(0)
    loads.wait(3)
    last = east_of(chunks - 1, *after_of(chunks - 1), first_turned)
    for r in range(2):
        east_o[r, 0] = last[r]

    def chunk(k, j, carry):
        west_before, here, turned = carry
        c = k * ROWS + j
        ahead = k * ROWS + j + 1 if j + 1 < ROWS else lax.rem(k * ROWS + ROWS, chunks)
        coming, coming_turned = after_of(ahead)
        face = east_of(c, here, turned, coming_turned)
        wet = here < TILE
        open_north = wet & ((sub < 7) | (spread_row(codes.at[1], c) < TILE))
        west_next = [rolled(x) for x in face]
        west = [jnp.where(lane == 0, west_before[r], west_next[r]) for r in range(2)]
        norths = [jnp.where(wet, n_in[0, c], 0.0), jnp.where(open_north, n_in[1, c], 0.0)]
        shifted = [pltpu.roll(x, 1, 0) for x in norths]
        south = [jnp.where(sub == 0, 0.0, shifted[0]), jnp.where(sub == 0, shifted[0], shifted[1])]
        fields, centers = [f_in[0, c], f_in[1, c]], []
        for r in range(2):
            center = jnp.where(wet, s_in[r, c], 1.0) + face[r] + west[r] + norths[r] + south[r]
            east_o[r, c + 1] = face[r]
            north_o[r, c] = norths[r]
            center_o[r, c] = center
            centers.append(center)
        smooth = jnp.where(sub < 4, fields[0], fields[1]) / jnp.where(sub < 4, centers[0], centers[1])
        first = [x[0][0:1] for x in (fields, centers, face, norths)] + [smooth[1:2]] * 2
        final = [x[1][7:8] for x in (fields, centers, face, norths)] + [smooth[6:7], norths[1][6:7]]
        for j in range(6):
            mate_o[j, c] = jnp.where(odd, first[j], final[j])
            other_o[j, c] = jnp.where(odd, final[j], first[j])
        return west_next, coming, coming_turned

    size = chunks // GROUPS // ROWS

    def step(k, carry):
        @pl.when((lax.rem(k, size) == 0) & (k < (GROUPS - 1) * size))
        def _():
            loads.wait(lax.div(k, size))

        for j in range(ROWS):
            carry = chunk(k, j, carry)

        @pl.when(lax.rem(k, size) == size - 1)
        def _():
            for i in range(2):
                saves.copy(i, lax.div(k, size)).start()

        return carry

    lax.fori_loop(0, chunks // ROWS, step, ([rolled(x) for x in last], first_code, first_turned))
    for group in range(GROUPS):
        saves.wait(group)


def apply_operator(z_pad, faces, blocks, out):
    east, north, center = faces
    chunks = z_pad.shape[1] - 2
    z_pad[:, 0] = z_pad[:, chunks]
    z_pad[:, chunks + 1] = z_pad[:, 1]
    n = PIECE
    sub, lane = iota((n, 8, 128), 1), iota((n, 8, 128), 2)

    def step(k, total):
        c = pl.multiple_of(k * n, n)
        own = [z_pad[r, pl.ds(c + 1, n)] for r in range(3)]
        faced = [north(r, pl.ds(c, n)) for r in range(3)]
        below = [pltpu.roll(faced[r] * own[r], 1, 1) for r in range(3)]
        above = [pltpu.roll(own[r], 7, 1) for r in range(3)]
        for r in range(blocks):
            ahead = pltpu.roll(z_pad[r, pl.ds(c + 1, n + 1)], 127, 2)
            ahead = jnp.where(lane == 127, ahead[1:], ahead[:-1])
            face = east(r, pl.ds(c, n + 1))
            behind = pltpu.roll(face * z_pad[r, pl.ds(c, n + 1)], 1, 2)
            behind = jnp.where(lane == 0, behind[:-1], behind[1:])
            image = (center(r, pl.ds(c, n)) * own[r] - face[1:] * ahead - behind
                     - faced[r] * jnp.where(sub == 7, above[(r + 1) % 3], above[r])
                     - jnp.where(sub == 0, below[(r + 2) % 3], below[r]))
            out[r, pl.ds(c, n)] = image
            if r < 2:
                total = total + jnp.sum(own[r] * image, axis=0)
        return total

    return lax.fori_loop(0, chunks // n, step, jnp.zeros((8, 128), F32))


def chooser(*views):
    return lambda r, part: views[r][part]


class Spread:
    def __init__(self, columns, patterns):
        self.columns = columns
        self.patterns = [[patterns[r, p] for p in range(ORDER)] for r in range(3)]
        self.sub = iota((8, 128), 0)

    def at(self, c):
        def row(k, p):
            return spread_row(self.columns.at[k, p], c)

        own = [row(0, p) for p in range(ORDER)]
        end = [jnp.where(self.sub < 4, row(1, p), row(2, p)) for p in range(ORDER)]
        return [sum(self.patterns[r][p] * x[p] for p in range(ORDER)) for r, x in enumerate((own, own, end))]


def second_kernel(info, parts, forcing, north_h, center_h, mate, other, inverse, codes_small, gather, scatter, lanes, patterns, east,
                  field, north, center, z_pad, image_o, sums_o, kept_o, jacobi_o, end_f, end_n,
                  codes, end_e, end_c, columns, sems):
    chunks = forcing.shape[1]
    loads = Loads([(forcing, field), (north_h, north), (center_h, center)], sems, chunks)
    loads.start()
    expand(codes_small, codes)
    tile = jnp.sum(parts[...], axis=0)
    sums = unpack(tile)
    coef = coarse_solve(inverse, sums)
    kept_o[0:8] = tile
    kept_o[8:16] = jnp.broadcast_to(total_of(sums * coef), (8, 128))
    column_tables(coef, codes, scatter, columns)
    spread = Spread(columns, patterns)
    sub = iota((8, 128), 0)
    after = jnp.logical_xor(sub < 4, info[1] == 1)

    def chunk(c, total):
        added = spread.at(c)

        def rows(j):
            return jnp.where(after, mate[j, c], other[j, c])

        faced = jnp.where(sub == 6, rows(5), rows(3))
        far = rows(0)
        beyond = rows(1) + jnp.where(sub == 0, pltpu.roll(north[1, c], 1, 0), 0.0)
        first = center[0, c] + jnp.where(sub == 0, pltpu.roll(faced, 1, 0), 0.0)
        both = jnp.where(sub == 3, pltpu.roll(first, 3, 0), jnp.where(beyond == 0.0, 1.0, beyond))
        inverted = 1.0 / both
        own = [jnp.where(sub == 0, pltpu.roll(inverted, 5, 0), 1.0 / first), 1.0 / center[1, c]]
        end_f[c] = far
        end_n[c] = faced
        end_e[c + 1] = rows(2)
        end_c[c] = both
        center[0, c] = first
        jacobi_o[0, c] = own[0]
        jacobi_o[1, c] = own[1]
        jacobi_o[2, c] = inverted
        smooth = [field[0, c] * own[0], field[1, c] * own[1],
                  jnp.where((sub == 1) | (sub == 6), rows(4), far * inverted)]
        for r in range(3):
            z_pad[r, c + 1] = smooth[r] + added[r]
        return total + (field[0, c] * smooth[0] + field[1, c] * smooth[1])

    size = chunks // GROUPS // ROWS

    def step(k, total):
        @pl.when(lax.rem(k, size) == 0)
        def _():
            loads.wait(lax.div(k, size))

        for j in range(ROWS):
            total = chunk(k * ROWS + j, total)
        return total

    smooth_total = lax.fori_loop(0, chunks // ROWS, step, jnp.zeros((8, 128), F32))
    end_e[0] = end_e[chunks]
    faces = (chooser(east.at[0], east.at[1], end_e), chooser(north.at[0], north.at[1], end_n),
             chooser(center.at[0], center.at[1], end_c))
    image_total = apply_operator(z_pad, faces, 3, image_o)
    tile = moments(image_o, codes, gather, lanes)
    for k in range(8):
        sums_o[k] = tile[k : k + 1]
    sums_o[8] = two_sums(smooth_total, image_total)


def third_kernel(parts, kept, inverse, forcing, image, codes_small, scatter, patterns, east, north, center,
                 jacobi, end_f, end_n, z_pad, image_o, sums_o, scalars_o, codes, columns, tile):
    chunks = forcing.shape[1]
    expand(codes_small, codes)
    rows = jnp.sum(parts[...], axis=0)
    for k in range(9):
        tile[k : k + 1] = rows[k]
    energy, image_energy = sums_of(tile[8:9])
    energy = energy + kept[8:9, 0:1]
    alpha = energy / image_energy
    sums = unpack(kept[0:8] - alpha * tile[0:8])
    coef = coarse_solve(inverse, sums)
    scalars_o[...] = scalar_rows([alpha, energy, total_of(sums * coef)])
    column_tables(coef, codes, scatter, columns)
    spread = Spread(columns, patterns)
    factor = jnp.broadcast_to(alpha, (8, 128))

    def chunk(c, total):
        added = spread.at(c)
        fields = [forcing[0, c], forcing[1, c], end_f[c]]
        for r in range(3):
            residual = fields[r] - factor * image[r, c]
            smooth = jacobi[r, c] * residual
            z_pad[r, c + 1] = smooth + added[r]
            if r < 2:
                total = total + residual * smooth
        return total

    def step(k, total):
        for j in range(ROWS):
            total = chunk(k * ROWS + j, total)
        return total

    smooth_total = lax.fori_loop(0, chunks // ROWS, step, jnp.zeros((8, 128), F32))
    faces = (chooser(east.at[0], east.at[1]), chooser(north.at[0], north.at[1], end_n), chooser(center.at[0], center.at[1]))
    image_total = apply_operator(z_pad, faces, 2, image_o)
    sums_o[...] = two_sums(smooth_total, image_total)


def pair_kernel(mine, mates, out):
    out[...] = jnp.broadcast_to((mine[...] + mates[...])[None], out.shape)


def last_kernel(parts, scalars, forcing, z_first, image_first, z_second, image_second, solution_o, residual_o,
                solution_v, residual_v, out_sems):
    chunks = forcing.shape[1]
    saves = Loads([(solution_v, solution_o), (residual_v, residual_o)], out_sems, chunks)
    energy_next, image_energy = sums_of(jnp.sum(parts[...], axis=0))
    alpha, energy = scalars[0:1, 0:1], scalars[1:2, 0:1]
    energy_next = energy_next + scalars[2:3, 0:1]
    beta = energy_next / energy
    alpha_next = energy_next / (image_energy - beta * energy_next / alpha)
    alpha, beta, alpha_next = [x.reshape(1, 1, 1) for x in (alpha, beta, alpha_next)]
    per_group = chunks // GROUPS // PIECE

    def step(k, carry):
        c = pl.multiple_of(k * PIECE, PIECE)
        part, shifted = pl.ds(c, PIECE), pl.ds(c + 1, PIECE)
        for r in range(2):
            z, image = z_first[r, shifted], image_first[r, part]
            solution_v[r, part] = alpha * z + alpha_next * (z_second[r, shifted] + beta * z)
            residual_v[r, part] = (forcing[r, part] - alpha * image) - alpha_next * (image_second[r, part] + beta * image)

        @pl.when(lax.rem(k, per_group) == per_group - 1)
        def _():
            for i in range(2):
                saves.copy(i, lax.div(k, per_group)).start()

        return carry

    lax.fori_loop(0, chunks // PIECE, step, 0)
    for group in range(GROUPS):
        saves.wait(group)


def body(forcing, east, north, storage, coarse_inverse, membership, land):
    rows, width = forcing.shape
    chunks = width // 128
    tile_rows = membership.shape[0]
    total_rows = tile_rows * TILE
    index = lax.axis_index(GY)
    start = index * rows
    info = jnp.stack([
        start % TILE // 8, index % 2, start // TILE,
        jnp.where(start + rows < total_rows, (start + rows) // TILE, -1), jnp.where(start > 0, (start - 1) // TILE, -1),
    ])
    inverse = jnp.transpose(coarse_inverse, (1, 2, 0))

    def blocked(x):
        return x.reshape(2, 8, chunks, 128).transpose(0, 2, 1, 3)

    forcing, east, north, storage = [blocked(x) for x in (forcing, east, north, storage)]
    devices = lax.axis_size(GY)
    mates = [(i, i ^ 1) for i in range(devices)]
    others = [(i, j) for i in range(devices) if (j := ((i + 1) ^ 1) - 1) in range(devices)]

    def call(kernel, outs, *args, scratch=()):
        places, kept_in = {"S": pltpu.SMEM, "H": pltpu.HBM}, {"V": pltpu.VMEM, "H": pltpu.HBM}
        kinds, values = [], []
        for kind, items in args:
            for x in items:
                kinds.append(kind)
                space = kept_in.get(kind)
                values.append(pltpu.with_memory_space_constraint(x, space) if space is not None else x)
        return pl.pallas_call(
            kernel,
            out_shape=[kept_in[k](s, d) if k in kept_in else jax.ShapeDtypeStruct(s, d) for k, s, d in outs],
            in_specs=[pl.BlockSpec(memory_space=places.get(k, pltpu.VMEM)) for k in kinds],
            out_specs=[pl.BlockSpec(memory_space=places.get(k, pltpu.VMEM)) for k, _, _ in outs],
            scratch_shapes=list(scratch),
            compiler_params=pltpu.CompilerParams(vmem_limit_bytes=VMEM_LIMIT),
        )(*values)

    def everywhere(mine):
        mates = lax.ppermute(mine, GY[2], [(0, 1), (1, 0)])
        (copies,) = call(pair_kernel, [("V", (lax.axis_size(GY[:2]),) + mine.shape, F32)], ("", [mine, mates]))
        return lax.all_to_all(copies, GY[:2], 0, 0)

    own_shape, all_shape, end_shape = (2, chunks, 8, 128), (3, chunks, 8, 128), (chunks, 8, 128)
    halo, pad_shape = (6, chunks, 1, 128), (3, chunks + 2, 8, 128)
    own_v = pltpu.VMEM(own_shape, F32)
    codes_v, columns = pltpu.VMEM((3, chunks, 128), F32), pltpu.VMEM((3, ORDER, chunks, 128), F32)

    def dma(*shape):
        return pltpu.SemaphoreType.DMA(shape)

    sums, codes, gather, scatter, lanes, patterns = call(
        moments_kernel,
        [("", (8, 128), F32), ("V", (8, membership.shape[1]), F32), ("V", (64, 128), BF16), ("V", (128, 128), BF16),
         ("V", (2, 32, 128), F32), ("V", (3, ORDER, 8, 128), F32)],
        ("S", [info]), ("H", [forcing, membership, land, *[jnp.asarray(x) for x in tables()]]),
        scratch=(own_v, codes_v, pltpu.VMEM(membership.shape, I32), pltpu.VMEM(land.shape, I32), dma(1, GROUPS), dma(7)),
    )
    parts = everywhere(sums)
    east, north, center, mate, other = call(
        faces_kernel,
        [("V", (2, chunks + 1, 8, 128), F32)] + [("H", own_shape, F32)] * 2 + [("V", halo, F32)] * 2,
        ("S", [info]), ("V", [codes]), ("H", [forcing, east, north, storage]),
        scratch=(own_v, own_v, codes_v) + (own_v,) * 4 + (dma(4, GROUPS), dma(2, GROUPS)),
    )
    mate = lax.ppermute(mate, GY, mates)
    other = lax.ppermute(other, GY, others)
    field, north, center, z_first, image_first, sums, kept, jacobi, end_f, end_n = call(
        second_kernel,
        [("V", own_shape, F32)] * 3 + [("V", pad_shape, F32), ("V", all_shape, F32), ("", (9, 1, 128), F32), ("V", (16, 128), F32),
         ("V", all_shape, F32), ("V", end_shape, F32), ("V", end_shape, F32)],
        ("S", [info]), ("", [parts]), ("H", [forcing, north, center]),
        ("V", [mate, other, inverse, codes, gather, scatter, lanes, patterns, east]),
        scratch=(codes_v, pltpu.VMEM((chunks + 1, 8, 128), F32), pltpu.VMEM(end_shape, F32), columns, dma(3, GROUPS)),
    )
    parts = everywhere(sums)
    z_second, image_second, sums, scalars = call(
        third_kernel,
        [("V", pad_shape, F32), ("V", own_shape, F32), ("", (1, 128), F32), ("V", (8, 128), F32)],
        ("", [parts]),
        ("V", [kept, inverse, field, image_first, codes, scatter, patterns, east, north, center, jacobi, end_f, end_n]),
        scratch=(codes_v, columns, pltpu.VMEM((16, 128), F32)),
    )
    parts = everywhere(sums)
    answer = call(
        last_kernel,
        [("H", own_shape, F32)] * 2,
        ("", [parts]), ("V", [scalars, field, z_first, image_first, z_second, image_second]),
        scratch=(own_v,) * 2 + (dma(2, GROUPS),),
    )
    return tuple(x.transpose(0, 2, 1, 3).reshape(rows, width) for x in answer)


def solution(mesh):
    finer = Mesh(mesh.devices.reshape(mesh.shape["ens"], 8, 8, 2), ("ens", "gy_0", "gy_1", "gy_2"))
    return jax.shard_map(
        body,
        mesh=finer,
        in_specs=(P(ENS_GY, None), P(GY, None), P(GY, None), P(GY, None), P(), P(), P()),
        out_specs=(P(ENS_GY, None), P(ENS_GY, None)),
        check_vma=False,
    )
```

```python
import jax
import jax.numpy as jnp
import numpy as np
from jax import lax
from jax.experimental import pallas as pl
from jax.experimental.pallas import tpu as pltpu
from jax.sharding import Mesh
from jax.sharding import PartitionSpec as P


TILE = 64
ORDER = 4
GY = ("gy_0", "gy_1", "gy_2")
ENS_GY = ("ens", "gy_0", "gy_1", "gy_2")
F32, BF16, I32 = jnp.float32, jnp.bfloat16, jnp.int32
ROWS = 32
PIECE = 32
BLOCK = 32
GROUPS = 4
HALVES = 2
VMEM_LIMIT = 24 * 2**20


def tables():
    degree = np.arange(ORDER)[:, None]
    mode = np.cos(np.pi * degree * (np.arange(TILE)[None, :] + 0.5) / TILE)
    p_of = np.tile(np.repeat(np.arange(ORDER), ORDER), 2)
    q_of = np.tile(np.arange(ORDER), 2 * ORDER)
    half = np.repeat(np.arange(2), ORDER * ORDER)
    lane = np.arange(128)
    cols = (mode[q_of][:, lane % TILE] * (half[:, None] == lane[None, :] // TILE)).astype(np.float32)
    high = cols.astype(BF16)
    low = (cols - high.astype(np.float32)).astype(BF16)
    gather = np.concatenate([np.concatenate([high, high], axis=1), np.concatenate([low, np.zeros_like(low)], axis=1)], axis=0)
    scatter = np.concatenate([high, high, low, np.zeros_like(low)], axis=0)
    rows = mode[p_of].reshape(32, 8, 8).transpose(1, 0, 2).astype(np.float32)
    row_lanes = np.tile(rows, (1, 1, 16))
    row_subs = np.broadcast_to(mode.reshape(ORDER, 8, 8, 1).transpose(1, 0, 2, 3), (8, ORDER, 8, 128)).astype(np.float32)
    ends = np.zeros((TILE // 16, ORDER, 8, 128), np.float32)
    for k in range(TILE // 16):
        ends[k, :, :4] = row_subs[(2 * k + 2) % 8, :, :4]
        ends[k, :, 4:] = row_subs[(2 * k - 1) % 8, :, 4:]
    return gather, scatter, row_lanes, row_subs, ends


def iota(shape, dim):
    return lax.broadcasted_iota(I32, shape, dim)


def onehot(codes):
    return jnp.where(codes == (iota(codes.shape, 1) % TILE).astype(F32), 1.0, 0.0).astype(BF16)


def spread_row(ref, row):
    return jnp.broadcast_to(ref[pl.ds(row, 1)], (8, 128))


def dot_nt(a, b):
    return lax.dot_general(a, b, (((1,), (1,)), ((), ())), preferred_element_type=F32)


def dot_nn(a, b):
    return lax.dot_general(a, b, (((1,), (0,)), ((), ())), preferred_element_type=F32)


def split(x):
    high = x.astype(BF16)
    return high, (x - high.astype(F32)).astype(BF16)


def expand(codes_small, out):
    chunks, tiles = out.shape[1], codes_small.shape[1]
    mine = iota((chunks, tiles), 1) // 2 == iota((chunks, tiles), 0)
    halves = jnp.where(iota((tiles, 128), 0) % 2 == iota((tiles, 128), 1) // TILE, 1.0, 0.0).astype(BF16)
    for k in range(3):
        out[k] = dot_nn(jnp.where(mine, codes_small[k : k + 1], 0.0).astype(BF16), halves)


def moments(field, codes, gather, lanes, loads=None):
    wide = [jnp.concatenate([lanes[r]] * (BLOCK * 8 // 128), axis=1) for r in range(2)]

    total = jnp.zeros((32, 128), F32)
    for k in range(codes.shape[1] // BLOCK):
        first = k * BLOCK
        if loads is not None and first % loads.size == 0:
            loads.wait(first // loads.size)
        lifted = jnp.zeros((32, BLOCK * 8), F32)
        for r in range(2):
            both = dot_nt(gather[...], jnp.concatenate(split(field[r, pl.ds(first, BLOCK)].reshape(BLOCK * 8, 128)), axis=1))
            lifted = lifted + wide[r] * (both[:32] + both[32:])
        own = onehot(jnp.concatenate([spread_row(codes.at[0], first + j) for j in range(BLOCK)], axis=0))
        parts = dot_nn(jnp.concatenate(split(lifted), axis=0), own)
        total = total + parts[:32] + parts[32:]
    sums = total[:16] + pltpu.roll(total[16:], TILE, 1)
    return jnp.where(iota((8, 128), 1) < TILE, sums[:8], pltpu.roll(sums[8:], TILE, 1))


def unpack(tile):
    return jnp.concatenate([tile, pltpu.roll(tile, TILE, 1)], axis=0)[:, :TILE]


def coarse_solve(inverse, sums):
    coef = jnp.zeros_like(sums)
    for j in range(sums.shape[0]):
        coef = coef + inverse[j] * sums[j : j + 1]
    return coef


def total_of(x):
    return jnp.sum(jnp.sum(x, axis=1, keepdims=True), axis=0, keepdims=True)


def column_tables(coef, codes, scatter, out):
    zero = jnp.zeros_like(coef)
    rows = [jnp.concatenate([coef, zero], axis=1), jnp.concatenate([zero, coef], axis=1)]
    high, low = split(jnp.concatenate(rows * 4, axis=0))
    for row in range(3):
        own = onehot(codes[row])
        per_tile = dot_nt(own, high) + dot_nt(own, low)
        lane = iota(per_tile.shape, 1)
        rounded = per_tile.astype(BF16).astype(F32)
        pieces = jnp.where(lane // 32 == 1, per_tile - rounded, rounded)
        split_p = [jnp.where(lane // ORDER % ORDER == p, pieces, 0.0).astype(BF16) for p in range(ORDER)]
        columns = dot_nn(jnp.concatenate(split_p, axis=0), scatter[...])
        for p in range(ORDER):
            out[row, p] = columns[p * codes.shape[1] : (p + 1) * codes.shape[1]]


def sum_kernel(parts, out):
    out[...] = jnp.broadcast_to(jnp.sum(parts[...], axis=0)[None], out.shape)


def scalar_rows(values):
    tile = jnp.zeros((8, 128), F32)
    for k, value in enumerate(values):
        tile = jnp.where(iota((8, 128), 0) == k, value, tile)
    return tile


class Loads:
    def __init__(self, pairs, sems, chunks, groups=GROUPS):
        self.pairs, self.sems, self.size, self.groups = pairs, sems, chunks // groups, groups

    def copy(self, i, group):
        source, target = self.pairs[i]
        part = pl.ds(pl.multiple_of(group * self.size, self.size), self.size)
        return pltpu.make_async_copy(source.at[:, part], target.at[:, part], self.sems.at[i, group])

    def start(self, order=None):
        for group in range(self.groups) if order is None else order:
            for i in range(len(self.pairs)):
                self.copy(i, group).start()

    def wait(self, group):
        for i in range(len(self.pairs)):
            self.copy(i, group).wait()


def moments_kernel(info, forcing, membership, land, gather, scatter, row_lanes, row_subs, ends,
                   sums_o, codes_o, gather_o, scatter_o, lanes_o, patterns_o, field, codes, member_in, land_in, sems, small):
    chunks = forcing.shape[1]
    block = info[0]
    pairs = [(membership, member_in), (land, land_in), (gather, gather_o), (row_lanes.at[pl.ds(block, 2)], lanes_o),
             (scatter, scatter_o), (row_subs.at[pl.ds(block, 2)], patterns_o.at[0:2]), (ends.at[lax.div(block, 2)], patterns_o.at[2])]
    copies = [pltpu.make_async_copy(x, y, small.at[i]) for i, (x, y) in enumerate(pairs)]
    for copy in copies:
        copy.start()
    loads = Loads([(forcing, field)], sems, chunks, HALVES)
    loads.start()
    for copy in copies:
        copy.wait()
    for k in range(3):
        row = pl.ds(jnp.maximum(info[2 + k], 0), 1)
        dry = (land_in[row] == 1) | (info[2 + k] < 0)
        codes_o[k : k + 1] = jnp.where(dry, TILE, member_in[row]).astype(F32)
    expand(codes_o, codes)
    tile = moments(field, codes, gather_o, lanes_o, loads)
    sums_o[...] = jnp.broadcast_to(tile[None], sums_o.shape)


def faces_kernel(info, codes_small, forcing, east, north, storage, east_o, north_h, center_h, mate_o, other_o,
                 north_o, center_o, codes, f_in, e_in, n_in, s_in, sems, out_sems):
    chunks = forcing.shape[1]
    loads = Loads([(east, e_in), (north, n_in), (storage, s_in), (forcing, f_in)], sems, chunks)
    loads.start((3, 0, 1, 2))
    saves = Loads([(north_o, north_h), (center_o, center_h)], out_sems, chunks)
    expand(codes_small, codes)
    lane, sub = iota((8, 128), 1), iota((8, 128), 0)
    odd = info[1] == 1

    def rolled(x):
        return pltpu.roll(x, 1, 1)

    def after_of(row):
        code = spread_row(codes.at[0], row)
        return code, pltpu.roll(code, 127, 1)

    def east_of(c, here, turned, turned_next):
        mask = (here < TILE) & (jnp.where(lane == 127, turned_next, turned) < TILE)
        return [jnp.where(mask, e_in[r, c], 0.0) for r in range(2)]

    first_code, first_turned = after_of(0)
    loads.wait(3)
    last = east_of(chunks - 1, *after_of(chunks - 1), first_turned)
    for r in range(2):
        east_o[r, 0] = last[r]

    def chunk(k, j, carry):
        west_before, here, turned = carry
        c = k * ROWS + j
        ahead = k * ROWS + j + 1 if j + 1 < ROWS else lax.rem(k * ROWS + ROWS, chunks)
        coming, coming_turned = after_of(ahead)
        face = east_of(c, here, turned, coming_turned)
        wet = here < TILE
        open_north = wet & ((sub < 7) | (spread_row(codes.at[1], c) < TILE))
        west_next = [rolled(x) for x in face]
        west = [jnp.where(lane == 0, west_before[r], west_next[r]) for r in range(2)]
        norths = [jnp.where(wet, n_in[0, c], 0.0), jnp.where(open_north, n_in[1, c], 0.0)]
        shifted = [pltpu.roll(x, 1, 0) for x in norths]
        south = [jnp.where(sub == 0, 0.0, shifted[0]), jnp.where(sub == 0, shifted[0], shifted[1])]
        fields, centers = [f_in[0, c], f_in[1, c]], []
        for r in range(2):
            center = jnp.where(wet, s_in[r, c], 1.0) + face[r] + west[r] + norths[r] + south[r]
            east_o[r, c + 1] = face[r]
            north_o[r, c] = norths[r]
            center_o[r, c] = center
            centers.append(center)
        smooth = jnp.where(sub < 4, fields[0], fields[1]) / jnp.where(sub < 4, centers[0], centers[1])
        first = [x[0][0:1] for x in (fields, centers, face, norths)] + [smooth[1:2]] * 2
        final = [x[1][7:8] for x in (fields, centers, face, norths)] + [smooth[6:7], norths[1][6:7]]
        for j in range(6):
            mate_o[j, c] = jnp.where(odd, first[j], final[j])
            other_o[j, c] = jnp.where(odd, final[j], first[j])
        return west_next, coming, coming_turned

    size = chunks // GROUPS // ROWS

    def step(k, carry):
        @pl.when((lax.rem(k, size) == 0) & (k < (GROUPS - 1) * size))
        def _():
            loads.wait(lax.div(k, size))

        for j in range(ROWS):
            carry = chunk(k, j, carry)

        @pl.when(lax.rem(k, size) == size - 1)
        def _():
            for i in range(2):
                saves.copy(i, lax.div(k, size)).start()

        return carry

    lax.fori_loop(0, chunks // ROWS, step, ([rolled(x) for x in last], first_code, first_turned))
    for group in range(GROUPS):
        saves.wait(group)


def apply_operator(z_pad, faces, blocks, out):
    east, north, center = faces
    chunks = z_pad.shape[1] - 2
    z_pad[:, 0] = z_pad[:, chunks]
    z_pad[:, chunks + 1] = z_pad[:, 1]
    n = PIECE
    sub, lane = iota((n, 8, 128), 1), iota((n, 8, 128), 2)

    def step(k, total):
        c = pl.multiple_of(k * n, n)
        own = [z_pad[r, pl.ds(c + 1, n)] for r in range(3)]
        faced = [north(r, pl.ds(c, n)) for r in range(3)]
        below = [pltpu.roll(faced[r] * own[r], 1, 1) for r in range(3)]
        above = [pltpu.roll(own[r], 7, 1) for r in range(3)]
        for r in range(blocks):
            ahead = pltpu.roll(z_pad[r, pl.ds(c + 1, n + 1)], 127, 2)
            ahead = jnp.where(lane == 127, ahead[1:], ahead[:-1])
            face = east(r, pl.ds(c, n + 1))
            behind = pltpu.roll(face * z_pad[r, pl.ds(c, n + 1)], 1, 2)
            behind = jnp.where(lane == 0, behind[:-1], behind[1:])
            image = (center(r, pl.ds(c, n)) * own[r] - face[1:] * ahead - behind
                     - faced[r] * jnp.where(sub == 7, above[(r + 1) % 3], above[r])
                     - jnp.where(sub == 0, below[(r + 2) % 3], below[r]))
            out[r, pl.ds(c, n)] = image
            if r < 2:
                total = total + jnp.sum(own[r] * image, axis=0)
        return total

    return lax.fori_loop(0, chunks // n, step, jnp.zeros((8, 128), F32))


def chooser(*views):
    return lambda r, part: views[r][part]


class Spread:
    def __init__(self, columns, patterns):
        self.columns = columns
        self.patterns = [[patterns[r, p] for p in range(ORDER)] for r in range(3)]
        self.sub = iota((8, 128), 0)

    def at(self, c):
        def row(k, p):
            return spread_row(self.columns.at[k, p], c)

        own = [row(0, p) for p in range(ORDER)]
        end = [jnp.where(self.sub < 4, row(1, p), row(2, p)) for p in range(ORDER)]
        return [sum(self.patterns[r][p] * x[p] for p in range(ORDER)) for r, x in enumerate((own, own, end))]


def second_kernel(info, parts, forcing, north_h, center_h, mate, other, inverse, codes_small, gather, scatter, lanes, patterns, east,
                  field, north, center, z_pad, image_o, sums_o, kept_o, jacobi_o, end_f, end_n,
                  codes, end_e, end_c, columns, sems):
    chunks = forcing.shape[1]
    loads = Loads([(forcing, field), (north_h, north), (center_h, center)], sems, chunks)
    loads.start()
    expand(codes_small, codes)
    tile = jnp.sum(parts[...], axis=0)
    sums = unpack(tile)
    coef = coarse_solve(inverse, sums)
    kept_o[0:8] = tile
    kept_o[8:16] = jnp.broadcast_to(total_of(sums * coef), (8, 128))
    column_tables(coef, codes, scatter, columns)
    spread = Spread(columns, patterns)
    sub = iota((8, 128), 0)
    after = jnp.logical_xor(sub < 4, info[1] == 1)

    def chunk(c, total):
        added = spread.at(c)

        def rows(j):
            return jnp.where(after, mate[j, c], other[j, c])

        faced = jnp.where(sub == 6, rows(5), rows(3))
        far = rows(0)
        beyond = rows(1) + jnp.where(sub == 0, pltpu.roll(north[1, c], 1, 0), 0.0)
        first = center[0, c] + jnp.where(sub == 0, pltpu.roll(faced, 1, 0), 0.0)
        both = jnp.where(sub == 3, pltpu.roll(first, 3, 0), jnp.where(beyond == 0.0, 1.0, beyond))
        inverted = 1.0 / both
        own = [jnp.where(sub == 0, pltpu.roll(inverted, 5, 0), 1.0 / first), 1.0 / center[1, c]]
        end_f[c] = far
        end_n[c] = faced
        end_e[c + 1] = rows(2)
        end_c[c] = both
        center[0, c] = first
        jacobi_o[0, c] = own[0]
        jacobi_o[1, c] = own[1]
        jacobi_o[2, c] = inverted
        smooth = [field[0, c] * own[0], field[1, c] * own[1],
                  jnp.where((sub == 1) | (sub == 6), rows(4), far * inverted)]
        for r in range(3):
            z_pad[r, c + 1] = smooth[r] + added[r]
        return total + (field[0, c] * smooth[0] + field[1, c] * smooth[1])

    size = chunks // GROUPS // ROWS

    def step(k, total):
        @pl.when(lax.rem(k, size) == 0)
        def _():
            loads.wait(lax.div(k, size))

        for j in range(ROWS):
            total = chunk(k * ROWS + j, total)
        return total

    smooth_total = lax.fori_loop(0, chunks // ROWS, step, jnp.zeros((8, 128), F32))
    end_e[0] = end_e[chunks]
    faces = (chooser(east.at[0], east.at[1], end_e), chooser(north.at[0], north.at[1], end_n),
             chooser(center.at[0], center.at[1], end_c))
    image_total = apply_operator(z_pad, faces, 3, image_o)
    tile = moments(image_o, codes, gather, lanes)
    scalars = scalar_rows([jnp.sum(smooth_total, axis=0, keepdims=True), jnp.sum(image_total, axis=0, keepdims=True)])
    sums_o[...] = jnp.broadcast_to(jnp.concatenate([tile, scalars], axis=0)[None], sums_o.shape)


def third_kernel(parts, kept, inverse, forcing, image, codes_small, scatter, patterns, east, north, center,
                 jacobi, end_f, end_n, z_pad, image_o, sums_o, scalars_o, codes, columns):
    chunks = forcing.shape[1]
    expand(codes_small, codes)
    tile = jnp.sum(parts[...], axis=0)
    energy = jnp.sum(tile[8:9], axis=1, keepdims=True) + kept[8:9, 0:1]
    alpha = energy / jnp.sum(tile[9:10], axis=1, keepdims=True)
    sums = unpack(kept[0:8] - alpha * tile[0:8])
    coef = coarse_solve(inverse, sums)
    scalars_o[...] = scalar_rows([alpha, energy, total_of(sums * coef)])
    column_tables(coef, codes, scatter, columns)
    spread = Spread(columns, patterns)
    factor = jnp.broadcast_to(alpha, (8, 128))

    def chunk(c, total):
        added = spread.at(c)
        fields = [forcing[0, c], forcing[1, c], end_f[c]]
        for r in range(3):
            residual = fields[r] - factor * image[r, c]
            smooth = jacobi[r, c] * residual
            z_pad[r, c + 1] = smooth + added[r]
            if r < 2:
                total = total + residual * smooth
        return total

    def step(k, total):
        for j in range(ROWS):
            total = chunk(k * ROWS + j, total)
        return total

    smooth_total = lax.fori_loop(0, chunks // ROWS, step, jnp.zeros((8, 128), F32))
    faces = (chooser(east.at[0], east.at[1]), chooser(north.at[0], north.at[1], end_n), chooser(center.at[0], center.at[1]))
    image_total = apply_operator(z_pad, faces, 2, image_o)
    smooth_row, image_row = [x + pltpu.roll(x, TILE, 1) for x in (smooth_total, image_total)]
    packed = jnp.where(iota((8, 128), 1) < TILE, smooth_row, image_row)
    sums_o[...] = jnp.sum(packed, axis=0, keepdims=True)


def pair_kernel(mine, mates, out):
    out[...] = jnp.broadcast_to((mine[...] + mates[...])[None], out.shape)


def last_kernel(parts, scalars, forcing, z_first, image_first, z_second, image_second, solution_o, residual_o,
                solution_v, residual_v, out_sems):
    chunks = forcing.shape[1]
    saves = Loads([(solution_v, solution_o), (residual_v, residual_o)], out_sems, chunks)
    row = jnp.sum(parts[...], axis=0)
    left = iota(row.shape, 1) < TILE
    alpha, energy = scalars[0:1, 0:1], scalars[1:2, 0:1]
    energy_next = jnp.sum(jnp.where(left, row, 0.0), axis=1, keepdims=True) + scalars[2:3, 0:1]
    beta = energy_next / energy
    alpha_next = energy_next / (jnp.sum(jnp.where(left, 0.0, row), axis=1, keepdims=True) - beta * energy_next / alpha)
    alpha, beta, alpha_next = [x.reshape(1, 1, 1) for x in (alpha, beta, alpha_next)]
    per_group = chunks // GROUPS // PIECE

    def step(k, carry):
        c = pl.multiple_of(k * PIECE, PIECE)
        part, shifted = pl.ds(c, PIECE), pl.ds(c + 1, PIECE)
        for r in range(2):
            z, image = z_first[r, shifted], image_first[r, part]
            solution_v[r, part] = alpha * z + alpha_next * (z_second[r, shifted] + beta * z)
            residual_v[r, part] = (forcing[r, part] - alpha * image) - alpha_next * (image_second[r, part] + beta * image)

        @pl.when(lax.rem(k, per_group) == per_group - 1)
        def _():
            for i in range(2):
                saves.copy(i, lax.div(k, per_group)).start()

        return carry

    lax.fori_loop(0, chunks // PIECE, step, 0)
    for group in range(GROUPS):
        saves.wait(group)


def body(forcing, east, north, storage, coarse_inverse, membership, land):
    rows, width = forcing.shape
    chunks = width // 128
    tile_rows = membership.shape[0]
    total_rows = tile_rows * TILE
    index = lax.axis_index(GY)
    start = index * rows
    info = jnp.stack([
        start % TILE // 8, index % 2, start // TILE,
        jnp.where(start + rows < total_rows, (start + rows) // TILE, -1), jnp.where(start > 0, (start - 1) // TILE, -1),
    ])
    inverse = jnp.transpose(coarse_inverse, (1, 2, 0))

    def blocked(x):
        return x.reshape(2, 8, chunks, 128).transpose(0, 2, 1, 3)

    forcing, east, north, storage = [blocked(x) for x in (forcing, east, north, storage)]
    devices = lax.axis_size(GY)
    mates = [(i, i ^ 1) for i in range(devices)]
    others = [(i, j) for i in range(devices) if (j := ((i + 1) ^ 1) - 1) in range(devices)]
    inner, outer = lax.axis_size(GY[1]) * lax.axis_size(GY[2]), lax.axis_size(GY[0])

    def call(kernel, outs, *args, scratch=()):
        places, kept_in = {"S": pltpu.SMEM, "H": pltpu.HBM}, {"V": pltpu.VMEM, "H": pltpu.HBM}
        kinds, values = [], []
        for kind, items in args:
            for x in items:
                kinds.append(kind)
                space = kept_in.get(kind)
                values.append(pltpu.with_memory_space_constraint(x, space) if space is not None else x)
        return pl.pallas_call(
            kernel,
            out_shape=[kept_in[k](s, d) if k in kept_in else jax.ShapeDtypeStruct(s, d) for k, s, d in outs],
            in_specs=[pl.BlockSpec(memory_space=places.get(k, pltpu.VMEM)) for k in kinds],
            out_specs=[pl.BlockSpec(memory_space=places.get(k, pltpu.VMEM)) for k, _, _ in outs],
            scratch_shapes=list(scratch),
            compiler_params=pltpu.CompilerParams(vmem_limit_bytes=VMEM_LIMIT),
        )(*values)

    def everywhere(copies):
        near = lax.all_to_all(copies, GY[1:], 0, 0)
        (copies,) = call(sum_kernel, [("V", (outer,) + near.shape[1:], F32)], ("V", [near]))
        return lax.all_to_all(copies, GY[0], 0, 0)

    own_shape, all_shape, end_shape = (2, chunks, 8, 128), (3, chunks, 8, 128), (chunks, 8, 128)
    halo, pad_shape = (6, chunks, 1, 128), (3, chunks + 2, 8, 128)
    own_v = pltpu.VMEM(own_shape, F32)
    codes_v, columns = pltpu.VMEM((3, chunks, 128), F32), pltpu.VMEM((3, ORDER, chunks, 128), F32)

    def dma(*shape):
        return pltpu.SemaphoreType.DMA(shape)

    sums, codes, gather, scatter, lanes, patterns = call(
        moments_kernel,
        [("", (inner, 8, 128), F32), ("V", (8, membership.shape[1]), F32), ("V", (64, 256), BF16), ("V", (128, 128), BF16),
         ("V", (2, 32, 128), F32), ("V", (3, ORDER, 8, 128), F32)],
        ("S", [info]), ("H", [forcing, membership, land, *[jnp.asarray(x) for x in tables()]]),
        scratch=(own_v, codes_v, pltpu.VMEM(membership.shape, I32), pltpu.VMEM(land.shape, I32), dma(1, HALVES), dma(7)),
    )
    parts = everywhere(sums)
    east, north, center, mate, other = call(
        faces_kernel,
        [("V", (2, chunks + 1, 8, 128), F32)] + [("H", own_shape, F32)] * 2 + [("V", halo, F32)] * 2,
        ("S", [info]), ("V", [codes]), ("H", [forcing, east, north, storage]),
        scratch=(own_v, own_v, codes_v) + (own_v,) * 4 + (dma(4, GROUPS), dma(2, GROUPS)),
    )
    mate = lax.ppermute(mate, GY, mates)
    other = lax.ppermute(other, GY, others)
    field, north, center, z_first, image_first, sums, kept, jacobi, end_f, end_n = call(
        second_kernel,
        [("V", own_shape, F32)] * 3 + [("V", pad_shape, F32), ("V", all_shape, F32), ("V", (inner, 16, 128), F32), ("V", (16, 128), F32),
         ("V", all_shape, F32), ("V", end_shape, F32), ("V", end_shape, F32)],
        ("S", [info]), ("V", [parts]), ("H", [forcing, north, center]),
        ("V", [mate, other, inverse, codes, gather, scatter, lanes, patterns, east]),
        scratch=(codes_v, pltpu.VMEM((chunks + 1, 8, 128), F32), pltpu.VMEM(end_shape, F32), columns, dma(3, GROUPS)),
    )
    parts = everywhere(sums)
    z_second, image_second, sums, scalars = call(
        third_kernel,
        [("V", pad_shape, F32), ("V", own_shape, F32), ("V", (1, 128), F32), ("V", (8, 128), F32)],
        ("V", [parts]),
        ("V", [kept, inverse, field, image_first, codes, scatter, patterns, east, north, center, jacobi, end_f, end_n]),
        scratch=(codes_v, columns),
    )
    chips = lax.axis_size(GY[:2])
    swapped = lax.ppermute(sums, GY[2], [(0, 1), (1, 0)])
    (sums,) = call(pair_kernel, [("V", (chips, 1, 128), F32)], ("V", [sums, swapped]))
    parts = lax.all_to_all(sums, GY[:2], 0, 0)
    answer = call(
        last_kernel,
        [("H", own_shape, F32)] * 2,
        ("V", [parts]), ("V", [scalars, field, z_first, image_first, z_second, image_second]),
        scratch=(own_v,) * 2 + (dma(2, GROUPS),),
    )
    return tuple(x.transpose(0, 2, 1, 3).reshape(rows, width) for x in answer)


def solution(mesh):
    finer = Mesh(mesh.devices.reshape(mesh.shape["ens"], 8, 8, 2), ("ens", "gy_0", "gy_1", "gy_2"))
    return jax.shard_map(
        body,
        mesh=finer,
        in_specs=(P(ENS_GY, None), P(GY, None), P(GY, None), P(GY, None), P(), P(), P()),
        out_specs=(P(ENS_GY, None), P(ENS_GY, None)),
        check_vma=False,
    )
```

```python
import jax
import jax.numpy as jnp
import numpy as np
from jax import lax
from jax.experimental import pallas as pl
from jax.experimental.pallas import tpu as pltpu
from jax.sharding import Mesh
from jax.sharding import PartitionSpec as P


TILE = 64
ORDER = 4
GY = ("gy_0", "gy_1", "gy_2")
ENS_GY = ("ens", "gy_0", "gy_1", "gy_2")
F32, BF16, I32 = jnp.float32, jnp.bfloat16, jnp.int32
ROWS = 32
PIECE = 32
BLOCK = 32
GROUPS = 4
HALVES = 2
VMEM_LIMIT = 24 * 2**20


def tables():
    degree = np.arange(ORDER)[:, None]
    mode = np.cos(np.pi * degree * (np.arange(TILE)[None, :] + 0.5) / TILE)
    p_of = np.tile(np.repeat(np.arange(ORDER), ORDER), 2)
    q_of = np.tile(np.arange(ORDER), 2 * ORDER)
    half = np.repeat(np.arange(2), ORDER * ORDER)
    lane = np.arange(128)
    cols = (mode[q_of][:, lane % TILE] * (half[:, None] == lane[None, :] // TILE)).astype(np.float32)
    high = cols.astype(BF16)
    low = (cols - high.astype(np.float32)).astype(BF16)
    gather = np.concatenate([np.concatenate([high, high], axis=1), np.concatenate([low, np.zeros_like(low)], axis=1)], axis=0)
    scatter = np.concatenate([high, high, low, np.zeros_like(low)], axis=0)
    rows = mode[p_of].reshape(32, 8, 8).transpose(1, 0, 2).astype(np.float32)
    row_lanes = np.tile(rows, (1, 1, 16))
    row_subs = np.broadcast_to(mode.reshape(ORDER, 8, 8, 1).transpose(1, 0, 2, 3), (8, ORDER, 8, 128)).astype(np.float32)
    ends = np.zeros((TILE // 16, ORDER, 8, 128), np.float32)
    for k in range(TILE // 16):
        ends[k, :, :4] = row_subs[(2 * k + 2) % 8, :, :4]
        ends[k, :, 4:] = row_subs[(2 * k - 1) % 8, :, 4:]
    return gather, scatter, row_lanes, row_subs, ends


def iota(shape, dim):
    return lax.broadcasted_iota(I32, shape, dim)


def onehot(codes):
    return jnp.where(codes == (iota(codes.shape, 1) % TILE).astype(F32), 1.0, 0.0).astype(BF16)


def spread_row(ref, row):
    return jnp.broadcast_to(ref[pl.ds(row, 1)], (8, 128))


def dot_nt(a, b):
    return lax.dot_general(a, b, (((1,), (1,)), ((), ())), preferred_element_type=F32)


def dot_nn(a, b):
    return lax.dot_general(a, b, (((1,), (0,)), ((), ())), preferred_element_type=F32)


def split(x):
    high = x.astype(BF16)
    return high, (x - high.astype(F32)).astype(BF16)


def expand(codes_small, out):
    chunks, tiles = out.shape[1], codes_small.shape[1]
    mine = iota((chunks, tiles), 1) // 2 == iota((chunks, tiles), 0)
    halves = jnp.where(iota((tiles, 128), 0) % 2 == iota((tiles, 128), 1) // TILE, 1.0, 0.0).astype(BF16)
    for k in range(3):
        out[k] = dot_nn(jnp.where(mine, codes_small[k : k + 1], 0.0).astype(BF16), halves)


def moments(field, codes, gather, lanes, loads=None):
    wide = [jnp.concatenate([lanes[r]] * (BLOCK * 8 // 128), axis=1) for r in range(2)]

    total = jnp.zeros((32, 128), F32)
    for k in range(codes.shape[1] // BLOCK):
        first = k * BLOCK
        if loads is not None and first % loads.size == 0:
            loads.wait(first // loads.size)
        lifted = jnp.zeros((32, BLOCK * 8), F32)
        for r in range(2):
            both = dot_nt(gather[...], jnp.concatenate(split(field[r, pl.ds(first, BLOCK)].reshape(BLOCK * 8, 128)), axis=1))
            lifted = lifted + wide[r] * (both[:32] + both[32:])
        own = onehot(jnp.concatenate([spread_row(codes.at[0], first + j) for j in range(BLOCK)], axis=0))
        parts = dot_nn(jnp.concatenate(split(lifted), axis=0), own)
        total = total + parts[:32] + parts[32:]
    sums = total[:16] + pltpu.roll(total[16:], TILE, 1)
    return jnp.where(iota((8, 128), 1) < TILE, sums[:8], pltpu.roll(sums[8:], TILE, 1))


def unpack(tile):
    return jnp.concatenate([tile, pltpu.roll(tile, TILE, 1)], axis=0)[:, :TILE]


def coarse_solve(inverse, sums):
    coef = jnp.zeros_like(sums)
    for j in range(sums.shape[0]):
        coef = coef + inverse[j] * sums[j : j + 1]
    return coef


def total_of(x):
    return jnp.sum(jnp.sum(x, axis=1, keepdims=True), axis=0, keepdims=True)


def column_tables(coef, codes, scatter, out):
    zero = jnp.zeros_like(coef)
    rows = [jnp.concatenate([coef, zero], axis=1), jnp.concatenate([zero, coef], axis=1)]
    high, low = split(jnp.concatenate(rows * 4, axis=0))
    for row in range(3):
        own = onehot(codes[row])
        per_tile = dot_nt(own, high) + dot_nt(own, low)
        lane = iota(per_tile.shape, 1)
        rounded = per_tile.astype(BF16).astype(F32)
        pieces = jnp.where(lane // 32 == 1, per_tile - rounded, rounded)
        split_p = [jnp.where(lane // ORDER % ORDER == p, pieces, 0.0).astype(BF16) for p in range(ORDER)]
        columns = dot_nn(jnp.concatenate(split_p, axis=0), scatter[...])
        for p in range(ORDER):
            out[row, p] = columns[p * codes.shape[1] : (p + 1) * codes.shape[1]]


def sum_kernel(parts, out):
    out[...] = jnp.broadcast_to(jnp.sum(parts[...], axis=0)[None], out.shape)


def scalar_rows(values):
    tile = jnp.zeros((8, 128), F32)
    for k, value in enumerate(values):
        tile = jnp.where(iota((8, 128), 0) == k, value, tile)
    return tile


class Loads:
    def __init__(self, pairs, sems, chunks, groups=GROUPS):
        self.pairs, self.sems, self.size, self.groups = pairs, sems, chunks // groups, groups

    def copy(self, i, group):
        source, target = self.pairs[i]
        part = pl.ds(pl.multiple_of(group * self.size, self.size), self.size)
        return pltpu.make_async_copy(source.at[:, part], target.at[:, part], self.sems.at[i, group])

    def start(self, order=None):
        for group in range(self.groups) if order is None else order:
            for i in range(len(self.pairs)):
                self.copy(i, group).start()

    def wait(self, group):
        for i in range(len(self.pairs)):
            self.copy(i, group).wait()


def position(membership):
    rows, total_rows = 2 * 8, membership.shape[0] * TILE
    index = lax.axis_index(GY)
    start = index * rows
    after = jnp.where(start + rows < total_rows, lax.div(start + rows, TILE), -1)
    before = jnp.where(start > 0, lax.div(start - 1, TILE), -1)
    return lax.div(lax.rem(start, TILE), 8), (lax.div(start, TILE), after, before)


def moments_kernel(forcing, membership, land, gather, scatter, row_lanes, row_subs, ends,
                   sums_o, codes_o, gather_o, scatter_o, lanes_o, patterns_o, field, codes, member_in, land_in, sems, small):
    chunks = forcing.shape[1]
    block, tile_rows = position(membership)
    pairs = [(membership, member_in), (land, land_in), (gather, gather_o), (row_lanes.at[pl.ds(block, 2)], lanes_o),
             (scatter, scatter_o), (row_subs.at[pl.ds(block, 2)], patterns_o.at[0:2]), (ends.at[lax.div(block, 2)], patterns_o.at[2])]
    copies = [pltpu.make_async_copy(x, y, small.at[i]) for i, (x, y) in enumerate(pairs)]
    for copy in copies:
        copy.start()
    loads = Loads([(forcing, field)], sems, chunks, HALVES)
    loads.start()
    for copy in copies:
        copy.wait()
    for k in range(3):
        row = pl.ds(jnp.maximum(tile_rows[k], 0), 1)
        dry = (land_in[row] == 1) | (tile_rows[k] < 0)
        codes_o[k : k + 1] = jnp.where(dry, TILE, member_in[row]).astype(F32)
    expand(codes_o, codes)
    tile = moments(field, codes, gather_o, lanes_o, loads)
    sums_o[...] = jnp.broadcast_to(tile[None], sums_o.shape)


def faces_kernel(codes_small, forcing, east, north, storage, east_o, north_h, center_h, mate_o, other_o,
                 north_o, center_o, codes, f_in, e_in, n_in, s_in, sems, out_sems):
    chunks = forcing.shape[1]
    loads = Loads([(east, e_in), (north, n_in), (storage, s_in), (forcing, f_in)], sems, chunks)
    loads.start((3, 0, 1, 2))
    saves = Loads([(north_o, north_h), (center_o, center_h)], out_sems, chunks)
    expand(codes_small, codes)
    lane, sub = iota((8, 128), 1), iota((8, 128), 0)
    odd = lax.rem(lax.axis_index(GY), 2) == 1

    def rolled(x):
        return pltpu.roll(x, 1, 1)

    def after_of(row):
        code = spread_row(codes.at[0], row)
        return code, pltpu.roll(code, 127, 1)

    def east_of(c, here, turned, turned_next):
        mask = (here < TILE) & (jnp.where(lane == 127, turned_next, turned) < TILE)
        return [jnp.where(mask, e_in[r, c], 0.0) for r in range(2)]

    first_code, first_turned = after_of(0)
    loads.wait(3)
    last = east_of(chunks - 1, *after_of(chunks - 1), first_turned)
    for r in range(2):
        east_o[r, 0] = last[r]

    def chunk(k, j, carry):
        west_before, here, turned = carry
        c = k * ROWS + j
        ahead = k * ROWS + j + 1 if j + 1 < ROWS else lax.rem(k * ROWS + ROWS, chunks)
        coming, coming_turned = after_of(ahead)
        face = east_of(c, here, turned, coming_turned)
        wet = here < TILE
        open_north = wet & ((sub < 7) | (spread_row(codes.at[1], c) < TILE))
        west_next = [rolled(x) for x in face]
        west = [jnp.where(lane == 0, west_before[r], west_next[r]) for r in range(2)]
        norths = [jnp.where(wet, n_in[0, c], 0.0), jnp.where(open_north, n_in[1, c], 0.0)]
        shifted = [pltpu.roll(x, 1, 0) for x in norths]
        south = [jnp.where(sub == 0, 0.0, shifted[0]), jnp.where(sub == 0, shifted[0], shifted[1])]
        fields, centers = [f_in[0, c], f_in[1, c]], []
        for r in range(2):
            center = jnp.where(wet, s_in[r, c], 1.0) + face[r] + west[r] + norths[r] + south[r]
            east_o[r, c + 1] = face[r]
            north_o[r, c] = norths[r]
            center_o[r, c] = center
            centers.append(center)
        smooth = jnp.where(sub < 4, fields[0], fields[1]) / jnp.where(sub < 4, centers[0], centers[1])
        first = [x[0][0:1] for x in (fields, centers, face, norths)] + [smooth[1:2]] * 2
        final = [x[1][7:8] for x in (fields, centers, face, norths)] + [smooth[6:7], norths[1][6:7]]
        for j in range(6):
            mate_o[j, c] = jnp.where(odd, first[j], final[j])
            other_o[j, c] = jnp.where(odd, final[j], first[j])
        return west_next, coming, coming_turned

    size = chunks // GROUPS // ROWS

    def step(k, carry):
        @pl.when((lax.rem(k, size) == 0) & (k < (GROUPS - 1) * size))
        def _():
            loads.wait(lax.div(k, size))

        for j in range(ROWS):
            carry = chunk(k, j, carry)

        @pl.when(lax.rem(k, size) == size - 1)
        def _():
            for i in range(2):
                saves.copy(i, lax.div(k, size)).start()

        return carry

    lax.fori_loop(0, chunks // ROWS, step, ([rolled(x) for x in last], first_code, first_turned))
    for group in range(GROUPS):
        saves.wait(group)


def apply_operator(z_pad, faces, blocks, out):
    east, north, center = faces
    chunks = z_pad.shape[1] - 2
    z_pad[:, 0] = z_pad[:, chunks]
    z_pad[:, chunks + 1] = z_pad[:, 1]
    n = PIECE
    sub, lane = iota((n, 8, 128), 1), iota((n, 8, 128), 2)

    def step(k, total):
        c = pl.multiple_of(k * n, n)
        own = [z_pad[r, pl.ds(c + 1, n)] for r in range(3)]
        faced = [north(r, pl.ds(c, n)) for r in range(3)]
        below = [pltpu.roll(faced[r] * own[r], 1, 1) for r in range(3)]
        above = [pltpu.roll(own[r], 7, 1) for r in range(3)]
        for r in range(blocks):
            ahead = pltpu.roll(z_pad[r, pl.ds(c + 1, n + 1)], 127, 2)
            ahead = jnp.where(lane == 127, ahead[1:], ahead[:-1])
            face = east(r, pl.ds(c, n + 1))
            behind = pltpu.roll(face * z_pad[r, pl.ds(c, n + 1)], 1, 2)
            behind = jnp.where(lane == 0, behind[:-1], behind[1:])
            image = (center(r, pl.ds(c, n)) * own[r] - face[1:] * ahead - behind
                     - faced[r] * jnp.where(sub == 7, above[(r + 1) % 3], above[r])
                     - jnp.where(sub == 0, below[(r + 2) % 3], below[r]))
            out[r, pl.ds(c, n)] = image
            if r < 2:
                total = total + jnp.sum(own[r] * image, axis=0)
        return total

    return lax.fori_loop(0, chunks // n, step, jnp.zeros((8, 128), F32))


def chooser(*views):
    return lambda r, part: views[r][part]


class Spread:
    def __init__(self, columns, patterns):
        self.columns = columns
        self.patterns = [[patterns[r, p] for p in range(ORDER)] for r in range(3)]
        self.sub = iota((8, 128), 0)

    def at(self, c):
        def row(k, p):
            return spread_row(self.columns.at[k, p], c)

        own = [row(0, p) for p in range(ORDER)]
        end = [jnp.where(self.sub < 4, row(1, p), row(2, p)) for p in range(ORDER)]
        return [sum(self.patterns[r][p] * x[p] for p in range(ORDER)) for r, x in enumerate((own, own, end))]


def second_kernel(parts, forcing, north_h, center_h, mate, other, inverse, codes_small, gather, scatter, lanes, patterns, east,
                  field, north, center, z_pad, image_o, sums_o, kept_o, jacobi_o, end_f, end_n,
                  codes, end_e, end_c, columns, sems):
    chunks = forcing.shape[1]
    loads = Loads([(forcing, field), (north_h, north), (center_h, center)], sems, chunks)
    loads.start()
    expand(codes_small, codes)
    tile = jnp.sum(parts[...], axis=0)
    sums = unpack(tile)
    coef = coarse_solve(inverse, sums)
    kept_o[0:8] = tile
    kept_o[8:16] = jnp.broadcast_to(total_of(sums * coef), (8, 128))
    column_tables(coef, codes, scatter, columns)
    spread = Spread(columns, patterns)
    sub = iota((8, 128), 0)
    after = jnp.logical_xor(sub < 4, lax.rem(lax.axis_index(GY), 2) == 1)

    def chunk(c, total):
        added = spread.at(c)

        def rows(j):
            return jnp.where(after, mate[j, c], other[j, c])

        faced = jnp.where(sub == 6, rows(5), rows(3))
        far = rows(0)
        beyond = rows(1) + jnp.where(sub == 0, pltpu.roll(north[1, c], 1, 0), 0.0)
        first = center[0, c] + jnp.where(sub == 0, pltpu.roll(faced, 1, 0), 0.0)
        both = jnp.where(sub == 3, pltpu.roll(first, 3, 0), jnp.where(beyond == 0.0, 1.0, beyond))
        inverted = 1.0 / both
        own = [jnp.where(sub == 0, pltpu.roll(inverted, 5, 0), 1.0 / first), 1.0 / center[1, c]]
        end_f[c] = far
        end_n[c] = faced
        end_e[c + 1] = rows(2)
        end_c[c] = both
        center[0, c] = first
        jacobi_o[0, c] = own[0]
        jacobi_o[1, c] = own[1]
        jacobi_o[2, c] = inverted
        smooth = [field[0, c] * own[0], field[1, c] * own[1],
                  jnp.where((sub == 1) | (sub == 6), rows(4), far * inverted)]
        for r in range(3):
            z_pad[r, c + 1] = smooth[r] + added[r]
        return total + (field[0, c] * smooth[0] + field[1, c] * smooth[1])

    size = chunks // GROUPS // ROWS

    def step(k, total):
        @pl.when(lax.rem(k, size) == 0)
        def _():
            loads.wait(lax.div(k, size))

        for j in range(ROWS):
            total = chunk(k * ROWS + j, total)
        return total

    smooth_total = lax.fori_loop(0, chunks // ROWS, step, jnp.zeros((8, 128), F32))
    end_e[0] = end_e[chunks]
    faces = (chooser(east.at[0], east.at[1], end_e), chooser(north.at[0], north.at[1], end_n),
             chooser(center.at[0], center.at[1], end_c))
    image_total = apply_operator(z_pad, faces, 3, image_o)
    tile = moments(image_o, codes, gather, lanes)
    scalars = scalar_rows([jnp.sum(smooth_total, axis=0, keepdims=True), jnp.sum(image_total, axis=0, keepdims=True)])
    sums_o[...] = jnp.broadcast_to(jnp.concatenate([tile, scalars], axis=0)[None], sums_o.shape)


def third_kernel(parts, kept, inverse, forcing, image, codes_small, scatter, patterns, east, north, center,
                 jacobi, end_f, end_n, z_pad, image_o, sums_o, scalars_o, codes, columns):
    chunks = forcing.shape[1]
    expand(codes_small, codes)
    tile = jnp.sum(parts[...], axis=0)
    energy = jnp.sum(tile[8:9], axis=1, keepdims=True) + kept[8:9, 0:1]
    alpha = energy / jnp.sum(tile[9:10], axis=1, keepdims=True)
    sums = unpack(kept[0:8] - alpha * tile[0:8])
    coef = coarse_solve(inverse, sums)
    scalars_o[...] = scalar_rows([alpha, energy, total_of(sums * coef)])
    column_tables(coef, codes, scatter, columns)
    spread = Spread(columns, patterns)
    factor = jnp.broadcast_to(alpha, (8, 128))

    def chunk(c, total):
        added = spread.at(c)
        fields = [forcing[0, c], forcing[1, c], end_f[c]]
        for r in range(3):
            residual = fields[r] - factor * image[r, c]
            smooth = jacobi[r, c] * residual
            z_pad[r, c + 1] = smooth + added[r]
            if r < 2:
                total = total + residual * smooth
        return total

    def step(k, total):
        for j in range(ROWS):
            total = chunk(k * ROWS + j, total)
        return total

    smooth_total = lax.fori_loop(0, chunks // ROWS, step, jnp.zeros((8, 128), F32))
    faces = (chooser(east.at[0], east.at[1]), chooser(north.at[0], north.at[1], end_n), chooser(center.at[0], center.at[1]))
    image_total = apply_operator(z_pad, faces, 2, image_o)
    smooth_row, image_row = [x + pltpu.roll(x, TILE, 1) for x in (smooth_total, image_total)]
    packed = jnp.where(iota((8, 128), 1) < TILE, smooth_row, image_row)
    sums_o[...] = jnp.sum(packed, axis=0, keepdims=True)


def pair_kernel(mine, mates, out):
    out[...] = jnp.broadcast_to((mine[...] + mates[...])[None], out.shape)


def last_kernel(parts, scalars, forcing, z_first, image_first, z_second, image_second, solution_o, residual_o,
                solution_v, residual_v, out_sems):
    chunks = forcing.shape[1]
    saves = Loads([(solution_v, solution_o), (residual_v, residual_o)], out_sems, chunks)
    row = jnp.sum(parts[...], axis=0)
    left = iota(row.shape, 1) < TILE
    alpha, energy = scalars[0:1, 0:1], scalars[1:2, 0:1]
    energy_next = jnp.sum(jnp.where(left, row, 0.0), axis=1, keepdims=True) + scalars[2:3, 0:1]
    beta = energy_next / energy
    alpha_next = energy_next / (jnp.sum(jnp.where(left, 0.0, row), axis=1, keepdims=True) - beta * energy_next / alpha)
    alpha, beta, alpha_next = [x.reshape(1, 1, 1) for x in (alpha, beta, alpha_next)]
    per_group = chunks // GROUPS // PIECE

    def step(k, carry):
        c = pl.multiple_of(k * PIECE, PIECE)
        part, shifted = pl.ds(c, PIECE), pl.ds(c + 1, PIECE)
        for r in range(2):
            z, image = z_first[r, shifted], image_first[r, part]
            solution_v[r, part] = alpha * z + alpha_next * (z_second[r, shifted] + beta * z)
            residual_v[r, part] = (forcing[r, part] - alpha * image) - alpha_next * (image_second[r, part] + beta * image)

        @pl.when(lax.rem(k, per_group) == per_group - 1)
        def _():
            for i in range(2):
                saves.copy(i, lax.div(k, per_group)).start()

        return carry

    lax.fori_loop(0, chunks // PIECE, step, 0)
    for group in range(GROUPS):
        saves.wait(group)


def body(forcing, east, north, storage, coarse_inverse, membership, land):
    rows, width = forcing.shape
    chunks = width // 128
    inverse = jnp.transpose(coarse_inverse, (1, 2, 0))

    def blocked(x):
        return x.reshape(2, 8, chunks, 128).transpose(0, 2, 1, 3)

    forcing, east, north, storage = [blocked(x) for x in (forcing, east, north, storage)]
    devices = lax.axis_size(GY)
    mates = [(i, i ^ 1) for i in range(devices)]
    others = [(i, j) for i in range(devices) if (j := ((i + 1) ^ 1) - 1) in range(devices)]
    inner, outer = lax.axis_size(GY[1]) * lax.axis_size(GY[2]), lax.axis_size(GY[0])

    def call(kernel, outs, *args, scratch=()):
        places, kept_in = {"H": pltpu.HBM}, {"V": pltpu.VMEM, "H": pltpu.HBM}
        kinds, values = [], []
        for kind, items in args:
            for x in items:
                kinds.append(kind)
                space = kept_in.get(kind)
                values.append(pltpu.with_memory_space_constraint(x, space) if space is not None else x)
        return pl.pallas_call(
            kernel,
            out_shape=[kept_in[k](s, d) if k in kept_in else jax.ShapeDtypeStruct(s, d) for k, s, d in outs],
            in_specs=[pl.BlockSpec(memory_space=places.get(k, pltpu.VMEM)) for k in kinds],
            out_specs=[pl.BlockSpec(memory_space=places.get(k, pltpu.VMEM)) for k, _, _ in outs],
            scratch_shapes=list(scratch),
            compiler_params=pltpu.CompilerParams(vmem_limit_bytes=VMEM_LIMIT),
        )(*values)

    def everywhere(copies):
        near = lax.all_to_all(copies, GY[1:], 0, 0)
        (copies,) = call(sum_kernel, [("V", (outer,) + near.shape[1:], F32)], ("V", [near]))
        return lax.all_to_all(copies, GY[0], 0, 0)

    own_shape, all_shape, end_shape = (2, chunks, 8, 128), (3, chunks, 8, 128), (chunks, 8, 128)
    halo, pad_shape = (6, chunks, 1, 128), (3, chunks + 2, 8, 128)
    own_v = pltpu.VMEM(own_shape, F32)
    codes_v, columns = pltpu.VMEM((3, chunks, 128), F32), pltpu.VMEM((3, ORDER, chunks, 128), F32)

    def dma(*shape):
        return pltpu.SemaphoreType.DMA(shape)

    sums, codes, gather, scatter, lanes, patterns = call(
        moments_kernel,
        [("", (inner, 8, 128), F32), ("V", (8, membership.shape[1]), F32), ("V", (64, 256), BF16), ("V", (128, 128), BF16),
         ("V", (2, 32, 128), F32), ("V", (3, ORDER, 8, 128), F32)],
        ("H", [forcing, membership, land, *[jnp.asarray(x) for x in tables()]]),
        scratch=(own_v, codes_v, pltpu.VMEM(membership.shape, I32), pltpu.VMEM(land.shape, I32), dma(1, HALVES), dma(7)),
    )
    parts = everywhere(sums)
    east, north, center, mate, other = call(
        faces_kernel,
        [("V", (2, chunks + 1, 8, 128), F32)] + [("H", own_shape, F32)] * 2 + [("V", halo, F32)] * 2,
        ("V", [codes]), ("H", [forcing, east, north, storage]),
        scratch=(own_v, own_v, codes_v) + (own_v,) * 4 + (dma(4, GROUPS), dma(2, GROUPS)),
    )
    mate = lax.ppermute(mate, GY, mates)
    other = lax.ppermute(other, GY, others)
    field, north, center, z_first, image_first, sums, kept, jacobi, end_f, end_n = call(
        second_kernel,
        [("V", own_shape, F32)] * 3 + [("V", pad_shape, F32), ("V", all_shape, F32), ("V", (inner, 16, 128), F32), ("V", (16, 128), F32),
         ("V", all_shape, F32), ("V", end_shape, F32), ("V", end_shape, F32)],
        ("V", [parts]), ("H", [forcing, north, center]),
        ("V", [mate, other, inverse, codes, gather, scatter, lanes, patterns, east]),
        scratch=(codes_v, pltpu.VMEM((chunks + 1, 8, 128), F32), pltpu.VMEM(end_shape, F32), columns, dma(3, GROUPS)),
    )
    parts = everywhere(sums)
    z_second, image_second, sums, scalars = call(
        third_kernel,
        [("V", pad_shape, F32), ("V", own_shape, F32), ("V", (1, 128), F32), ("V", (8, 128), F32)],
        ("V", [parts]),
        ("V", [kept, inverse, field, image_first, codes, scatter, patterns, east, north, center, jacobi, end_f, end_n]),
        scratch=(codes_v, columns),
    )
    chips = lax.axis_size(GY[:2])
    swapped = lax.ppermute(sums, GY[2], [(0, 1), (1, 0)])
    (sums,) = call(pair_kernel, [("V", (chips, 1, 128), F32)], ("V", [sums, swapped]))
    parts = lax.all_to_all(sums, GY[:2], 0, 0)
    answer = call(
        last_kernel,
        [("H", own_shape, F32)] * 2,
        ("V", [parts]), ("V", [scalars, field, z_first, image_first, z_second, image_second]),
        scratch=(own_v,) * 2 + (dma(2, GROUPS),),
    )
    return tuple(x.transpose(0, 2, 1, 3).reshape(rows, width) for x in answer)


def solution(mesh):
    finer = Mesh(mesh.devices.reshape(mesh.shape["ens"], 8, 8, 2), ("ens", "gy_0", "gy_1", "gy_2"))
    return jax.shard_map(
        body,
        mesh=finer,
        in_specs=(P(ENS_GY, None), P(GY, None), P(GY, None), P(GY, None), P(), P(), P()),
        out_specs=(P(ENS_GY, None), P(ENS_GY, None)),
        check_vma=False,
    )
```

```python
import jax
import jax.numpy as jnp
import numpy as np
from jax import lax
from jax.experimental import pallas as pl
from jax.experimental.pallas import tpu as pltpu
from jax.sharding import Mesh
from jax.sharding import PartitionSpec as P


TILE = 64
ORDER = 4
GY = ("gy_0", "gy_1", "gy_2")
ENS_GY = ("ens", "gy_0", "gy_1", "gy_2")
F32, BF16, I32 = jnp.float32, jnp.bfloat16, jnp.int32
ROWS = 32
PIECE = 32
BLOCK = 32
GROUPS = 4
HALVES = 2
EIGHTHS = 8
VMEM_LIMIT = 24 * 2**20


def tables():
    degree = np.arange(ORDER)[:, None]
    mode = np.cos(np.pi * degree * (np.arange(TILE)[None, :] + 0.5) / TILE)
    p_of = np.tile(np.repeat(np.arange(ORDER), ORDER), 2)
    q_of = np.tile(np.arange(ORDER), 2 * ORDER)
    half = np.repeat(np.arange(2), ORDER * ORDER)
    lane = np.arange(128)
    cols = (mode[q_of][:, lane % TILE] * (half[:, None] == lane[None, :] // TILE)).astype(np.float32)
    high = cols.astype(BF16)
    low = (cols - high.astype(np.float32)).astype(BF16)
    gather = np.concatenate([np.concatenate([high, high], axis=1), np.concatenate([low, np.zeros_like(low)], axis=1)], axis=0)
    scatter = np.concatenate([high, high, low, np.zeros_like(low)], axis=0)
    rows = mode[p_of].reshape(32, 8, 8).transpose(1, 0, 2).astype(np.float32)
    row_lanes = np.tile(rows, (1, 1, 16))
    row_subs = np.broadcast_to(mode.reshape(ORDER, 8, 8, 1).transpose(1, 0, 2, 3), (8, ORDER, 8, 128)).astype(np.float32)
    ends = np.zeros((TILE // 16, ORDER, 8, 128), np.float32)
    for k in range(TILE // 16):
        ends[k, :, :4] = row_subs[(2 * k + 2) % 8, :, :4]
        ends[k, :, 4:] = row_subs[(2 * k - 1) % 8, :, 4:]
    return gather, scatter, row_lanes, row_subs, ends


def iota(shape, dim):
    return lax.broadcasted_iota(I32, shape, dim)


def onehot(codes):
    return jnp.where(codes == (iota(codes.shape, 1) % TILE).astype(F32), 1.0, 0.0).astype(BF16)


def spread_row(ref, row):
    return jnp.broadcast_to(ref[pl.ds(row, 1)], (8, 128))


def dot_nt(a, b):
    return lax.dot_general(a, b, (((1,), (1,)), ((), ())), preferred_element_type=F32)


def dot_nn(a, b):
    return lax.dot_general(a, b, (((1,), (0,)), ((), ())), preferred_element_type=F32)


def split(x):
    high = x.astype(BF16)
    return high, (x - high.astype(F32)).astype(BF16)


def expand(codes_small, out):
    chunks, tiles = out.shape[1], codes_small.shape[1]
    mine = iota((chunks, tiles), 1) // 2 == iota((chunks, tiles), 0)
    halves = jnp.where(iota((tiles, 128), 0) % 2 == iota((tiles, 128), 1) // TILE, 1.0, 0.0).astype(BF16)
    for k in range(3):
        out[k] = dot_nn(jnp.where(mine, codes_small[k : k + 1], 0.0).astype(BF16), halves)


def moments(field, codes, gather, lanes, loads=None):
    wide = [jnp.concatenate([lanes[r]] * (BLOCK * 8 // 128), axis=1) for r in range(2)]

    total = jnp.zeros((32, 128), F32)
    for k in range(codes.shape[1] // BLOCK):
        first = k * BLOCK
        if loads is not None and first % loads.size == 0:
            loads.wait(first // loads.size)
        lifted = jnp.zeros((32, BLOCK * 8), F32)
        for r in range(2):
            both = dot_nt(gather[...], jnp.concatenate(split(field[r, pl.ds(first, BLOCK)].reshape(BLOCK * 8, 128)), axis=1))
            lifted = lifted + wide[r] * (both[:32] + both[32:])
        own = onehot(jnp.concatenate([spread_row(codes.at[0], first + j) for j in range(BLOCK)], axis=0))
        parts = dot_nn(jnp.concatenate(split(lifted), axis=0), own)
        total = total + parts[:32] + parts[32:]
    sums = total[:16] + pltpu.roll(total[16:], TILE, 1)
    return jnp.where(iota((8, 128), 1) < TILE, sums[:8], pltpu.roll(sums[8:], TILE, 1))


def unpack(tile):
    return jnp.concatenate([tile, pltpu.roll(tile, TILE, 1)], axis=0)[:, :TILE]


def coarse_solve(inverse, sums):
    coef = jnp.zeros_like(sums)
    for j in range(sums.shape[0]):
        coef = coef + inverse[j] * sums[j : j + 1]
    return coef


def total_of(x):
    return jnp.sum(jnp.sum(x, axis=1, keepdims=True), axis=0, keepdims=True)


def column_tables(coef, codes, scatter, out):
    zero = jnp.zeros_like(coef)
    rows = [jnp.concatenate([coef, zero], axis=1), jnp.concatenate([zero, coef], axis=1)]
    high, low = split(jnp.concatenate(rows * 4, axis=0))
    for row in range(3):
        own = onehot(codes[row])
        per_tile = dot_nt(own, high) + dot_nt(own, low)
        lane = iota(per_tile.shape, 1)
        rounded = per_tile.astype(BF16).astype(F32)
        pieces = jnp.where(lane // 32 == 1, per_tile - rounded, rounded)
        split_p = [jnp.where(lane // ORDER % ORDER == p, pieces, 0.0).astype(BF16) for p in range(ORDER)]
        columns = dot_nn(jnp.concatenate(split_p, axis=0), scatter[...])
        for p in range(ORDER):
            out[row, p] = columns[p * codes.shape[1] : (p + 1) * codes.shape[1]]


def sum_kernel(parts, out):
    out[...] = jnp.broadcast_to(jnp.sum(parts[...], axis=0)[None], out.shape)


def two_sums(left, right):
    left, right = [x + pltpu.roll(x, TILE, 1) for x in (left, right)]
    return jnp.sum(jnp.where(iota((8, 128), 1) < TILE, left, right), axis=0, keepdims=True)


def sums_of(row):
    left = iota(row.shape, 1) < TILE
    return [jnp.sum(jnp.where(x, row, 0.0), axis=1, keepdims=True) for x in (left, jnp.logical_not(left))]


def scalar_rows(values):
    tile = jnp.zeros((8, 128), F32)
    for k, value in enumerate(values):
        tile = jnp.where(iota((8, 128), 0) == k, value, tile)
    return tile


class Loads:
    def __init__(self, pairs, sems, chunks, groups=GROUPS):
        self.pairs, self.sems, self.size, self.groups = pairs, sems, chunks // groups, groups

    def copy(self, i, group):
        source, target = self.pairs[i]
        part = pl.ds(pl.multiple_of(group * self.size, self.size), self.size)
        return pltpu.make_async_copy(source.at[:, part], target.at[:, part], self.sems.at[i, group])

    def start(self, order=None):
        for group in range(self.groups) if order is None else order:
            for i in range(len(self.pairs)):
                self.copy(i, group).start()

    def wait(self, group):
        for i in range(len(self.pairs)):
            self.copy(i, group).wait()


def position(membership):
    rows, total_rows = 2 * 8, membership.shape[0] * TILE
    index = lax.axis_index(GY)
    start = index * rows
    after = jnp.where(start + rows < total_rows, lax.div(start + rows, TILE), -1)
    before = jnp.where(start > 0, lax.div(start - 1, TILE), -1)
    return lax.div(lax.rem(start, TILE), 8), (lax.div(start, TILE), after, before)


def moments_kernel(forcing, membership, land, gather, scatter, row_lanes, row_subs, ends,
                   sums_o, codes_o, gather_o, scatter_o, lanes_o, patterns_o, field, codes, member_in, land_in, sems, small):
    chunks = forcing.shape[1]
    block, tile_rows = position(membership)
    pairs = [(membership, member_in), (land, land_in), (gather, gather_o), (row_lanes.at[pl.ds(block, 2)], lanes_o),
             (scatter, scatter_o), (row_subs.at[pl.ds(block, 2)], patterns_o.at[0:2]), (ends.at[lax.div(block, 2)], patterns_o.at[2])]
    copies = [pltpu.make_async_copy(x, y, small.at[i]) for i, (x, y) in enumerate(pairs)]
    for copy in copies:
        copy.start()
    loads = Loads([(forcing, field)], sems, chunks, HALVES)
    loads.start()
    for copy in copies[:4]:
        copy.wait()
    for k in range(3):
        row = pl.ds(jnp.maximum(tile_rows[k], 0), 1)
        dry = (land_in[row] == 1) | (tile_rows[k] < 0)
        codes_o[k : k + 1] = jnp.where(dry, TILE, member_in[row]).astype(F32)
    expand(codes_o, codes)
    tile = moments(field, codes, gather_o, lanes_o, loads)
    sums_o[...] = jnp.broadcast_to(tile[None], sums_o.shape)
    for copy in copies[4:]:
        copy.wait()


def faces_kernel(codes_small, forcing, east, north, storage, east_o, north_h, center_h, mate_o, other_o,
                 north_o, center_o, codes, f_in, e_in, n_in, s_in, sems, out_sems):
    chunks = forcing.shape[1]
    loads = Loads([(east, e_in), (north, n_in), (storage, s_in), (forcing, f_in)], sems, chunks)
    loads.start((3, 0, 1, 2))
    saves = Loads([(north_o, north_h), (center_o, center_h)], out_sems, chunks)
    expand(codes_small, codes)
    lane, sub = iota((8, 128), 1), iota((8, 128), 0)
    odd = lax.rem(lax.axis_index(GY), 2) == 1

    def rolled(x):
        return pltpu.roll(x, 1, 1)

    def after_of(row):
        code = spread_row(codes.at[0], row)
        return code, pltpu.roll(code, 127, 1)

    def east_of(c, here, turned, turned_next):
        mask = (here < TILE) & (jnp.where(lane == 127, turned_next, turned) < TILE)
        return [jnp.where(mask, e_in[r, c], 0.0) for r in range(2)]

    first_code, first_turned = after_of(0)
    loads.wait(3)
    last = east_of(chunks - 1, *after_of(chunks - 1), first_turned)
    for r in range(2):
        east_o[r, 0] = last[r]

    def chunk(k, j, carry):
        west_before, here, turned = carry
        c = k * ROWS + j
        ahead = k * ROWS + j + 1 if j + 1 < ROWS else lax.rem(k * ROWS + ROWS, chunks)
        coming, coming_turned = after_of(ahead)
        face = east_of(c, here, turned, coming_turned)
        wet = here < TILE
        open_north = wet & ((sub < 7) | (spread_row(codes.at[1], c) < TILE))
        west_next = [rolled(x) for x in face]
        west = [jnp.where(lane == 0, west_before[r], west_next[r]) for r in range(2)]
        norths = [jnp.where(wet, n_in[0, c], 0.0), jnp.where(open_north, n_in[1, c], 0.0)]
        shifted = [pltpu.roll(x, 1, 0) for x in norths]
        south = [jnp.where(sub == 0, 0.0, shifted[0]), jnp.where(sub == 0, shifted[0], shifted[1])]
        fields, centers = [f_in[0, c], f_in[1, c]], []
        for r in range(2):
            center = jnp.where(wet, s_in[r, c], 1.0) + face[r] + west[r] + norths[r] + south[r]
            east_o[r, c + 1] = face[r]
            north_o[r, c] = norths[r]
            center_o[r, c] = center
            centers.append(center)
        smooth = jnp.where(sub < 4, fields[0], fields[1]) / jnp.where(sub < 4, centers[0], centers[1])
        first = [x[0][0:1] for x in (fields, centers, face, norths)] + [smooth[1:2]] * 2
        final = [x[1][7:8] for x in (fields, centers, face, norths)] + [smooth[6:7], norths[1][6:7]]
        for j in range(6):
            mate_o[j, c] = jnp.where(odd, first[j], final[j])
            other_o[j, c] = jnp.where(odd, final[j], first[j])
        return west_next, coming, coming_turned

    size = chunks // GROUPS // ROWS

    def step(k, carry):
        @pl.when((lax.rem(k, size) == 0) & (k < (GROUPS - 1) * size))
        def _():
            loads.wait(lax.div(k, size))

        for j in range(ROWS):
            carry = chunk(k, j, carry)

        @pl.when(lax.rem(k, size) == size - 1)
        def _():
            for i in range(2):
                saves.copy(i, lax.div(k, size)).start()

        return carry

    lax.fori_loop(0, chunks // ROWS, step, ([rolled(x) for x in last], first_code, first_turned))
    for group in range(GROUPS):
        saves.wait(group)


def apply_operator(z_pad, faces, blocks, out):
    east, north, center = faces
    chunks = z_pad.shape[1] - 2
    z_pad[:, 0] = z_pad[:, chunks]
    z_pad[:, chunks + 1] = z_pad[:, 1]
    n = PIECE if blocks == 3 else 2 * PIECE
    sub, lane = iota((n, 8, 128), 1), iota((n, 8, 128), 2)

    def step(k, total):
        c = pl.multiple_of(k * n, n)
        own = [z_pad[r, pl.ds(c + 1, n)] for r in range(3)]
        faced = [north(r, pl.ds(c, n)) for r in range(3)]
        below = [pltpu.roll(faced[r] * own[r], 1, 1) for r in range(3)]
        above = [pltpu.roll(own[r], 7, 1) for r in range(3)]
        for r in range(blocks):
            ahead = pltpu.roll(z_pad[r, pl.ds(c + 1, n + 1)], 127, 2)
            ahead = jnp.where(lane == 127, ahead[1:], ahead[:-1])
            face = east(r, pl.ds(c, n + 1))
            behind = pltpu.roll(face * z_pad[r, pl.ds(c, n + 1)], 1, 2)
            behind = jnp.where(lane == 0, behind[:-1], behind[1:])
            image = (center(r, pl.ds(c, n)) * own[r] - face[1:] * ahead - behind
                     - faced[r] * jnp.where(sub == 7, above[(r + 1) % 3], above[r])
                     - jnp.where(sub == 0, below[(r + 2) % 3], below[r]))
            out[r, pl.ds(c, n)] = image
            if r < 2:
                total = total + jnp.sum(own[r] * image, axis=0)
        return total

    return lax.fori_loop(0, chunks // n, step, jnp.zeros((8, 128), F32))


def chooser(*views):
    return lambda r, part: views[r][part]


class Spread:
    def __init__(self, columns, patterns):
        self.columns = columns
        self.patterns = [[patterns[r, p] for p in range(ORDER)] for r in range(3)]
        self.sub = iota((8, 128), 0)

    def at(self, c):
        def row(k, p):
            return spread_row(self.columns.at[k, p], c)

        own = [row(0, p) for p in range(ORDER)]
        end = [jnp.where(self.sub < 4, row(1, p), row(2, p)) for p in range(ORDER)]
        return [sum(self.patterns[r][p] * x[p] for p in range(ORDER)) for r, x in enumerate((own, own, end))]


def second_kernel(parts, forcing, north_h, center_h, mate, other, inverse, codes_small, gather, scatter, lanes, patterns, east,
                  field, north, center, z_pad, image_o, sums_o, kept_o, jacobi_o, end_f, end_n,
                  codes, end_e, end_c, columns, sems):
    chunks = forcing.shape[1]
    loads = Loads([(forcing, field), (north_h, north), (center_h, center)], sems, chunks, EIGHTHS)
    loads.start()
    expand(codes_small, codes)
    tile = jnp.sum(parts[...], axis=0)
    sums = unpack(tile)
    coef = coarse_solve(inverse, sums)
    kept_o[0:8] = tile
    kept_o[8:16] = jnp.broadcast_to(total_of(sums * coef), (8, 128))
    column_tables(coef, codes, scatter, columns)
    spread = Spread(columns, patterns)
    sub = iota((8, 128), 0)
    after = jnp.logical_xor(sub < 4, lax.rem(lax.axis_index(GY), 2) == 1)

    def chunk(c, total):
        added = spread.at(c)

        def rows(j):
            return jnp.where(after, mate[j, c], other[j, c])

        faced = jnp.where(sub == 6, rows(5), rows(3))
        far = rows(0)
        beyond = rows(1) + jnp.where(sub == 0, pltpu.roll(north[1, c], 1, 0), 0.0)
        first = center[0, c] + jnp.where(sub == 0, pltpu.roll(faced, 1, 0), 0.0)
        both = jnp.where(sub == 3, pltpu.roll(first, 3, 0), jnp.where(beyond == 0.0, 1.0, beyond))
        inverted = 1.0 / both
        own = [jnp.where(sub == 0, pltpu.roll(inverted, 5, 0), 1.0 / first), 1.0 / center[1, c]]
        end_f[c] = far
        end_n[c] = faced
        end_e[c + 1] = rows(2)
        end_c[c] = both
        center[0, c] = first
        jacobi_o[0, c] = own[0]
        jacobi_o[1, c] = own[1]
        jacobi_o[2, c] = inverted
        smooth = [field[0, c] * own[0], field[1, c] * own[1],
                  jnp.where((sub == 1) | (sub == 6), rows(4), far * inverted)]
        for r in range(3):
            z_pad[r, c + 1] = smooth[r] + added[r]
        return total + (field[0, c] * smooth[0] + field[1, c] * smooth[1])

    rows_a_step = chunks // EIGHTHS

    def step(k, total):
        loads.wait(k)
        for j in range(rows_a_step):
            total = chunk(k * rows_a_step + j, total)
        return total

    smooth_total = lax.fori_loop(0, EIGHTHS, step, jnp.zeros((8, 128), F32))
    end_e[0] = end_e[chunks]
    faces = (chooser(east.at[0], east.at[1], end_e), chooser(north.at[0], north.at[1], end_n),
             chooser(center.at[0], center.at[1], end_c))
    image_total = apply_operator(z_pad, faces, 3, image_o)
    tile = moments(image_o, codes, gather, lanes)
    for k in range(9):
        row = tile[k : k + 1] if k < 8 else two_sums(smooth_total, image_total)
        sums_o[:, k] = jnp.broadcast_to(row[None], (sums_o.shape[0], 1, 128))


def third_kernel(parts, kept, inverse, forcing, image, codes_small, scatter, patterns, east, north, center,
                 jacobi, end_f, end_n, z_pad, image_o, sums_o, scalars_o, codes, columns, tile):
    chunks = forcing.shape[1]
    expand(codes_small, codes)
    rows = jnp.sum(parts[...], axis=0)
    for k in range(8):
        tile[k : k + 1] = rows[k]
    energy, image_energy = sums_of(rows[8])
    energy = energy + kept[8:9, 0:1]
    alpha = energy / image_energy
    sums = unpack(kept[0:8] - alpha * tile[...])
    coef = coarse_solve(inverse, sums)
    scalars_o[...] = scalar_rows([alpha, energy, total_of(sums * coef)])
    column_tables(coef, codes, scatter, columns)
    spread = Spread(columns, patterns)
    factor = jnp.broadcast_to(alpha, (8, 128))

    def chunk(c, total):
        added = spread.at(c)
        fields = [forcing[0, c], forcing[1, c], end_f[c]]
        for r in range(3):
            residual = fields[r] - factor * image[r, c]
            smooth = jacobi[r, c] * residual
            z_pad[r, c + 1] = smooth + added[r]
            if r < 2:
                total = total + residual * smooth
        return total

    def step(k, total):
        for j in range(ROWS):
            total = chunk(k * ROWS + j, total)
        return total

    smooth_total = lax.fori_loop(0, chunks // ROWS, step, jnp.zeros((8, 128), F32))
    faces = (chooser(east.at[0], east.at[1]), chooser(north.at[0], north.at[1], end_n), chooser(center.at[0], center.at[1]))
    image_total = apply_operator(z_pad, faces, 2, image_o)
    sums_o[...] = two_sums(smooth_total, image_total)


def pair_kernel(mine, mates, out):
    out[...] = jnp.broadcast_to((mine[...] + mates[...])[None], out.shape)


def last_kernel(parts, scalars, forcing, z_first, image_first, z_second, image_second, solution_o, residual_o,
                solution_v, residual_v, out_sems):
    chunks = forcing.shape[1]
    saves = Loads([(solution_v, solution_o), (residual_v, residual_o)], out_sems, chunks)
    energy_next, image_energy = sums_of(jnp.sum(parts[...], axis=0))
    alpha, energy = scalars[0:1, 0:1], scalars[1:2, 0:1]
    energy_next = energy_next + scalars[2:3, 0:1]
    beta = energy_next / energy
    alpha_next = energy_next / (image_energy - beta * energy_next / alpha)
    alpha, beta, alpha_next = [x.reshape(1, 1, 1) for x in (alpha, beta, alpha_next)]
    per_group = chunks // GROUPS // PIECE

    def step(k, carry):
        c = pl.multiple_of(k * PIECE, PIECE)
        part, shifted = pl.ds(c, PIECE), pl.ds(c + 1, PIECE)
        for r in range(2):
            z, image = z_first[r, shifted], image_first[r, part]
            solution_v[r, part] = alpha * z + alpha_next * (z_second[r, shifted] + beta * z)
            residual_v[r, part] = (forcing[r, part] - alpha * image) - alpha_next * (image_second[r, part] + beta * image)

        @pl.when(lax.rem(k, per_group) == per_group - 1)
        def _():
            for i in range(2):
                saves.copy(i, lax.div(k, per_group)).start()

        return carry

    lax.fori_loop(0, chunks // PIECE, step, 0)
    for group in range(GROUPS):
        saves.wait(group)


def body(forcing, east, north, storage, coarse_inverse, membership, land):
    rows, width = forcing.shape
    chunks = width // 128
    inverse = jnp.transpose(coarse_inverse, (1, 2, 0))

    def blocked(x):
        return x.reshape(2, 8, chunks, 128).transpose(0, 2, 1, 3)

    forcing, east, north, storage = [blocked(x) for x in (forcing, east, north, storage)]
    devices = lax.axis_size(GY)
    mates = [(i, i ^ 1) for i in range(devices)]
    others = [(i, j) for i in range(devices) if (j := ((i + 1) ^ 1) - 1) in range(devices)]
    inner, outer = lax.axis_size(GY[1]) * lax.axis_size(GY[2]), lax.axis_size(GY[0])

    def call(kernel, outs, *args, scratch=()):
        places, kept_in = {"H": pltpu.HBM}, {"V": pltpu.VMEM, "H": pltpu.HBM}
        kinds, values = [], []
        for kind, items in args:
            for x in items:
                kinds.append(kind)
                space = kept_in.get(kind)
                values.append(pltpu.with_memory_space_constraint(x, space) if space is not None else x)
        return pl.pallas_call(
            kernel,
            out_shape=[kept_in[k](s, d) if k in kept_in else jax.ShapeDtypeStruct(s, d) for k, s, d in outs],
            in_specs=[pl.BlockSpec(memory_space=places.get(k, pltpu.VMEM)) for k in kinds],
            out_specs=[pl.BlockSpec(memory_space=places.get(k, pltpu.VMEM)) for k, _, _ in outs],
            scratch_shapes=list(scratch),
            compiler_params=pltpu.CompilerParams(vmem_limit_bytes=VMEM_LIMIT),
        )(*values)

    def everywhere(copies):
        near = lax.all_to_all(copies, GY[1:], 0, 0)
        (copies,) = call(sum_kernel, [("V", (outer,) + near.shape[1:], F32)], ("V", [near]))
        return lax.all_to_all(copies, GY[0], 0, 0)

    own_shape, all_shape, end_shape = (2, chunks, 8, 128), (3, chunks, 8, 128), (chunks, 8, 128)
    halo, pad_shape = (6, chunks, 1, 128), (3, chunks + 2, 8, 128)
    own_v = pltpu.VMEM(own_shape, F32)
    codes_v, columns = pltpu.VMEM((3, chunks, 128), F32), pltpu.VMEM((3, ORDER, chunks, 128), F32)

    def dma(*shape):
        return pltpu.SemaphoreType.DMA(shape)

    sums, codes, gather, scatter, lanes, patterns = call(
        moments_kernel,
        [("", (inner, 8, 128), F32), ("V", (8, membership.shape[1]), F32), ("V", (64, 256), BF16), ("V", (128, 128), BF16),
         ("V", (2, 32, 128), F32), ("V", (3, ORDER, 8, 128), F32)],
        ("H", [forcing, membership, land, *[jnp.asarray(x) for x in tables()]]),
        scratch=(own_v, codes_v, pltpu.VMEM(membership.shape, I32), pltpu.VMEM(land.shape, I32), dma(1, HALVES), dma(7)),
    )
    parts = everywhere(sums)
    east, north, center, mate, other = call(
        faces_kernel,
        [("V", (2, chunks + 1, 8, 128), F32)] + [("H", own_shape, F32)] * 2 + [("V", halo, F32)] * 2,
        ("V", [codes]), ("H", [forcing, east, north, storage]),
        scratch=(own_v, own_v, codes_v) + (own_v,) * 4 + (dma(4, GROUPS), dma(2, GROUPS)),
    )
    mate = lax.ppermute(mate, GY, mates)
    other = lax.ppermute(other, GY, others)
    field, north, center, z_first, image_first, sums, kept, jacobi, end_f, end_n = call(
        second_kernel,
        [("V", own_shape, F32)] * 3 + [("V", pad_shape, F32), ("V", all_shape, F32), ("V", (inner, 9, 1, 128), F32), ("V", (16, 128), F32),
         ("V", all_shape, F32), ("V", end_shape, F32), ("V", end_shape, F32)],
        ("V", [parts]), ("H", [forcing, north, center]),
        ("V", [mate, other, inverse, codes, gather, scatter, lanes, patterns, east]),
        scratch=(codes_v, pltpu.VMEM((chunks + 1, 8, 128), F32), pltpu.VMEM(end_shape, F32), columns, dma(3, EIGHTHS)),
    )
    parts = everywhere(sums)
    z_second, image_second, sums, scalars = call(
        third_kernel,
        [("V", pad_shape, F32), ("V", own_shape, F32), ("V", (1, 128), F32), ("V", (8, 128), F32)],
        ("V", [parts]),
        ("V", [kept, inverse, field, image_first, codes, scatter, patterns, east, north, center, jacobi, end_f, end_n]),
        scratch=(codes_v, columns, pltpu.VMEM((8, 128), F32)),
    )
    chips = lax.axis_size(GY[:2])
    swapped = lax.ppermute(sums, GY[2], [(0, 1), (1, 0)])
    (sums,) = call(pair_kernel, [("V", (chips, 1, 128), F32)], ("V", [sums, swapped]))
    parts = lax.all_to_all(sums, GY[:2], 0, 0)
    answer = call(
        last_kernel,
        [("H", own_shape, F32)] * 2,
        ("V", [parts]), ("V", [scalars, field, z_first, image_first, z_second, image_second]),
        scratch=(own_v,) * 2 + (dma(2, GROUPS),),
    )
    return tuple(x.transpose(0, 2, 1, 3).reshape(rows, width) for x in answer)


def solution(mesh):
    finer = Mesh(mesh.devices.reshape(mesh.shape["ens"], 8, 8, 2), ("ens", "gy_0", "gy_1", "gy_2"))
    return jax.shard_map(
        body,
        mesh=finer,
        in_specs=(P(ENS_GY, None), P(GY, None), P(GY, None), P(GY, None), P(), P(), P()),
        out_specs=(P(ENS_GY, None), P(ENS_GY, None)),
        check_vma=False,
    )
```

```python
import jax
import jax.numpy as jnp
import numpy as np
from jax import lax
from jax.experimental import pallas as pl
from jax.experimental.pallas import tpu as pltpu
from jax.sharding import Mesh
from jax.sharding import PartitionSpec as P


TILE = 64
ORDER = 4
GY = ("gy_0", "gy_1", "gy_2")
ENS_GY = ("ens", "gy_0", "gy_1", "gy_2")
F32, BF16, I32 = jnp.float32, jnp.bfloat16, jnp.int32
ROWS = 32
PIECE = 32
BLOCK = 64
GROUPS = 4
HALVES = 2
VMEM_LIMIT = 24 * 2**20


def tables():
    degree = np.arange(ORDER)[:, None]
    mode = np.cos(np.pi * degree * (np.arange(TILE)[None, :] + 0.5) / TILE)
    p_of = np.tile(np.repeat(np.arange(ORDER), ORDER), 2)
    q_of = np.tile(np.arange(ORDER), 2 * ORDER)
    half = np.repeat(np.arange(2), ORDER * ORDER)
    lane = np.arange(128)
    cols = (mode[q_of][:, lane % TILE] * (half[:, None] == lane[None, :] // TILE)).astype(np.float32)
    high = cols.astype(BF16)
    low = (cols - high.astype(np.float32)).astype(BF16)
    gather = np.concatenate([np.concatenate([high, high], axis=1), np.concatenate([low, np.zeros_like(low)], axis=1)], axis=0)
    scatter = np.concatenate([high, high, low, np.zeros_like(low)], axis=0)
    rows = mode[p_of].reshape(32, 8, 8).transpose(1, 0, 2).astype(np.float32)
    row_lanes = np.tile(rows, (1, 1, 16))
    row_subs = np.broadcast_to(mode.reshape(ORDER, 8, 8, 1).transpose(1, 0, 2, 3), (8, ORDER, 8, 128)).astype(np.float32)
    ends = np.zeros((TILE // 16, ORDER, 8, 128), np.float32)
    for k in range(TILE // 16):
        ends[k, :, :4] = row_subs[(2 * k + 2) % 8, :, :4]
        ends[k, :, 4:] = row_subs[(2 * k - 1) % 8, :, 4:]
    return gather, scatter, row_lanes, row_subs, ends


def iota(shape, dim):
    return lax.broadcasted_iota(I32, shape, dim)


def onehot(codes):
    return jnp.where(codes == (iota(codes.shape, 1) % TILE).astype(F32), 1.0, 0.0).astype(BF16)


def spread_row(ref, row):
    return jnp.broadcast_to(ref[pl.ds(row, 1)], (8, 128))


def dot_nt(a, b):
    return lax.dot_general(a, b, (((1,), (1,)), ((), ())), preferred_element_type=F32)


def dot_nn(a, b):
    return lax.dot_general(a, b, (((1,), (0,)), ((), ())), preferred_element_type=F32)


def split(x):
    high = x.astype(BF16)
    return high, (x - high.astype(F32)).astype(BF16)


def expand(codes_small, out):
    chunks, tiles = out.shape[1], codes_small.shape[1]
    mine = iota((chunks, tiles), 1) // 2 == iota((chunks, tiles), 0)
    halves = jnp.where(iota((tiles, 128), 0) % 2 == iota((tiles, 128), 1) // TILE, 1.0, 0.0).astype(BF16)
    for k in range(3):
        out[k] = dot_nn(jnp.where(mine, codes_small[k : k + 1], 0.0).astype(BF16), halves)


def moments(field, codes, gather, lanes, loads=None):
    wide = [jnp.concatenate([lanes[r]] * (BLOCK * 8 // 128), axis=1) for r in range(2)]

    total = jnp.zeros((32, 128), F32)
    for k in range(codes.shape[1] // BLOCK):
        first = k * BLOCK
        if loads is not None and first % loads.size == 0:
            loads.wait(first // loads.size)
        lifted = jnp.zeros((32, BLOCK * 8), F32)
        for r in range(2):
            both = dot_nt(gather[...], jnp.concatenate(split(field[r, pl.ds(first, BLOCK)].reshape(BLOCK * 8, 128)), axis=1))
            lifted = lifted + wide[r] * (both[:32] + both[32:])
        own = onehot(jnp.concatenate([spread_row(codes.at[0], first + j) for j in range(BLOCK)], axis=0))
        parts = dot_nn(jnp.concatenate(split(lifted), axis=0), own)
        total = total + parts[:32] + parts[32:]
    sums = total[:16] + pltpu.roll(total[16:], TILE, 1)
    return jnp.where(iota((8, 128), 1) < TILE, sums[:8], pltpu.roll(sums[8:], TILE, 1))


def unpack(tile):
    return jnp.concatenate([tile, pltpu.roll(tile, TILE, 1)], axis=0)[:, :TILE]


def coarse_solve(inverse, sums):
    coef = jnp.zeros_like(sums)
    for j in range(sums.shape[0]):
        coef = coef + inverse[j] * sums[j : j + 1]
    return coef


def total_of(x):
    return jnp.sum(jnp.sum(x, axis=1, keepdims=True), axis=0, keepdims=True)


def column_tables(coef, codes, scatter, out):
    zero = jnp.zeros_like(coef)
    rows = [jnp.concatenate([coef, zero], axis=1), jnp.concatenate([zero, coef], axis=1)]
    high, low = split(jnp.concatenate(rows * 4, axis=0))
    for row in range(3):
        own = onehot(codes[row])
        per_tile = dot_nt(own, high) + dot_nt(own, low)
        lane = iota(per_tile.shape, 1)
        rounded = per_tile.astype(BF16).astype(F32)
        pieces = jnp.where(lane // 32 == 1, per_tile - rounded, rounded)
        split_p = [jnp.where(lane // ORDER % ORDER == p, pieces, 0.0).astype(BF16) for p in range(ORDER)]
        columns = dot_nn(jnp.concatenate(split_p, axis=0), scatter[...])
        for p in range(ORDER):
            out[row, p] = columns[p * codes.shape[1] : (p + 1) * codes.shape[1]]


def sum_kernel(parts, out):
    out[...] = jnp.broadcast_to(jnp.sum(parts[...], axis=0)[None], out.shape)


def two_sums(left, right):
    left, right = [x + pltpu.roll(x, TILE, 1) for x in (left, right)]
    return jnp.sum(jnp.where(iota((8, 128), 1) < TILE, left, right), axis=0, keepdims=True)


def sums_of(row):
    left = iota(row.shape, 1) < TILE
    return [jnp.sum(jnp.where(x, row, 0.0), axis=1, keepdims=True) for x in (left, jnp.logical_not(left))]


def scalar_rows(values):
    tile = jnp.zeros((8, 128), F32)
    for k, value in enumerate(values):
        tile = jnp.where(iota((8, 128), 0) == k, value, tile)
    return tile


class Loads:
    def __init__(self, pairs, sems, chunks, groups=GROUPS):
        self.pairs, self.sems, self.size, self.groups = pairs, sems, chunks // groups, groups

    def copy(self, i, group):
        source, target = self.pairs[i]
        part = pl.ds(pl.multiple_of(group * self.size, self.size), self.size)
        return pltpu.make_async_copy(source.at[:, part], target.at[:, part], self.sems.at[i, group])

    def start(self, order=None):
        for group in range(self.groups) if order is None else order:
            for i in range(len(self.pairs)):
                self.copy(i, group).start()

    def wait(self, group):
        for i in range(len(self.pairs)):
            self.copy(i, group).wait()


def position(membership):
    rows, total_rows = 2 * 8, membership.shape[0] * TILE
    index = lax.axis_index(GY)
    start = index * rows
    after = jnp.where(start + rows < total_rows, lax.div(start + rows, TILE), -1)
    before = jnp.where(start > 0, lax.div(start - 1, TILE), -1)
    return lax.div(lax.rem(start, TILE), 8), (lax.div(start, TILE), after, before)


def moments_kernel(forcing, membership, land, gather, scatter, row_lanes, row_subs, ends,
                   sums_o, codes_o, gather_o, scatter_o, lanes_o, patterns_o, field, codes, member_in, land_in, sems, small):
    chunks = forcing.shape[1]
    block, tile_rows = position(membership)
    pairs = [(membership, member_in), (land, land_in), (gather, gather_o), (row_lanes.at[pl.ds(block, 2)], lanes_o),
             (scatter, scatter_o), (row_subs.at[pl.ds(block, 2)], patterns_o.at[0:2]), (ends.at[lax.div(block, 2)], patterns_o.at[2])]
    copies = [pltpu.make_async_copy(x, y, small.at[i]) for i, (x, y) in enumerate(pairs)]
    for copy in copies:
        copy.start()
    loads = Loads([(forcing, field)], sems, chunks, HALVES)
    loads.start()
    for copy in copies:
        copy.wait()
    for k in range(3):
        row = pl.ds(jnp.maximum(tile_rows[k], 0), 1)
        dry = (land_in[row] == 1) | (tile_rows[k] < 0)
        codes_o[k : k + 1] = jnp.where(dry, TILE, member_in[row]).astype(F32)
    expand(codes_o, codes)
    tile = moments(field, codes, gather_o, lanes_o, loads)
    sums_o[...] = jnp.broadcast_to(tile[None], sums_o.shape)


def faces_kernel(codes_small, forcing, east, north, storage, east_o, north_h, center_h, mate_o, other_o,
                 north_o, center_o, codes, f_in, e_in, n_in, s_in, sems, out_sems):
    chunks = forcing.shape[1]
    loads = Loads([(east, e_in), (north, n_in), (storage, s_in), (forcing, f_in)], sems, chunks)
    loads.start((3, 0, 1, 2))
    saves = Loads([(north_o, north_h), (center_o, center_h)], out_sems, chunks)
    expand(codes_small, codes)
    lane, sub = iota((8, 128), 1), iota((8, 128), 0)
    odd = lax.rem(lax.axis_index(GY), 2) == 1

    def rolled(x):
        return pltpu.roll(x, 1, 1)

    def after_of(row):
        code = spread_row(codes.at[0], row)
        return code, pltpu.roll(code, 127, 1)

    def east_of(c, here, turned, turned_next):
        mask = (here < TILE) & (jnp.where(lane == 127, turned_next, turned) < TILE)
        return [jnp.where(mask, e_in[r, c], 0.0) for r in range(2)]

    first_code, first_turned = after_of(0)
    loads.wait(3)
    last = east_of(chunks - 1, *after_of(chunks - 1), first_turned)
    for r in range(2):
        east_o[r, 0] = last[r]

    def chunk(k, j, carry):
        west_before, here, turned = carry
        c = k * ROWS + j
        ahead = k * ROWS + j + 1 if j + 1 < ROWS else lax.rem(k * ROWS + ROWS, chunks)
        coming, coming_turned = after_of(ahead)
        face = east_of(c, here, turned, coming_turned)
        wet = here < TILE
        open_north = wet & ((sub < 7) | (spread_row(codes.at[1], c) < TILE))
        west_next = [rolled(x) for x in face]
        west = [jnp.where(lane == 0, west_before[r], west_next[r]) for r in range(2)]
        norths = [jnp.where(wet, n_in[0, c], 0.0), jnp.where(open_north, n_in[1, c], 0.0)]
        shifted = [pltpu.roll(x, 1, 0) for x in norths]
        south = [jnp.where(sub == 0, 0.0, shifted[0]), jnp.where(sub == 0, shifted[0], shifted[1])]
        fields, centers = [f_in[0, c], f_in[1, c]], []
        for r in range(2):
            center = jnp.where(wet, s_in[r, c], 1.0) + face[r] + west[r] + norths[r] + south[r]
            east_o[r, c + 1] = face[r]
            north_o[r, c] = norths[r]
            center_o[r, c] = center
            centers.append(center)
        smooth = jnp.where(sub < 4, fields[0], fields[1]) / jnp.where(sub < 4, centers[0], centers[1])
        first = [x[0][0:1] for x in (fields, centers, face, norths)] + [smooth[1:2]] * 2
        final = [x[1][7:8] for x in (fields, centers, face, norths)] + [smooth[6:7], norths[1][6:7]]
        for j in range(6):
            mate_o[j, c] = jnp.where(odd, first[j], final[j])
            other_o[j, c] = jnp.where(odd, final[j], first[j])
        return west_next, coming, coming_turned

    size = chunks // GROUPS // ROWS

    def step(k, carry):
        @pl.when((lax.rem(k, size) == 0) & (k < (GROUPS - 1) * size))
        def _():
            loads.wait(lax.div(k, size))

        for j in range(ROWS):
            carry = chunk(k, j, carry)

        @pl.when(lax.rem(k, size) == size - 1)
        def _():
            for i in range(2):
                saves.copy(i, lax.div(k, size)).start()

        return carry

    lax.fori_loop(0, chunks // ROWS, step, ([rolled(x) for x in last], first_code, first_turned))
    for group in range(GROUPS):
        saves.wait(group)


def apply_operator(z_pad, faces, blocks, out):
    east, north, center = faces
    chunks = z_pad.shape[1] - 2
    z_pad[:, 0] = z_pad[:, chunks]
    z_pad[:, chunks + 1] = z_pad[:, 1]
    n = PIECE
    sub, lane = iota((n, 8, 128), 1), iota((n, 8, 128), 2)

    def step(k, total):
        c = pl.multiple_of(k * n, n)
        own = [z_pad[r, pl.ds(c + 1, n)] for r in range(3)]
        faced = [north(r, pl.ds(c, n)) for r in range(3)]
        below = [pltpu.roll(faced[r] * own[r], 1, 1) for r in range(3)]
        above = [pltpu.roll(own[r], 7, 1) for r in range(3)]
        for r in range(blocks):
            ahead = pltpu.roll(z_pad[r, pl.ds(c + 1, n + 1)], 127, 2)
            ahead = jnp.where(lane == 127, ahead[1:], ahead[:-1])
            face = east(r, pl.ds(c, n + 1))
            behind = pltpu.roll(face * z_pad[r, pl.ds(c, n + 1)], 1, 2)
            behind = jnp.where(lane == 0, behind[:-1], behind[1:])
            image = (center(r, pl.ds(c, n)) * own[r] - face[1:] * ahead - behind
                     - faced[r] * jnp.where(sub == 7, above[(r + 1) % 3], above[r])
                     - jnp.where(sub == 0, below[(r + 2) % 3], below[r]))
            out[r, pl.ds(c, n)] = image
            if r < 2:
                total = total + jnp.sum(own[r] * image, axis=0)
        return total

    return lax.fori_loop(0, chunks // n, step, jnp.zeros((8, 128), F32))


def chooser(*views):
    return lambda r, part: views[r][part]


class Spread:
    def __init__(self, columns, patterns):
        self.columns = columns
        self.patterns = [[patterns[r, p] for p in range(ORDER)] for r in range(3)]
        self.sub = iota((8, 128), 0)

    def at(self, c):
        def row(k, p):
            return spread_row(self.columns.at[k, p], c)

        own = [row(0, p) for p in range(ORDER)]
        end = [jnp.where(self.sub < 4, row(1, p), row(2, p)) for p in range(ORDER)]
        return [sum(self.patterns[r][p] * x[p] for p in range(ORDER)) for r, x in enumerate((own, own, end))]


def second_kernel(parts, forcing, north_h, center_h, mate, other, inverse, codes_small, gather, scatter, lanes, patterns, east,
                  field, north, center, z_pad, image_o, sums_o, kept_o, jacobi_o, end_f, end_n,
                  codes, end_e, end_c, columns, sems):
    chunks = forcing.shape[1]
    loads = Loads([(forcing, field), (north_h, north), (center_h, center)], sems, chunks)
    loads.start()
    expand(codes_small, codes)
    tile = jnp.sum(parts[...], axis=0)
    sums = unpack(tile)
    coef = coarse_solve(inverse, sums)
    kept_o[0:8] = tile
    kept_o[8:16] = jnp.broadcast_to(total_of(sums * coef), (8, 128))
    column_tables(coef, codes, scatter, columns)
    spread = Spread(columns, patterns)
    sub = iota((8, 128), 0)
    after = jnp.logical_xor(sub < 4, lax.rem(lax.axis_index(GY), 2) == 1)

    def chunk(c, total):
        added = spread.at(c)

        def rows(j):
            return jnp.where(after, mate[j, c], other[j, c])

        faced = jnp.where(sub == 6, rows(5), rows(3))
        far = rows(0)
        beyond = rows(1) + jnp.where(sub == 0, pltpu.roll(north[1, c], 1, 0), 0.0)
        first = center[0, c] + jnp.where(sub == 0, pltpu.roll(faced, 1, 0), 0.0)
        both = jnp.where(sub == 3, pltpu.roll(first, 3, 0), jnp.where(beyond == 0.0, 1.0, beyond))
        inverted = 1.0 / both
        own = [jnp.where(sub == 0, pltpu.roll(inverted, 5, 0), 1.0 / first), 1.0 / center[1, c]]
        end_f[c] = far
        end_n[c] = faced
        end_e[c + 1] = rows(2)
        end_c[c] = both
        center[0, c] = first
        jacobi_o[0, c] = own[0]
        jacobi_o[1, c] = own[1]
        jacobi_o[2, c] = inverted
        smooth = [field[0, c] * own[0], field[1, c] * own[1],
                  jnp.where((sub == 1) | (sub == 6), rows(4), far * inverted)]
        for r in range(3):
            z_pad[r, c + 1] = smooth[r] + added[r]
        return total + (field[0, c] * smooth[0] + field[1, c] * smooth[1])

    size = chunks // GROUPS // ROWS

    def step(k, total):
        @pl.when(lax.rem(k, size) == 0)
        def _():
            loads.wait(lax.div(k, size))

        for j in range(ROWS):
            total = chunk(k * ROWS + j, total)
        return total

    smooth_total = lax.fori_loop(0, chunks // ROWS, step, jnp.zeros((8, 128), F32))
    end_e[0] = end_e[chunks]
    faces = (chooser(east.at[0], east.at[1], end_e), chooser(north.at[0], north.at[1], end_n),
             chooser(center.at[0], center.at[1], end_c))
    image_total = apply_operator(z_pad, faces, 3, image_o)
    tile = moments(image_o, codes, gather, lanes)
    for k in range(9):
        row = tile[k : k + 1] if k < 8 else two_sums(smooth_total, image_total)
        sums_o[:, k] = jnp.broadcast_to(row[None], (sums_o.shape[0], 1, 128))


def third_kernel(parts, kept, inverse, forcing, image, codes_small, scatter, patterns, east, north, center,
                 jacobi, end_f, end_n, z_pad, image_o, sums_o, scalars_o, codes, columns, tile):
    chunks = forcing.shape[1]
    expand(codes_small, codes)
    rows = jnp.sum(parts[...], axis=0)
    for k in range(8):
        tile[k : k + 1] = rows[k]
    energy, image_energy = sums_of(rows[8])
    energy = energy + kept[8:9, 0:1]
    alpha = energy / image_energy
    sums = unpack(kept[0:8] - alpha * tile[...])
    coef = coarse_solve(inverse, sums)
    scalars_o[...] = scalar_rows([alpha, energy, total_of(sums * coef)])
    column_tables(coef, codes, scatter, columns)
    spread = Spread(columns, patterns)
    factor = jnp.broadcast_to(alpha, (8, 128))

    def chunk(c, total):
        added = spread.at(c)
        fields = [forcing[0, c], forcing[1, c], end_f[c]]
        for r in range(3):
            residual = fields[r] - factor * image[r, c]
            smooth = jacobi[r, c] * residual
            z_pad[r, c + 1] = smooth + added[r]
            if r < 2:
                total = total + residual * smooth
        return total

    def step(k, total):
        for j in range(ROWS):
            total = chunk(k * ROWS + j, total)
        return total

    smooth_total = lax.fori_loop(0, chunks // ROWS, step, jnp.zeros((8, 128), F32))
    faces = (chooser(east.at[0], east.at[1]), chooser(north.at[0], north.at[1], end_n), chooser(center.at[0], center.at[1]))
    image_total = apply_operator(z_pad, faces, 2, image_o)
    sums_o[...] = two_sums(smooth_total, image_total)


def pair_kernel(mine, mates, out):
    out[...] = jnp.broadcast_to((mine[...] + mates[...])[None], out.shape)


def last_kernel(parts, scalars, forcing, z_first, image_first, z_second, image_second, solution_o, residual_o,
                solution_v, residual_v, out_sems):
    chunks = forcing.shape[1]
    saves = Loads([(solution_v, solution_o), (residual_v, residual_o)], out_sems, chunks)
    energy_next, image_energy = sums_of(jnp.sum(parts[...], axis=0))
    alpha, energy = scalars[0:1, 0:1], scalars[1:2, 0:1]
    energy_next = energy_next + scalars[2:3, 0:1]
    beta = energy_next / energy
    alpha_next = energy_next / (image_energy - beta * energy_next / alpha)
    alpha, beta, alpha_next = [x.reshape(1, 1, 1) for x in (alpha, beta, alpha_next)]
    per_group = chunks // GROUPS // PIECE

    def step(k, carry):
        c = pl.multiple_of(k * PIECE, PIECE)
        part, shifted = pl.ds(c, PIECE), pl.ds(c + 1, PIECE)
        for r in range(2):
            z, image = z_first[r, shifted], image_first[r, part]
            solution_v[r, part] = alpha * z + alpha_next * (z_second[r, shifted] + beta * z)
            residual_v[r, part] = (forcing[r, part] - alpha * image) - alpha_next * (image_second[r, part] + beta * image)

        @pl.when(lax.rem(k, per_group) == per_group - 1)
        def _():
            for i in range(2):
                saves.copy(i, lax.div(k, per_group)).start()

        return carry

    lax.fori_loop(0, chunks // PIECE, step, 0)
    for group in range(GROUPS):
        saves.wait(group)


def body(forcing, east, north, storage, coarse_inverse, membership, land):
    rows, width = forcing.shape
    chunks = width // 128
    inverse = jnp.transpose(coarse_inverse, (1, 2, 0))

    def blocked(x):
        return x.reshape(2, 8, chunks, 128).transpose(0, 2, 1, 3)

    forcing, east, north, storage = [blocked(x) for x in (forcing, east, north, storage)]
    devices = lax.axis_size(GY)
    mates = [(i, i ^ 1) for i in range(devices)]
    others = [(i, j) for i in range(devices) if (j := ((i + 1) ^ 1) - 1) in range(devices)]
    inner, outer = lax.axis_size(GY[1]) * lax.axis_size(GY[2]), lax.axis_size(GY[0])

    def call(kernel, outs, *args, scratch=()):
        places, kept_in = {"H": pltpu.HBM}, {"V": pltpu.VMEM, "H": pltpu.HBM}
        kinds, values = [], []
        for kind, items in args:
            for x in items:
                kinds.append(kind)
                space = kept_in.get(kind)
                values.append(pltpu.with_memory_space_constraint(x, space) if space is not None else x)
        return pl.pallas_call(
            kernel,
            out_shape=[kept_in[k](s, d) if k in kept_in else jax.ShapeDtypeStruct(s, d) for k, s, d in outs],
            in_specs=[pl.BlockSpec(memory_space=places.get(k, pltpu.VMEM)) for k in kinds],
            out_specs=[pl.BlockSpec(memory_space=places.get(k, pltpu.VMEM)) for k, _, _ in outs],
            scratch_shapes=list(scratch),
            compiler_params=pltpu.CompilerParams(vmem_limit_bytes=VMEM_LIMIT),
        )(*values)

    def everywhere(copies):
        near = lax.all_to_all(copies, GY[1:], 0, 0)
        (copies,) = call(sum_kernel, [("V", (outer,) + near.shape[1:], F32)], ("V", [near]))
        return lax.all_to_all(copies, GY[0], 0, 0)

    own_shape, all_shape, end_shape = (2, chunks, 8, 128), (3, chunks, 8, 128), (chunks, 8, 128)
    halo, pad_shape = (6, chunks, 1, 128), (3, chunks + 2, 8, 128)
    own_v = pltpu.VMEM(own_shape, F32)
    codes_v, columns = pltpu.VMEM((3, chunks, 128), F32), pltpu.VMEM((3, ORDER, chunks, 128), F32)

    def dma(*shape):
        return pltpu.SemaphoreType.DMA(shape)

    sums, codes, gather, scatter, lanes, patterns = call(
        moments_kernel,
        [("", (inner, 8, 128), F32), ("V", (8, membership.shape[1]), F32), ("V", (64, 256), BF16), ("V", (128, 128), BF16),
         ("V", (2, 32, 128), F32), ("V", (3, ORDER, 8, 128), F32)],
        ("H", [forcing, membership, land, *[jnp.asarray(x) for x in tables()]]),
        scratch=(own_v, codes_v, pltpu.VMEM(membership.shape, I32), pltpu.VMEM(land.shape, I32), dma(1, HALVES), dma(7)),
    )
    parts = everywhere(sums)
    east, north, center, mate, other = call(
        faces_kernel,
        [("V", (2, chunks + 1, 8, 128), F32)] + [("H", own_shape, F32)] * 2 + [("V", halo, F32)] * 2,
        ("V", [codes]), ("H", [forcing, east, north, storage]),
        scratch=(own_v, own_v, codes_v) + (own_v,) * 4 + (dma(4, GROUPS), dma(2, GROUPS)),
    )
    mate = lax.ppermute(mate, GY, mates)
    other = lax.ppermute(other, GY, others)
    field, north, center, z_first, image_first, sums, kept, jacobi, end_f, end_n = call(
        second_kernel,
        [("V", own_shape, F32)] * 3 + [("V", pad_shape, F32), ("V", all_shape, F32), ("V", (inner, 9, 1, 128), F32), ("V", (16, 128), F32),
         ("V", all_shape, F32), ("V", end_shape, F32), ("V", end_shape, F32)],
        ("V", [parts]), ("H", [forcing, north, center]),
        ("V", [mate, other, inverse, codes, gather, scatter, lanes, patterns, east]),
        scratch=(codes_v, pltpu.VMEM((chunks + 1, 8, 128), F32), pltpu.VMEM(end_shape, F32), columns, dma(3, GROUPS)),
    )
    parts = everywhere(sums)
    z_second, image_second, sums, scalars = call(
        third_kernel,
        [("V", pad_shape, F32), ("V", own_shape, F32), ("V", (1, 128), F32), ("V", (8, 128), F32)],
        ("V", [parts]),
        ("V", [kept, inverse, field, image_first, codes, scatter, patterns, east, north, center, jacobi, end_f, end_n]),
        scratch=(codes_v, columns, pltpu.VMEM((8, 128), F32)),
    )
    chips = lax.axis_size(GY[:2])
    swapped = lax.ppermute(sums, GY[2], [(0, 1), (1, 0)])
    (sums,) = call(pair_kernel, [("V", (chips, 1, 128), F32)], ("V", [sums, swapped]))
    parts = lax.all_to_all(sums, GY[:2], 0, 0)
    answer = call(
        last_kernel,
        [("H", own_shape, F32)] * 2,
        ("V", [parts]), ("V", [scalars, field, z_first, image_first, z_second, image_second]),
        scratch=(own_v,) * 2 + (dma(2, GROUPS),),
    )
    return tuple(x.transpose(0, 2, 1, 3).reshape(rows, width) for x in answer)


def solution(mesh):
    finer = Mesh(mesh.devices.reshape(mesh.shape["ens"], 8, 8, 2), ("ens", "gy_0", "gy_1", "gy_2"))
    return jax.shard_map(
        body,
        mesh=finer,
        in_specs=(P(ENS_GY, None), P(GY, None), P(GY, None), P(GY, None), P(), P(), P()),
        out_specs=(P(ENS_GY, None), P(ENS_GY, None)),
        check_vma=False,
    )
```
